32 devices in a mesh: dp: 16 (over z, x, core), mp: 2 (over y).
Axes of the slice: x: 2, y: 2, z: 4, core: 2. Of those that a mesh axis runs over, the one named last changes fastest.
Arguments:
- inputs: bfloat16 [8192, 2048], P(('dp', 'mp')), may hold values from -6 to 6
- segment_ids: int32 [16, 512], P('dp'), may hold values from 0 to 3, never falling along the last dimension, each value on 1 to 256 neighbouring positions
- norm1_gain: float32 [2048], replicated, may hold values from 0.5 to 1.5
- norm1_shift: float32 [2048], replicated, may hold values from -3 to 3
- qkv_weight: bfloat16 [3, 2048, 2048], P(None, 'dp', 'mp'), may hold values from -0.125 to 0.125
- qkv_bias: float32 [3, 2048], P(None, 'mp'), may hold values from -64 to 64
- out_weight: bfloat16 [2048, 2048], P('mp', 'dp'), may hold values from -0.5 to 0.5
- norm2_gain: float32 [2048], replicated, may hold values from 0.5 to 1.5
- norm2_shift: float32 [2048], replicated, may hold values from -3 to 3
- gate_weight: bfloat16 [2048, 5632], P('dp', 'mp'), may hold values from -0.125 to 0.125
- up_weight: bfloat16 [2048, 5632], P('dp', 'mp'), may hold values from -0.125 to 0.125
- down_weight: bfloat16 [5632, 2048], P('mp', 'dp'), may hold values from -0.078125 to 0.078125
- cotangent: bfloat16 [8192, 2048], P(('dp', 'mp')), may hold values from -6 to 6
Outputs:
- output: bfloat16 [8192, 2048], P(('dp', 'mp'))
- input_grad: float32 [8192, 2048], P(('dp', 'mp'))
- norm1_gain_grad: float32 [2048], replicated
- norm1_shift_grad: float32 [2048], replicated
- qkv_weight_grad: float32 [3, 2048, 2048], P(None, 'dp', 'mp')
- qkv_bias_grad: float32 [3, 2048], P(None, 'mp')
- out_weight_grad: float32 [2048, 2048], P('mp', 'dp')
- norm2_gain_grad: float32 [2048], replicated
- norm2_shift_grad: float32 [2048], replicated
- gate_weight_grad: float32 [2048, 5632], P('dp', 'mp')
- up_weight_grad: float32 [2048, 5632], P('dp', 'mp')
- down_weight_grad: float32 [5632, 2048], P('mp', 'dp')
The draws below stay inside these ranges and needn't reach their ends.
Inputs may be any that keep to these rules, and one draw needn't show every extreme that they name: Within each row of segment_ids the numbers never fall; each number covers 1 to 256 positions of a row, and one covers exactly 256.
All inputs are finite; a program needn't handle non-finite values.
Results may differ from the reference program's by a relative error of at most 0.017.
The reference program's roundings to bfloat16 on the way count: a program that leaves them out, or rounds other values in their place, can miss the bound.
Values may be sent and summed in bfloat16 or wider, within the bound.
A program may use at most 320 MiB of HBM per device.

```python
import math
import jax
import jax.numpy as jnp
import numpy as np
from jax import lax

D = 2048
FF = 5632
HEAD_DIM = 64
ROT = 16
SEQ = 512
HEADS = 32
SEQS = 16
TOKENS = 8192


def draw_qkv_bias(key, part):
    base = jax.random.truncated_normal(jax.random.fold_in(key, 11), -6.0, 6.0, (3, D), jnp.float32) * 0.5
    return base


def level_of(own_key, shape, split, smallest, high):
    loudness = 1.0
    for dim, shards_of in split:
        heights = jax.random.uniform(jax.random.fold_in(jax.random.fold_in(own_key, 6), dim), (shards_of,), jnp.float32, smallest / len(split), high / len(split))
        loudness = loudness * jnp.repeat(jnp.exp(heights), shape[dim] // shards_of).reshape((-1,) + (1,) * (len(shape) - 1 - dim))
    return loudness


def profile(number_of, total, limit, lean):
    weights = [(1 << 20) // math.isqrt(standing ** lean) + 1 for standing in range(2, number_of + 1)]
    spare, holding = total - limit - (number_of - 1), [1] * (number_of - 1)
    while spare > 0:
        candidates = [i for i in range(number_of - 1) if holding[i] < limit]
        whole, budget = sum([weights[i] for i in candidates]), spare
        for i in candidates:
            extra = min(limit - holding[i], max(1, budget * weights[i] // whole), spare)
            holding[i] = holding[i] + extra
            spare = spare - extra
    return np.array([limit] + holding)


def uneven_parts(key, count, total, bound, slope):
    if count == 2:
        one = jax.random.randint(key, (), max(1, total - bound), min(bound, total - 1) + 1)
        return jnp.stack([one, total - one])
    lengths = jnp.asarray(profile(count, total, bound, slope), jnp.int32)
    couples = (count - 1) // 2
    donor, receiver = lengths[1:1 + 2 * couples:2], lengths[2:2 + 2 * couples:2]
    room = jnp.minimum(donor - 1, bound - receiver)
    passed = jax.random.randint(jax.random.fold_in(key, 1), (couples,), 0, 1 << 20) % (room + 1)
    lengths = lengths.at[1:1 + 2 * couples:2].set(donor - passed).at[2:2 + 2 * couples:2].set(receiver + passed)
    return lengths[jax.random.permutation(jax.random.fold_in(key, 2), count)]


def gaussian(own_key, dims, spread, limit, split=(), kind=jnp.bfloat16):
    result = jax.random.normal(own_key, dims, jnp.float32) * spread
    if len(split) > 0:
        result = level_of(own_key, dims, split, -0.22, 0.18) * result
    return jnp.clip(result, min=-limit, max=limit).astype(kind)


def setup_inputs(seed: int = 0) -> dict:
    key_list = jax.random.split(jax.random.key(seed), 14)
    inputs = gaussian(key_list[0], (TOKENS, D), 1.0, 6.0, ((0, 32),))
    segment_ids = jax.vmap(lambda own: jnp.searchsorted(jnp.cumsum(uneven_parts(own, 4, SEQ, SEQ // 2, 0)), jnp.arange(SEQ), side="right"))(jax.random.split(key_list[1], SEQS)).reshape((SEQS, SEQ)).astype(jnp.int32)
    norm1_gain = jnp.clip(1.0 + 0.1 * jax.random.normal(key_list[2], (D,), jnp.float32), 0.5, 1.5)
    norm1_shift = gaussian(key_list[3], (D,), 0.5, 3.0, (), jnp.float32)
    qkv_weight = gaussian(key_list[4], (3, D, D), D ** -0.5, 0.125, ((1, 16), (2, 2)))
    qkv_bias = draw_qkv_bias(jax.random.fold_in(key_list[13], 71), 0)
    out_weight = gaussian(key_list[6], (D, D), (D // 16) ** -0.5, 0.5, ((0, 2), (1, 16)))
    norm2_gain = jnp.clip(1.0 + 0.1 * jax.random.normal(key_list[7], (D,), jnp.float32), 0.5, 1.5)
    norm2_shift = gaussian(key_list[8], (D,), 0.5, 3.0, (), jnp.float32)
    gate_weight = gaussian(key_list[9], (D, FF), D ** -0.5, 0.125, ((0, 16), (1, 2)))
    up_weight = gaussian(key_list[10], (D, FF), D ** -0.5, 0.125, ((0, 16), (1, 2)))
    down_weight = gaussian(key_list[11], (FF, D), FF ** -0.5, 0.078125, ((0, 2), (1, 16)))
    cotangent = gaussian(key_list[12], (TOKENS, D), 1.0, 6.0, ((0, 32),))
    return {"inputs": inputs, "segment_ids": segment_ids, "norm1_gain": norm1_gain, "norm1_shift": norm1_shift, "qkv_weight": qkv_weight, "qkv_bias": qkv_bias, "out_weight": out_weight, "norm2_gain": norm2_gain, "norm2_shift": norm2_shift, "gate_weight": gate_weight, "up_weight": up_weight, "down_weight": down_weight, "cotangent": cotangent}


NEG = -1e+30
EPS = 1e-05
BASE = 10000.0

def layer_norm(values, norm_gain, norm_shift):
    center = values - lax.optimization_barrier(jnp.mean(values, axis=-1, keepdims=True))
    inverse = lax.rsqrt(lax.optimization_barrier(jnp.mean(center * center, axis=-1, keepdims=True)) + EPS)
    scaled = center * inverse
    return (scaled * norm_gain + norm_shift, scaled, inverse)

def norm_back(grads, scaled, inverse, norm_gain):
    weighted = grads * norm_gain
    return inverse * (weighted - lax.optimization_barrier(jnp.mean(weighted, axis=-1, keepdims=True)) - scaled * lax.optimization_barrier(jnp.mean(weighted * scaled, axis=-1, keepdims=True)))

def rotary_tables(segments, rotary_dims):
    length = segments.shape[0]
    places = jnp.arange(length, dtype=jnp.int32)
    earlier = (segments[None, :] < segments[:, None]).astype(jnp.int32)
    position = (places - lax.optimization_barrier(jnp.sum(earlier, axis=1))).astype(jnp.float32)
    half_dims = rotary_dims // 2
    frequency = BASE ** (-2.0 * jnp.arange(half_dims, dtype=jnp.float32) / rotary_dims)
    angles = position[:, None] * frequency[None, :]
    return (jnp.cos(angles), jnp.sin(angles))

def rotate(values, cosine, sine_table, rotary_dims, turn_sign):
    half_dims = rotary_dims // 2
    leading = values[..., :half_dims]
    trailing = values[..., half_dims:rotary_dims]
    cos_rows = cosine[:, None, :]
    sin_rows = turn_sign * sine_table[:, None, :]
    return jnp.concatenate([leading * cos_rows - trailing * sin_rows, trailing * cos_rows + leading * sin_rows, values[..., rotary_dims:]], axis=-1)

def product(form, left, right):
    return jnp.einsum(form, left.astype(jnp.float32), right.astype(jnp.float32))

def masked_scores(query, key, allowed, score_scale):
    scores = product('qhd,khd->hqk', query, key) * score_scale
    return jnp.where(allowed[None], scores, NEG)

def reference(inputs, segment_ids, norm1_gain, norm1_shift, qkv_weight, qkv_bias, out_weight, norm2_gain, norm2_shift, gate_weight, up_weight, down_weight, cotangent):
    score_scale = HEAD_DIM ** (-0.5)
    rows_all = inputs.reshape(SEQS, SEQ, D)
    cot_all = cotangent.reshape(SEQS, SEQ, D)
    places = jnp.arange(SEQ, dtype=jnp.int32)
    causal = places[None, :] <= places[:, None]
    rotated_cols = jnp.arange(D, dtype=jnp.int32) % HEAD_DIM < ROT

    def one_sequence(carry, items):
        rows, cot_rows, segments = items
        stream = rows.astype(jnp.float32)
        normed_wide, scaled_one, inverse_one = layer_norm(stream, norm1_gain, norm1_shift)
        normed_one = normed_wide.astype(jnp.bfloat16)
        projected = jnp.stack([jnp.dot(normed_one, qkv_weight[member], preferred_element_type=jnp.float32) + qkv_bias[member] for member in range(3)])
        shaped = projected.reshape(3, SEQ, HEADS, HEAD_DIM)
        cosine, sine_table = rotary_tables(segments, ROT)
        query = rotate(shaped[0], cosine, sine_table, ROT, 1.0).astype(jnp.bfloat16)
        key_rot = rotate(shaped[1], cosine, sine_table, ROT, 1.0).astype(jnp.bfloat16)
        value = shaped[2].astype(jnp.bfloat16)
        allowed = causal & (segments[:, None] == segments[None, :])
        scores = masked_scores(query, key_rot, allowed, score_scale)
        row_max = lax.optimization_barrier(jnp.max(scores, axis=-1, keepdims=True))
        exponent = jnp.exp(scores - row_max)
        row_total = lax.optimization_barrier(jnp.sum(exponent, axis=-1, keepdims=True))
        log_total = row_max + jnp.log(row_total)
        probs_low = (exponent / row_total).astype(jnp.bfloat16)
        mixed_heads = product('hqk,khd->qhd', probs_low, value).astype(jnp.bfloat16)
        mixed = mixed_heads.reshape(SEQ, D)
        middle = stream + jnp.dot(mixed, out_weight, preferred_element_type=jnp.float32)
        normed_wide2, scaled_two, inverse_two = layer_norm(middle, norm2_gain, norm2_shift)
        normed_two = normed_wide2.astype(jnp.bfloat16)
        gate = jnp.dot(normed_two, gate_weight, preferred_element_type=jnp.float32)
        upward = jnp.dot(normed_two, up_weight, preferred_element_type=jnp.float32)
        sigma = jax.nn.sigmoid(gate)
        hidden = (gate * sigma * upward).astype(jnp.bfloat16)
        output = (middle + jnp.dot(hidden, down_weight, preferred_element_type=jnp.float32)).astype(jnp.bfloat16)
        cot_wide = cot_rows.astype(jnp.float32)
        down_term = jnp.dot(hidden.T, cot_rows, preferred_element_type=jnp.float32)
        hidden_grad = jnp.dot(cot_rows, down_weight.T, preferred_element_type=jnp.float32)
        gate_act = (hidden_grad * upward * sigma * (1.0 + gate * (1.0 - sigma))).astype(jnp.bfloat16)
        up_act = (hidden_grad * gate * sigma).astype(jnp.bfloat16)
        gate_term = jnp.dot(normed_two.T, gate_act, preferred_element_type=jnp.float32)
        up_term = jnp.dot(normed_two.T, up_act, preferred_element_type=jnp.float32)
        normed_two_grad = jnp.dot(gate_act, gate_weight.T, preferred_element_type=jnp.float32) + jnp.dot(up_act, up_weight.T, preferred_element_type=jnp.float32)
        gain_two = lax.optimization_barrier(jnp.sum(normed_two_grad * scaled_two, axis=0))
        shift_two = lax.optimization_barrier(jnp.sum(normed_two_grad, axis=0))
        middle_grad = cot_wide + norm_back(normed_two_grad, scaled_two, inverse_two, norm2_gain)
        middle_low = middle_grad.astype(jnp.bfloat16)
        out_term = jnp.dot(mixed.T, middle_low, preferred_element_type=jnp.float32)
        mixed_grad = jnp.dot(middle_low, out_weight.T, preferred_element_type=jnp.float32).astype(jnp.bfloat16).reshape(SEQ, HEADS, HEAD_DIM)
        probs_wide = jnp.exp(scores - log_total)
        value_grad = product('hqk,qhd->khd', probs_wide.astype(jnp.bfloat16), mixed_grad)
        prob_grad = product('qhd,khd->hqk', mixed_grad, value)
        row_delta = jnp.transpose(lax.optimization_barrier(jnp.sum(mixed_grad.astype(jnp.float32) * mixed_heads.astype(jnp.float32), axis=-1)))
        score_grad = (probs_wide * (prob_grad - row_delta[:, :, None]) * score_scale).astype(jnp.bfloat16)
        query_grad = product('hqk,khd->qhd', score_grad, key_rot)
        key_grad = product('hqk,qhd->khd', score_grad, query)
        query_back = rotate(query_grad, cosine, sine_table, ROT, -1.0)
        key_back = rotate(key_grad, cosine, sine_table, ROT, -1.0)
        proj_grad = jnp.stack([query_back.reshape(SEQ, D), key_back.reshape(SEQ, D), value_grad.reshape(SEQ, D)])
        bias_sums = lax.optimization_barrier(jnp.sum(proj_grad, axis=1))
        bias_term = jnp.stack([bias_sums[0], jnp.where(rotated_cols, bias_sums[1], 0.0), bias_sums[2]])
        proj_low = proj_grad.astype(jnp.bfloat16)
        qkv_term = jnp.stack([jnp.dot(normed_one.T, proj_low[member], preferred_element_type=jnp.float32) for member in range(3)])
        normed_one_grad = jnp.dot(proj_low[0], qkv_weight[0].T, preferred_element_type=jnp.float32)
        normed_one_grad = normed_one_grad + jnp.dot(proj_low[1], qkv_weight[1].T, preferred_element_type=jnp.float32)
        normed_one_grad = normed_one_grad + jnp.dot(proj_low[2], qkv_weight[2].T, preferred_element_type=jnp.float32)
        gain_one = lax.optimization_barrier(jnp.sum(normed_one_grad * scaled_one, axis=0))
        shift_one = lax.optimization_barrier(jnp.sum(normed_one_grad, axis=0))
        input_grad = middle_grad + norm_back(normed_one_grad, scaled_one, inverse_one, norm1_gain)
        terms = (gain_one, shift_one, qkv_term, bias_term, out_term, gain_two, shift_two, gate_term, up_term, down_term)
        carry = tuple((old + new for old, new in zip(carry, terms)))
        return (carry, (output, input_grad))
    start = (jnp.zeros((D,), jnp.float32), jnp.zeros((D,), jnp.float32), jnp.zeros((3, D, D), jnp.float32), jnp.zeros((3, D), jnp.float32), jnp.zeros((D, D), jnp.float32), jnp.zeros((D,), jnp.float32), jnp.zeros((D,), jnp.float32), jnp.zeros((D, FF), jnp.float32), jnp.zeros((D, FF), jnp.float32), jnp.zeros((FF, D), jnp.float32))
    sums, (outputs, grads) = lax.scan(one_sequence, start, (rows_all, cot_all, segment_ids))
    return (outputs.reshape(TOKENS, D), grads.reshape(TOKENS, D), sums[0], sums[1], sums[2], sums[3], sums[4], sums[5], sums[6], sums[7], sums[8], sums[9])
```

```python
import functools

import jax
import jax.numpy as jnp
from jax import lax
from jax.experimental import pallas as pl
from jax.experimental.pallas import tpu as pltpu
from jax.sharding import PartitionSpec as P

HEAD_DIM = 64
ROT = 16


NEG = -1e30
EPS = 1e-05
BASE = 10000.0

MESH = pl.DeviceIdType.MESH
VMEM_LIMIT = 60 * 1024 * 1024


def chip_at(spot, chips):
    side = spot // (chips // 2)
    return (spot + side * (chips - 1 - 2 * spot)) * 2 + side


def span(start, size):
    return pl.ds(pl.multiple_of(start, size), size)


def remote(src, dst, send, recv, who):
    return pltpu.make_async_remote_copy(
        src_ref=src,
        dst_ref=dst,
        send_sem=send,
        recv_sem=recv,
        device_id={"dp": who},
        device_id_type=MESH,
    )


def ring_kernel(chips, gathers, scatters, *refs):
    refs = list(refs)

    def take(number):
        taken = refs[:number]
        del refs[:number]
        return taken

    shards, parts, fulls, outs = take(gathers), take(scatters), take(gathers), take(scatters)
    mine, pair, ring, last = take(scatters), take(scatters), take(scatters), take(scatters)
    if gathers:
        keep_sem, give_sem, got_sem, lend_sem, lent_sem = take(5)
    if scatters:
        load_sem, pair_send, pair_recv, send_sem, recv_sem, last_send, last_recv = take(7)
    device = lax.axis_index("dp")
    chip, core = device // 2, device % 2
    row, side = chip // 2, chip % 2
    spot, way = row + side * (chips - 1 - 2 * row), 1 - 2 * core
    partner = device + way
    after = chip_at((spot + 1) % chips, chips)
    before = chip_at((spot + chips - 1) % chips, chips)
    source = chip_at((spot + chips - way) % chips, chips)
    target = chip_at((spot + chips + way) % chips, chips) * 2 + core
    barrier = pltpu.get_barrier_semaphore()
    for who in (source * 2, source * 2 + 1, partner):
        pl.semaphore_signal(barrier, inc=1, device_id={"dp": who}, device_id_type=MESH)
    pl.semaphore_wait(barrier, 3)
    ends = []

    def begin(copy, end):
        copy.start()
        ends.append(end)
        return copy

    for i in range(gathers):
        unit, cols = shards[i].shape[0], shards[i].shape[1] // 2
        own = fulls[i].at[span(device * unit, unit), :]
        for half, who in ((0, after * 2), (1, before * 2 + 1)):
            copy = remote(
                shards[i].at[:, pl.ds(half * cols, cols)],
                fulls[i].at[span(device * unit, unit), pl.ds(half * cols, cols)],
                give_sem.at[i, half],
                got_sem.at[i, core],
                who,
            )
            begin(copy, copy.wait_send)
        copy = remote(shards[i], own, lend_sem.at[i, 0], lent_sem.at[i, 0], partner)
        begin(copy, copy.wait)
        copy = pltpu.make_async_copy(shards[i], own, keep_sem.at[i])
        begin(copy, copy.wait)

    loads, pairs = {}, {}
    for step in range(chips):
        away = chip_at((spot + 2 * chips + way * (step + 1)) % chips, chips)
        here = chip_at((spot + 2 * chips - way * (step + 1)) % chips, chips)
        for i in range(scatters):
            rows, cols = mine[i].shape[1:]
            copy = remote(
                parts[i].at[span(away * rows, rows), span((1 - core) * cols, cols)],
                pair[i].at[step],
                pair_send.at[i, step],
                pair_recv.at[i, step],
                partner,
            )
            pairs[step, i] = begin(copy, copy.wait_send)
            loads[step, i] = pltpu.make_async_copy(
                parts[i].at[span(here * rows, rows), span(core * cols, cols)],
                mine[i].at[step],
                load_sem.at[i, step],
            )
            loads[step, i].start()

    def gather_step(i, step):
        held = chip_at((spot + 2 * chips - way * step) % chips, chips)
        unit, cols = shards[i].shape[0], shards[i].shape[1] // 2
        block = fulls[i].at[span(held * 2 * unit, 2 * unit), span(core * cols, cols)]
        if step == 1:
            for sender in range(2):
                piece = fulls[i].at[span((held * 2 + sender) * unit, unit), span(core * cols, cols)]
                remote(piece, piece, give_sem.at[i, 0], got_sem.at[i, sender], target).wait_recv()
        else:
            remote(block, block, give_sem.at[i, 0], got_sem.at[i, step], target).wait_recv()
        if step < chips - 1:
            copy = remote(block, block, give_sem.at[i, step + 1], got_sem.at[i, step + 1], target)
            begin(copy, copy.wait_send)
        copy = remote(block, block, lend_sem.at[i, step], lent_sem.at[i, step], partner)
        begin(copy, copy.wait)

    def scatter_step(i, step):
        rows, cols = mine[i].shape[1:]
        lines = min(rows, 32)
        loads[step, i].wait()
        pairs[step, i].wait_recv()
        if step > 0:
            came = ring[i].at[step - 1]
            remote(came, came, send_sem.at[i, 0], recv_sem.at[i, step - 1], target).wait_recv()

        @pl.loop(0, rows // lines)
        def _(k):
            at = span(k * lines, lines)
            total = mine[i][step, at, :].astype(jnp.float32)
            total = total + pair[i][step, at, :].astype(jnp.float32)
            if step > 0:
                total = total + ring[i][step - 1, at, :].astype(jnp.float32)
            if step < chips - 1:
                mine[i][step, at, :] = total.astype(jnp.bfloat16)
            else:
                last[i][at, :] = total

        if step < chips - 1:
            copy = remote(
                mine[i].at[step], ring[i].at[step], send_sem.at[i, step], recv_sem.at[i, step], target
            )
            begin(copy, copy.wait_send)
        else:
            unit = rows // 2
            place = outs[i].at[:, span(core * cols, cols)]
            copy = remote(
                last[i].at[span((1 - core) * unit, unit), :],
                place,
                last_send.at[i, 0],
                last_recv.at[i],
                partner,
            )
            begin(copy, copy.wait)
            copy = pltpu.make_async_copy(
                last[i].at[span(core * unit, unit), :], place, last_send.at[i, 1]
            )
            begin(copy, copy.wait)

    for step in range(chips):
        for i in range(gathers):
            if step > 0:
                gather_step(i, step)
        for i in range(scatters):
            scatter_step(i, step)
    for end in ends:
        end()


def ring_call(shards, parts, call_id):
    size = lax.axis_size("dp")
    chips = size // 2
    gathers, scatters = len(shards), len(parts)
    outs = [jax.ShapeDtypeStruct((s.shape[0] * size, s.shape[1]), s.dtype) for s in shards]
    outs += [jax.ShapeDtypeStruct((p.shape[0] // size, p.shape[1]), jnp.float32) for p in parts]
    blocks = [(p.shape[0] // chips, p.shape[1] // 2) for p in parts]
    scratch = [pltpu.VMEM((chips,) + b, jnp.bfloat16) for b in blocks] * 2
    scratch += [pltpu.VMEM((chips - 1,) + b, jnp.bfloat16) for b in blocks]
    scratch += [pltpu.VMEM(b, jnp.float32) for b in blocks]
    if gathers:
        scratch += [pltpu.SemaphoreType.DMA((gathers,))]
        scratch += [pltpu.SemaphoreType.DMA((gathers, chips))] * 4
    if scatters:
        scratch += [pltpu.SemaphoreType.DMA((scatters, chips))] * 5
        scratch += [pltpu.SemaphoreType.DMA((scatters, 2)), pltpu.SemaphoreType.DMA((scatters,))]
    moved = sum(s.size * 2 * size for s in shards) + sum(p.size * 2 for p in parts)
    return list(
        pl.pallas_call(
            functools.partial(ring_kernel, chips, gathers, scatters),
            out_shape=outs,
            in_specs=[pl.BlockSpec(memory_space=pltpu.VMEM)] * gathers
            + [pl.BlockSpec(memory_space=pl.ANY)] * scatters,
            out_specs=[pl.BlockSpec(memory_space=pl.ANY)] * (gathers + scatters),
            scratch_shapes=scratch,
            compiler_params=pltpu.CompilerParams(
                collective_id=call_id, has_side_effects=True, vmem_limit_bytes=VMEM_LIMIT
            ),
            cost_estimate=pl.CostEstimate(flops=0, bytes_accessed=moved, transcendentals=0),
        )(*shards, *parts)
    )


def layer_norm(values, norm_gain, norm_shift):
    center = values - jnp.mean(values, axis=-1, keepdims=True)
    inverse = lax.rsqrt(jnp.mean(center * center, axis=-1, keepdims=True) + EPS)
    scaled = center * inverse
    return (scaled * norm_gain + norm_shift, scaled, inverse)


def norm_back(grads, scaled, inverse, norm_gain):
    weighted = grads * norm_gain
    return inverse * (
        weighted
        - jnp.mean(weighted, axis=-1, keepdims=True)
        - scaled * jnp.mean(weighted * scaled, axis=-1, keepdims=True)
    )


def rotary_tables(segments, places, rotary_dims):
    earlier = (segments[None, :] < segments[:, None]).astype(jnp.int32)
    position = (places - jnp.sum(earlier, axis=1)).astype(jnp.float32)
    half_dims = rotary_dims // 2
    frequency = BASE ** (-2.0 * jnp.arange(half_dims, dtype=jnp.float32) / rotary_dims)
    angles = position[:, None] * frequency[None, :]
    return (jnp.cos(angles), jnp.sin(angles))


def rotate(values, cosine, sine_table, rotary_dims, turn_sign):
    half_dims = rotary_dims // 2
    leading = values[..., :half_dims]
    trailing = values[..., half_dims:rotary_dims]
    cos_rows = cosine[:, None, :]
    sin_rows = turn_sign * sine_table[:, None, :]
    return jnp.concatenate(
        [
            leading * cos_rows - trailing * sin_rows,
            trailing * cos_rows + leading * sin_rows,
            values[..., rotary_dims:],
        ],
        axis=-1,
    )


def masked_scores(query, key_rot, allowed, score_scale):
    scores = (
        jnp.einsum("qhd,khd->hqk", query, key_rot, preferred_element_type=jnp.float32) * score_scale
    )
    return jnp.where(allowed[None], scores, NEG)


def swap(values):
    return lax.ppermute(values, "mp", [(0, 1), (1, 0)])


def half_sum(part):
    half = part.shape[0] // 2
    other = swap(part[half:].astype(jnp.bfloat16))
    return part[:half] + other.astype(jnp.float32)


def grow(rows):
    return jnp.concatenate([rows, swap(rows)], axis=0)


def scatter(term, axis):
    return lax.psum_scatter(term, "dp", scatter_dimension=axis, tiled=True).astype(jnp.float32)


def body(
    inputs,
    segment_ids,
    norm1_gain,
    norm1_shift,
    qkv_weight,
    qkv_bias,
    out_weight,
    norm2_gain,
    norm2_shift,
    gate_weight,
    up_weight,
    down_weight,
    cotangent,
):
    score_scale = HEAD_DIM ** (-0.5)
    rows_here = inputs.shape[0]
    width = inputs.shape[1]
    input_rows = grow(inputs)
    cot_rows = grow(cotangent)
    *qkv_full, out_turned = ring_call(
        [qkv_weight[0], qkv_weight[1], qkv_weight[2], out_weight.T], [], 0
    )
    gate_weight, out_turned = lax.optimization_barrier((gate_weight, out_turned))
    gate_full = lax.all_gather(gate_weight, "dp", axis=0, tiled=True)
    stream_rows = input_rows.astype(jnp.float32)
    stream = stream_rows[:rows_here]
    normed_wide, scaled_rows, inverse_rows = layer_norm(stream_rows, norm1_gain, norm1_shift)
    normed_one = normed_wide.astype(jnp.bfloat16)
    scaled_one = scaled_rows[:rows_here]
    inverse_one = inverse_rows[:rows_here]
    seq_len = normed_one.shape[0]
    local_width = qkv_full[0].shape[1]
    head_count = local_width // HEAD_DIM
    turn = lax.axis_index("mp") * rows_here
    segments = jnp.roll(segment_ids[0], -turn)
    places = jnp.roll(jnp.arange(seq_len, dtype=jnp.int32), -turn)
    allowed = (places[None, :] <= places[:, None]) & (segments[:, None] == segments[None, :])
    cosine, sine_table = rotary_tables(segments, places, ROT)
    shaped = [
        (jnp.dot(normed_one, full, preferred_element_type=jnp.float32) + bias).reshape(
            seq_len, head_count, HEAD_DIM
        )
        for full, bias in zip(qkv_full, qkv_bias)
    ]
    query = rotate(shaped[0], cosine, sine_table, ROT, 1.0).astype(jnp.bfloat16)
    key_rot = rotate(shaped[1], cosine, sine_table, ROT, 1.0).astype(jnp.bfloat16)
    value = shaped[2].astype(jnp.bfloat16)
    scores = masked_scores(query, key_rot, allowed, score_scale)
    row_max = jnp.max(scores, axis=-1, keepdims=True)
    exponent = jnp.exp(scores - row_max)
    row_total = jnp.sum(exponent, axis=-1, keepdims=True)
    log_total = row_max + jnp.log(row_total)
    probs_low = (exponent / row_total).astype(jnp.bfloat16)
    mixed_heads = jnp.einsum(
        "hqk,khd->qhd", probs_low, value, preferred_element_type=jnp.float32
    ).astype(jnp.bfloat16)
    mixed = mixed_heads.reshape(seq_len, local_width)
    branch = jnp.dot(mixed, out_turned.T, preferred_element_type=jnp.float32)
    middle = stream + half_sum(branch)
    normed_wide2, scaled_two, inverse_two = layer_norm(middle, norm2_gain, norm2_shift)
    normed_here, up_weight, down_weight = lax.optimization_barrier(
        (normed_wide2.astype(jnp.bfloat16), up_weight, down_weight)
    )
    normed_two = grow(normed_here)
    up_full, down_turned = ring_call([up_weight, down_weight.T], [], 1)
    gate = jnp.dot(normed_two, gate_full, preferred_element_type=jnp.float32)
    upward = jnp.dot(normed_two, up_full, preferred_element_type=jnp.float32)
    sigma = jax.nn.sigmoid(gate)
    hidden = (gate * sigma * upward).astype(jnp.bfloat16)
    down_term = jnp.dot(cot_rows.T, hidden, preferred_element_type=jnp.float32)
    down_low, down_turned = lax.optimization_barrier((down_term.astype(jnp.bfloat16), down_turned))
    down_weight_grad = scatter(down_low, 0).T
    hidden_grad = jnp.dot(cot_rows, down_turned, preferred_element_type=jnp.float32)
    gate_act = (hidden_grad * upward * sigma * (1.0 + gate * (1.0 - sigma))).astype(jnp.bfloat16)
    up_act = (hidden_grad * gate * sigma).astype(jnp.bfloat16)
    normed_part = jnp.dot(gate_act, gate_full.T, preferred_element_type=jnp.float32) + jnp.dot(
        up_act, up_full.T, preferred_element_type=jnp.float32
    )
    gate_term = jnp.dot(normed_two.T, gate_act, preferred_element_type=jnp.float32)
    up_term = jnp.dot(normed_two.T, up_act, preferred_element_type=jnp.float32)
    gate_weight_grad = scatter(gate_term.astype(jnp.bfloat16), 0)
    feed_part = jnp.dot(hidden, down_turned.T, preferred_element_type=jnp.float32)
    output = (middle + half_sum(feed_part)).astype(jnp.bfloat16)
    normed_two_grad = half_sum(normed_part)
    gain_two = jnp.sum(normed_two_grad * scaled_two, axis=0)
    shift_two = jnp.sum(normed_two_grad, axis=0)
    middle_grad = cotangent.astype(jnp.float32) + norm_back(
        normed_two_grad, scaled_two, inverse_two, norm2_gain
    )
    middle_rows = grow(middle_grad.astype(jnp.bfloat16))
    out_term = jnp.dot(middle_rows.T, mixed, preferred_element_type=jnp.float32)
    mixed_grad = (
        jnp.dot(middle_rows, out_turned, preferred_element_type=jnp.float32)
        .astype(jnp.bfloat16)
        .reshape(seq_len, head_count, HEAD_DIM)
    )
    probs_wide = jnp.exp(scores - log_total)
    value_grad = jnp.einsum(
        "hqk,qhd->khd",
        probs_wide.astype(jnp.bfloat16),
        mixed_grad,
        preferred_element_type=jnp.float32,
    )
    prob_grad = jnp.einsum("qhd,khd->hqk", mixed_grad, value, preferred_element_type=jnp.float32)
    row_delta = jnp.transpose(
        jnp.sum(mixed_grad.astype(jnp.float32) * mixed_heads.astype(jnp.float32), axis=-1)
    )
    score_grad = (probs_wide * (prob_grad - row_delta[:, :, None]) * score_scale).astype(
        jnp.bfloat16
    )
    query_grad = jnp.einsum("hqk,khd->qhd", score_grad, key_rot, preferred_element_type=jnp.float32)
    key_grad = jnp.einsum("hqk,qhd->khd", score_grad, query, preferred_element_type=jnp.float32)
    query_back = rotate(query_grad, cosine, sine_table, ROT, -1.0)
    key_back = rotate(key_grad, cosine, sine_table, ROT, -1.0)
    proj_grad = [
        part.reshape(seq_len, local_width) for part in (query_back, key_back, value_grad)
    ]
    rotated_cols = jnp.arange(local_width, dtype=jnp.int32) % HEAD_DIM < ROT
    bias_sums = [jnp.sum(part, axis=0) for part in proj_grad]
    bias_term = [bias_sums[0], jnp.where(rotated_cols, bias_sums[1], 0.0), bias_sums[2]]
    proj_low = [part.astype(jnp.bfloat16) for part in proj_grad]
    normed_one_part = jnp.zeros((), jnp.float32)
    for part, full in zip(proj_low, qkv_full):
        normed_one_part = normed_one_part + jnp.dot(
            part, full.T, preferred_element_type=jnp.float32
        )
    normed_one_grad = half_sum(normed_one_part)
    gain_one = jnp.sum(normed_one_part * scaled_rows, axis=0)
    shift_one = jnp.sum(normed_one_part, axis=0)
    norm_sums = jnp.concatenate([gain_one, shift_one, gain_two, shift_two])
    norm_sums = norm_sums + swap(norm_sums)
    sums = jnp.concatenate([norm_sums] + bias_term)
    spare = -sums.size % (8 * 256)
    qkv_term = [
        jnp.dot(normed_one.T, part, preferred_element_type=jnp.float32) for part in proj_low
    ]
    all_sums, up_weight_grad, out_grad_turned, *qkv_weight_grad = ring_call(
        [jnp.pad(sums, (0, spare)).reshape(8, -1)],
        [term.astype(jnp.bfloat16) for term in [up_term, out_term] + qkv_term],
        2,
    )
    out_weight_grad = out_grad_turned.T
    qkv_weight_grad = jnp.stack(qkv_weight_grad)
    all_sums = jnp.sum(all_sums.reshape(-1, 8, all_sums.shape[1]), axis=0).reshape(-1)
    gain_one, shift_one, gain_two, shift_two = all_sums[: 4 * width].reshape(4, width)
    qkv_bias_grad = all_sums[4 * width : sums.size].reshape(3, local_width)
    input_grad = middle_grad + norm_back(normed_one_grad, scaled_one, inverse_one, norm1_gain)
    return (
        output,
        input_grad,
        gain_one,
        shift_one,
        qkv_weight_grad,
        qkv_bias_grad,
        out_weight_grad,
        gain_two,
        shift_two,
        gate_weight_grad,
        up_weight_grad,
        down_weight_grad,
    )


def solution(mesh):
    in_specs = (
        P(("dp", "mp"), None),
        P("dp", None),
        P(),
        P(),
        P(None, "dp", "mp"),
        P(None, "mp"),
        P("mp", "dp"),
        P(),
        P(),
        P("dp", "mp"),
        P("dp", "mp"),
        P("mp", "dp"),
        P(("dp", "mp"), None),
    )
    out_specs = (
        P(("dp", "mp"), None),
        P(("dp", "mp"), None),
        P(),
        P(),
        P(None, "dp", "mp"),
        P(None, "mp"),
        P("mp", "dp"),
        P(),
        P(),
        P("dp", "mp"),
        P("dp", "mp"),
        P("mp", "dp"),
    )
    return jax.shard_map(body, mesh=mesh, in_specs=in_specs, out_specs=out_specs, check_vma=False)
```

```python
import functools

import jax
import jax.numpy as jnp
from jax import lax
from jax.experimental import pallas as pl
from jax.experimental.pallas import tpu as pltpu
from jax.sharding import PartitionSpec as P

HEAD_DIM = 64
ROT = 16


NEG = -1e30
EPS = 1e-05
BASE = 10000.0

MESH = pl.DeviceIdType.MESH
VMEM_LIMIT = 60 * 1024 * 1024


def chip_at(spot, chips):
    side = spot // (chips // 2)
    return (spot + side * (chips - 1 - 2 * spot)) * 2 + side


def span(start, size):
    return pl.ds(pl.multiple_of(start, size), size)


def remote(src, dst, send, recv, who):
    return pltpu.make_async_remote_copy(
        src_ref=src,
        dst_ref=dst,
        send_sem=send,
        recv_sem=recv,
        device_id={"dp": who},
        device_id_type=MESH,
    )


def ring_kernel(chips, gathers, swaps, groups, *refs):
    refs = list(refs)
    scatters = sum(groups)

    def take(number):
        taken = refs[:number]
        del refs[:number]
        return taken

    shards, sends, parts = take(gathers), take(swaps), take(scatters)
    fulls, gets, grouped = take(gathers), take(swaps), take(len(groups))
    outs = []
    for group, out in zip(groups, grouped):
        outs += [out] if group == 1 else [out.at[j] for j in range(group)]
    mine, pair, ring, last = take(scatters), take(scatters), take(scatters), take(scatters)
    if gathers:
        keep_sem, give_sem, got_sem, lend_sem, lent_sem = take(5)
    if swaps:
        swap_send, swap_recv = take(2)
    if scatters:
        load_sem, pair_send, pair_recv, send_sem, recv_sem, last_send, last_recv = take(7)
    device = lax.axis_index("dp")
    chip, core = device // 2, device % 2
    row, side = chip // 2, chip % 2
    spot, way = row + side * (chips - 1 - 2 * row), 1 - 2 * core
    partner = device + way
    after = chip_at((spot + 1) % chips, chips)
    before = chip_at((spot + chips - 1) % chips, chips)
    source = chip_at((spot + chips - way) % chips, chips)
    target = chip_at((spot + chips + way) % chips, chips) * 2 + core
    barrier = pltpu.get_barrier_semaphore()
    for who in (source * 2, source * 2 + 1, partner):
        pl.semaphore_signal(barrier, inc=1, device_id={"dp": who}, device_id_type=MESH)
    if swaps:
        other = 1 - lax.axis_index("mp")
        pl.semaphore_signal(barrier, inc=1, device_id={"mp": other}, device_id_type=MESH)
    pl.semaphore_wait(barrier, 4 if swaps else 3)
    ends = []

    def begin(copy, end):
        copy.start()
        ends.append(end)
        return copy

    for i in range(swaps):
        copy = pltpu.make_async_remote_copy(
            src_ref=sends[i],
            dst_ref=gets[i],
            send_sem=swap_send.at[i],
            recv_sem=swap_recv.at[i],
            device_id={"mp": other},
            device_id_type=MESH,
        )
        begin(copy, copy.wait)
    for i in range(gathers):
        unit, cols = shards[i].shape[0], shards[i].shape[1] // 2
        own = fulls[i].at[span(device * unit, unit), :]
        for half, who in ((0, after * 2), (1, before * 2 + 1)):
            copy = remote(
                shards[i].at[:, pl.ds(half * cols, cols)],
                fulls[i].at[span(device * unit, unit), pl.ds(half * cols, cols)],
                give_sem.at[i, half],
                got_sem.at[i, core],
                who,
            )
            begin(copy, copy.wait_send)
        copy = remote(shards[i], own, lend_sem.at[i, 0], lent_sem.at[i, 0], partner)
        begin(copy, copy.wait)
        copy = pltpu.make_async_copy(shards[i], own, keep_sem.at[i])
        begin(copy, copy.wait)

    loads, pairs = {}, {}
    for step in range(chips):
        away = chip_at((spot + 2 * chips + way * (step + 1)) % chips, chips)
        here = chip_at((spot + 2 * chips - way * (step + 1)) % chips, chips)
        for i in range(scatters):
            rows, cols = mine[i].shape[1:]
            copy = remote(
                parts[i].at[span(away * rows, rows), span((1 - core) * cols, cols)],
                pair[i].at[step],
                pair_send.at[i, step],
                pair_recv.at[i, step],
                partner,
            )
            pairs[step, i] = begin(copy, copy.wait_send)
            loads[step, i] = pltpu.make_async_copy(
                parts[i].at[span(here * rows, rows), span(core * cols, cols)],
                mine[i].at[step],
                load_sem.at[i, step],
            )
            loads[step, i].start()

    def gather_step(i, step):
        held = chip_at((spot + 2 * chips - way * step) % chips, chips)
        unit, cols = shards[i].shape[0], shards[i].shape[1] // 2
        block = fulls[i].at[span(held * 2 * unit, 2 * unit), span(core * cols, cols)]
        if step == 1:
            for sender in range(2):
                piece = fulls[i].at[span((held * 2 + sender) * unit, unit), span(core * cols, cols)]
                remote(piece, piece, give_sem.at[i, 0], got_sem.at[i, sender], target).wait_recv()
        else:
            remote(block, block, give_sem.at[i, 0], got_sem.at[i, step], target).wait_recv()
        if step < chips - 1:
            copy = remote(block, block, give_sem.at[i, step + 1], got_sem.at[i, step + 1], target)
            begin(copy, copy.wait_send)
        copy = remote(block, block, lend_sem.at[i, step], lent_sem.at[i, step], partner)
        begin(copy, copy.wait)

    def scatter_step(i, step):
        rows, cols = mine[i].shape[1:]
        lines = min(rows, 32)
        loads[step, i].wait()
        pairs[step, i].wait_recv()
        if step > 0:
            came = ring[i].at[step - 1]
            remote(came, came, send_sem.at[i, 0], recv_sem.at[i, step - 1], target).wait_recv()

        @pl.loop(0, rows // lines)
        def _(k):
            at = span(k * lines, lines)
            total = mine[i][step, at, :].astype(jnp.float32)
            total = total + pair[i][step, at, :].astype(jnp.float32)
            if step > 0:
                total = total + ring[i][step - 1, at, :].astype(jnp.float32)
            if step < chips - 1:
                mine[i][step, at, :] = total.astype(jnp.bfloat16)
            else:
                last[i][at, :] = total

        if step < chips - 1:
            copy = remote(
                mine[i].at[step], ring[i].at[step], send_sem.at[i, step], recv_sem.at[i, step], target
            )
            begin(copy, copy.wait_send)
        else:
            unit = rows // 2
            place = outs[i].at[:, span(core * cols, cols)]
            copy = remote(
                last[i].at[span((1 - core) * unit, unit), :],
                place,
                last_send.at[i, 0],
                last_recv.at[i],
                partner,
            )
            begin(copy, copy.wait)
            copy = pltpu.make_async_copy(
                last[i].at[span(core * unit, unit), :], place, last_send.at[i, 1]
            )
            begin(copy, copy.wait)

    for step in range(chips):
        for i in range(gathers):
            if step > 0:
                gather_step(i, step)
        for i in range(scatters):
            scatter_step(i, step)
    for end in ends:
        end()


def ring_call(call_id, shards=(), sends=(), parts=(), groups=()):
    size = lax.axis_size("dp")
    chips = size // 2
    gathers, swaps, scatters = len(shards), len(sends), len(parts)
    outs = [jax.ShapeDtypeStruct((s.shape[0] * size, s.shape[1]), s.dtype) for s in shards]
    outs += [jax.ShapeDtypeStruct(s.shape, s.dtype) for s in sends]
    first = 0
    for group in groups:
        shape = (parts[first].shape[0] // size, parts[first].shape[1])
        outs.append(jax.ShapeDtypeStruct(shape if group == 1 else (group,) + shape, jnp.float32))
        first += group
    blocks = [(p.shape[0] // chips, p.shape[1] // 2) for p in parts]
    scratch = [pltpu.VMEM((chips,) + b, jnp.bfloat16) for b in blocks] * 2
    scratch += [pltpu.VMEM((chips - 1,) + b, jnp.bfloat16) for b in blocks]
    scratch += [pltpu.VMEM(b, jnp.float32) for b in blocks]
    if gathers:
        scratch += [pltpu.SemaphoreType.DMA((gathers,))]
        scratch += [pltpu.SemaphoreType.DMA((gathers, chips))] * 4
    if swaps:
        scratch += [pltpu.SemaphoreType.DMA((swaps,))] * 2
    if scatters:
        scratch += [pltpu.SemaphoreType.DMA((scatters, chips))] * 5
        scratch += [pltpu.SemaphoreType.DMA((scatters, 2)), pltpu.SemaphoreType.DMA((scatters,))]
    moved = sum(s.size * 2 * size for s in shards) + sum(p.size * 2 for p in parts)
    return list(
        pl.pallas_call(
            functools.partial(ring_kernel, chips, gathers, swaps, tuple(groups)),
            out_shape=outs,
            in_specs=[pl.BlockSpec(memory_space=pltpu.VMEM)] * gathers
            + [pl.BlockSpec(memory_space=pl.ANY)] * (swaps + scatters),
            out_specs=[pl.BlockSpec(memory_space=pl.ANY)] * len(outs),
            scratch_shapes=scratch,
            compiler_params=pltpu.CompilerParams(
                collective_id=call_id, has_side_effects=True, vmem_limit_bytes=VMEM_LIMIT
            ),
            cost_estimate=pl.CostEstimate(flops=0, bytes_accessed=moved, transcendentals=0),
        )(*shards, *sends, *parts)
    )


def layer_norm(values, norm_gain, norm_shift):
    center = values - jnp.mean(values, axis=-1, keepdims=True)
    inverse = lax.rsqrt(jnp.mean(center * center, axis=-1, keepdims=True) + EPS)
    scaled = center * inverse
    return (scaled * norm_gain + norm_shift, scaled, inverse)


def norm_back(grads, scaled, inverse, norm_gain):
    weighted = grads * norm_gain
    return inverse * (
        weighted
        - jnp.mean(weighted, axis=-1, keepdims=True)
        - scaled * jnp.mean(weighted * scaled, axis=-1, keepdims=True)
    )


def rotary_tables(segments, places, rotary_dims):
    earlier = (segments[None, :] < segments[:, None]).astype(jnp.int32)
    position = (places - jnp.sum(earlier, axis=1)).astype(jnp.float32)
    half_dims = rotary_dims // 2
    frequency = BASE ** (-2.0 * jnp.arange(half_dims, dtype=jnp.float32) / rotary_dims)
    angles = position[:, None] * frequency[None, :]
    return (jnp.cos(angles), jnp.sin(angles))


def rotate(values, cosine, sine_table, rotary_dims, turn_sign):
    half_dims = rotary_dims // 2
    leading = values[..., :half_dims]
    trailing = values[..., half_dims:rotary_dims]
    cos_rows = cosine[:, None, :]
    sin_rows = turn_sign * sine_table[:, None, :]
    return jnp.concatenate(
        [
            leading * cos_rows - trailing * sin_rows,
            trailing * cos_rows + leading * sin_rows,
            values[..., rotary_dims:],
        ],
        axis=-1,
    )


def masked_scores(query, key_rot, allowed, score_scale):
    scores = (
        jnp.einsum("qhd,khd->hqk", query, key_rot, preferred_element_type=jnp.float32) * score_scale
    )
    return jnp.where(allowed[None], scores, NEG)


def swap(values):
    return lax.ppermute(values, "mp", [(0, 1), (1, 0)])


def half_sum(part):
    half = part.shape[0] // 2
    other = swap(part[half:].astype(jnp.bfloat16))
    return part[:half] + other.astype(jnp.float32)


def grow(rows):
    return jnp.concatenate([rows, swap(rows)], axis=0)


def scatter(term, axis):
    return lax.psum_scatter(term, "dp", scatter_dimension=axis, tiled=True).astype(jnp.float32)


def body(
    inputs,
    segment_ids,
    norm1_gain,
    norm1_shift,
    qkv_weight,
    qkv_bias,
    out_weight,
    norm2_gain,
    norm2_shift,
    gate_weight,
    up_weight,
    down_weight,
    cotangent,
):
    score_scale = HEAD_DIM ** (-0.5)
    rows_here = inputs.shape[0]
    width = inputs.shape[1]
    *qkv_full, out_turned, far_inputs, far_cot = ring_call(
        0,
        shards=[qkv_weight[0], qkv_weight[1], qkv_weight[2], out_weight.T],
        sends=[inputs, cotangent],
    )
    input_rows = jnp.concatenate([inputs, far_inputs], axis=0)
    cot_rows = jnp.concatenate([cotangent, far_cot], axis=0)
    gate_full = lax.all_gather(gate_weight, "dp", axis=0, tiled=True)
    up_full = lax.all_gather(up_weight, "dp", axis=0, tiled=True)
    stream_rows = input_rows.astype(jnp.float32)
    stream = stream_rows[:rows_here]
    normed_wide, scaled_rows, inverse_rows = layer_norm(stream_rows, norm1_gain, norm1_shift)
    normed_one = normed_wide.astype(jnp.bfloat16)
    scaled_one = scaled_rows[:rows_here]
    inverse_one = inverse_rows[:rows_here]
    seq_len = normed_one.shape[0]
    local_width = qkv_full[0].shape[1]
    head_count = local_width // HEAD_DIM
    turn = lax.axis_index("mp") * rows_here
    segments = jnp.roll(segment_ids[0], -turn)
    places = jnp.roll(jnp.arange(seq_len, dtype=jnp.int32), -turn)
    allowed = (places[None, :] <= places[:, None]) & (segments[:, None] == segments[None, :])
    cosine, sine_table = rotary_tables(segments, places, ROT)
    shaped = [
        (jnp.dot(normed_one, full, preferred_element_type=jnp.float32) + bias).reshape(
            seq_len, head_count, HEAD_DIM
        )
        for full, bias in zip(qkv_full, qkv_bias)
    ]
    query = rotate(shaped[0], cosine, sine_table, ROT, 1.0).astype(jnp.bfloat16)
    key_rot = rotate(shaped[1], cosine, sine_table, ROT, 1.0).astype(jnp.bfloat16)
    value = shaped[2].astype(jnp.bfloat16)
    scores = masked_scores(query, key_rot, allowed, score_scale)
    row_max = jnp.max(scores, axis=-1, keepdims=True)
    exponent = jnp.exp(scores - row_max)
    row_total = jnp.sum(exponent, axis=-1, keepdims=True)
    log_total = row_max + jnp.log(row_total)
    probs_low = (exponent / row_total).astype(jnp.bfloat16)
    mixed_heads = jnp.einsum(
        "hqk,khd->qhd", probs_low, value, preferred_element_type=jnp.float32
    ).astype(jnp.bfloat16)
    mixed = mixed_heads.reshape(seq_len, local_width)
    branch = jnp.dot(mixed, out_turned.T, preferred_element_type=jnp.float32)
    middle = stream + half_sum(branch)
    normed_wide2, scaled_two, inverse_two = layer_norm(middle, norm2_gain, norm2_shift)
    normed_here = normed_wide2.astype(jnp.bfloat16)
    down_turned, normed_far = ring_call(1, shards=[down_weight.T], sends=[normed_here])
    normed_two = jnp.concatenate([normed_here, normed_far], axis=0)
    gate = jnp.dot(normed_two, gate_full, preferred_element_type=jnp.float32)
    upward = jnp.dot(normed_two, up_full, preferred_element_type=jnp.float32)
    sigma = jax.nn.sigmoid(gate)
    hidden = (gate * sigma * upward).astype(jnp.bfloat16)
    down_term = jnp.dot(cot_rows.T, hidden, preferred_element_type=jnp.float32)
    down_low, down_turned = lax.optimization_barrier((down_term.astype(jnp.bfloat16), down_turned))
    down_weight_grad = scatter(down_low, 0).T
    hidden_grad = jnp.dot(cot_rows, down_turned, preferred_element_type=jnp.float32)
    gate_act = (hidden_grad * upward * sigma * (1.0 + gate * (1.0 - sigma))).astype(jnp.bfloat16)
    up_act = (hidden_grad * gate * sigma).astype(jnp.bfloat16)
    normed_part = jnp.dot(gate_act, gate_full.T, preferred_element_type=jnp.float32) + jnp.dot(
        up_act, up_full.T, preferred_element_type=jnp.float32
    )
    part_low, gate_act, up_act = lax.optimization_barrier(
        (normed_part[rows_here:].astype(jnp.bfloat16), gate_act, up_act)
    )
    normed_two_grad = normed_part[:rows_here] + swap(part_low).astype(jnp.float32)
    gate_term = jnp.dot(normed_two.T, gate_act, preferred_element_type=jnp.float32)
    up_term = jnp.dot(normed_two.T, up_act, preferred_element_type=jnp.float32)
    gate_weight_grad = scatter(gate_term.astype(jnp.bfloat16), 0)
    gain_two = jnp.sum(normed_two_grad * scaled_two, axis=0)
    shift_two = jnp.sum(normed_two_grad, axis=0)
    middle_grad = cotangent.astype(jnp.float32) + norm_back(
        normed_two_grad, scaled_two, inverse_two, norm2_gain
    )
    middle_low, hidden = lax.optimization_barrier((middle_grad.astype(jnp.bfloat16), hidden))
    middle_rows = grow(middle_low)
    feed_part = jnp.dot(hidden, down_turned.T, preferred_element_type=jnp.float32)
    out_term = jnp.dot(middle_rows.T, mixed, preferred_element_type=jnp.float32)
    mixed_grad = (
        jnp.dot(middle_rows, out_turned, preferred_element_type=jnp.float32)
        .astype(jnp.bfloat16)
        .reshape(seq_len, head_count, HEAD_DIM)
    )
    probs_wide = jnp.exp(scores - log_total)
    value_grad = jnp.einsum(
        "hqk,qhd->khd",
        probs_wide.astype(jnp.bfloat16),
        mixed_grad,
        preferred_element_type=jnp.float32,
    )
    prob_grad = jnp.einsum("qhd,khd->hqk", mixed_grad, value, preferred_element_type=jnp.float32)
    row_delta = jnp.transpose(
        jnp.sum(mixed_grad.astype(jnp.float32) * mixed_heads.astype(jnp.float32), axis=-1)
    )
    score_grad = (probs_wide * (prob_grad - row_delta[:, :, None]) * score_scale).astype(
        jnp.bfloat16
    )
    query_grad = jnp.einsum("hqk,khd->qhd", score_grad, key_rot, preferred_element_type=jnp.float32)
    key_grad = jnp.einsum("hqk,qhd->khd", score_grad, query, preferred_element_type=jnp.float32)
    query_back = rotate(query_grad, cosine, sine_table, ROT, -1.0)
    key_back = rotate(key_grad, cosine, sine_table, ROT, -1.0)
    proj_grad = [
        part.reshape(seq_len, local_width) for part in (query_back, key_back, value_grad)
    ]
    rotated_cols = jnp.arange(local_width, dtype=jnp.int32) % HEAD_DIM < ROT
    bias_sums = [jnp.sum(part, axis=0) for part in proj_grad]
    bias_term = [bias_sums[0], jnp.where(rotated_cols, bias_sums[1], 0.0), bias_sums[2]]
    proj_low = [part.astype(jnp.bfloat16) for part in proj_grad]
    normed_one_part = jnp.zeros((), jnp.float32)
    for part, full in zip(proj_low, qkv_full):
        normed_one_part = normed_one_part + jnp.dot(
            part, full.T, preferred_element_type=jnp.float32
        )
    gain_one = jnp.sum(normed_one_part * scaled_rows, axis=0)
    shift_one = jnp.sum(normed_one_part, axis=0)
    norm_sums = jnp.concatenate([gain_one, shift_one, gain_two, shift_two])
    norm_sums = norm_sums + swap(norm_sums)
    sums = jnp.concatenate([norm_sums] + bias_term)
    spare = -sums.size % (8 * 256)
    qkv_term = [
        jnp.dot(normed_one.T, part, preferred_element_type=jnp.float32) for part in proj_low
    ]
    all_sums, far_part, far_feed, up_weight_grad, out_grad_turned, qkv_weight_grad = ring_call(
        2,
        shards=[jnp.pad(sums, (0, spare)).reshape(8, -1)],
        sends=[part[rows_here:].astype(jnp.bfloat16) for part in (normed_one_part, feed_part)],
        parts=[term.astype(jnp.bfloat16) for term in [up_term, out_term] + qkv_term],
        groups=[1, 1, 3],
    )
    out_weight_grad = out_grad_turned.T
    normed_one_grad = normed_one_part[:rows_here] + far_part.astype(jnp.float32)
    feed = feed_part[:rows_here] + far_feed.astype(jnp.float32)
    output = (middle + feed).astype(jnp.bfloat16)
    all_sums = jnp.sum(all_sums.reshape(-1, 8, all_sums.shape[1]), axis=0).reshape(-1)
    gain_one, shift_one, gain_two, shift_two = all_sums[: 4 * width].reshape(4, width)
    qkv_bias_grad = all_sums[4 * width : sums.size].reshape(3, local_width)
    input_grad = middle_grad + norm_back(normed_one_grad, scaled_one, inverse_one, norm1_gain)
    return (
        output,
        input_grad,
        gain_one,
        shift_one,
        qkv_weight_grad,
        qkv_bias_grad,
        out_weight_grad,
        gain_two,
        shift_two,
        gate_weight_grad,
        up_weight_grad,
        down_weight_grad,
    )


def solution(mesh):
    in_specs = (
        P(("dp", "mp"), None),
        P("dp", None),
        P(),
        P(),
        P(None, "dp", "mp"),
        P(None, "mp"),
        P("mp", "dp"),
        P(),
        P(),
        P("dp", "mp"),
        P("dp", "mp"),
        P("mp", "dp"),
        P(("dp", "mp"), None),
    )
    out_specs = (
        P(("dp", "mp"), None),
        P(("dp", "mp"), None),
        P(),
        P(),
        P(None, "dp", "mp"),
        P(None, "mp"),
        P("mp", "dp"),
        P(),
        P(),
        P("dp", "mp"),
        P("dp", "mp"),
        P("mp", "dp"),
    )
    return jax.shard_map(body, mesh=mesh, in_specs=in_specs, out_specs=out_specs, check_vma=False)
```

```python
import functools

import jax
import jax.numpy as jnp
from jax import lax
from jax.experimental import pallas as pl
from jax.experimental.pallas import tpu as pltpu
from jax.sharding import PartitionSpec as P

HEAD_DIM = 64
ROT = 16


NEG = -1e30
EPS = 1e-05
BASE = 10000.0

MESH = pl.DeviceIdType.MESH
VMEM_LIMIT = 60 * 1024 * 1024


def chip_at(spot, chips):
    side = spot // (chips // 2)
    return (spot + side * (chips - 1 - 2 * spot)) * 2 + side


def span(start, size):
    return pl.ds(pl.multiple_of(start, size), size)


def remote(src, dst, send, recv, who):
    return pltpu.make_async_remote_copy(
        src_ref=src,
        dst_ref=dst,
        send_sem=send,
        recv_sem=recv,
        device_id={"dp": who},
        device_id_type=MESH,
    )


def ring_kernel(chips, gathers, swaps, groups, *refs):
    refs = list(refs)
    scatters = sum(groups)

    def take(number):
        taken = refs[:number]
        del refs[:number]
        return taken

    shards, sends, parts = take(gathers), take(swaps), take(scatters)
    fulls, gets, grouped = take(gathers), take(swaps), take(len(groups))
    outs = []
    for group, out in zip(groups, grouped):
        outs += [out] if group == 1 else [out.at[j] for j in range(group)]
    mine, pair, ring, last = take(scatters), take(scatters), take(scatters), take(scatters)
    if gathers:
        keep_sem, give_sem, got_sem, lend_sem, lent_sem = take(5)
    if swaps:
        swap_send, swap_recv = take(2)
    if scatters:
        load_sem, pair_send, pair_recv, send_sem, recv_sem, last_send, last_recv = take(7)
    device = lax.axis_index("dp")
    chip, core = device // 2, device % 2
    row, side = chip // 2, chip % 2
    spot, way = row + side * (chips - 1 - 2 * row), 1 - 2 * core
    partner = device + way
    after = chip_at((spot + 1) % chips, chips)
    before = chip_at((spot + chips - 1) % chips, chips)
    source = chip_at((spot + chips - way) % chips, chips)
    target = chip_at((spot + chips + way) % chips, chips) * 2 + core
    barrier = pltpu.get_barrier_semaphore()
    for who in (source * 2, source * 2 + 1, partner):
        pl.semaphore_signal(barrier, inc=1, device_id={"dp": who}, device_id_type=MESH)
    if swaps:
        other = 1 - lax.axis_index("mp")
        pl.semaphore_signal(barrier, inc=1, device_id={"mp": other}, device_id_type=MESH)
    pl.semaphore_wait(barrier, 4 if swaps else 3)
    ends = []

    def begin(copy, end):
        copy.start()
        ends.append(end)
        return copy

    for i in range(swaps):
        copy = pltpu.make_async_remote_copy(
            src_ref=sends[i],
            dst_ref=gets[i],
            send_sem=swap_send.at[i],
            recv_sem=swap_recv.at[i],
            device_id={"mp": other},
            device_id_type=MESH,
        )
        begin(copy, copy.wait)
    for i in range(gathers):
        unit, cols = shards[i].shape[0], shards[i].shape[1] // 2
        own = fulls[i].at[span(device * unit, unit), :]
        for half, who in ((0, after * 2), (1, before * 2 + 1)):
            copy = remote(
                shards[i].at[:, pl.ds(half * cols, cols)],
                fulls[i].at[span(device * unit, unit), pl.ds(half * cols, cols)],
                give_sem.at[i, half],
                got_sem.at[i, core],
                who,
            )
            begin(copy, copy.wait_send)
        copy = remote(shards[i], own, lend_sem.at[i, 0], lent_sem.at[i, 0], partner)
        begin(copy, copy.wait)
        copy = pltpu.make_async_copy(shards[i], own, keep_sem.at[i])
        begin(copy, copy.wait)

    loads, pairs = {}, {}
    for step in range(chips):
        away = chip_at((spot + 2 * chips + way * (step + 1)) % chips, chips)
        here = chip_at((spot + 2 * chips - way * (step + 1)) % chips, chips)
        for i in range(scatters):
            rows, cols = mine[i].shape[1:]
            copy = remote(
                parts[i].at[span(away * rows, rows), span((1 - core) * cols, cols)],
                pair[i].at[step],
                pair_send.at[i, step],
                pair_recv.at[i, step],
                partner,
            )
            pairs[step, i] = begin(copy, copy.wait_send)
            loads[step, i] = pltpu.make_async_copy(
                parts[i].at[span(here * rows, rows), span(core * cols, cols)],
                mine[i].at[step],
                load_sem.at[i, step],
            )
            loads[step, i].start()

    def gather_step(i, step):
        held = chip_at((spot + 2 * chips - way * step) % chips, chips)
        unit, cols = shards[i].shape[0], shards[i].shape[1] // 2
        block = fulls[i].at[span(held * 2 * unit, 2 * unit), span(core * cols, cols)]
        if step == 1:
            for sender in range(2):
                piece = fulls[i].at[span((held * 2 + sender) * unit, unit), span(core * cols, cols)]
                remote(piece, piece, give_sem.at[i, 0], got_sem.at[i, sender], target).wait_recv()
        else:
            remote(block, block, give_sem.at[i, 0], got_sem.at[i, step], target).wait_recv()
        if step < chips - 1:
            copy = remote(block, block, give_sem.at[i, step + 1], got_sem.at[i, step + 1], target)
            begin(copy, copy.wait_send)
        copy = remote(block, block, lend_sem.at[i, step], lent_sem.at[i, step], partner)
        begin(copy, copy.wait)

    def scatter_step(i, step):
        rows, cols = mine[i].shape[1:]
        lines = min(rows, 32)
        loads[step, i].wait()
        pairs[step, i].wait_recv()
        if step > 0:
            came = ring[i].at[step - 1]
            remote(came, came, send_sem.at[i, 0], recv_sem.at[i, step - 1], target).wait_recv()

        @pl.loop(0, rows // lines)
        def _(k):
            at = span(k * lines, lines)
            total = mine[i][step, at, :].astype(jnp.float32)
            total = total + pair[i][step, at, :].astype(jnp.float32)
            if step > 0:
                total = total + ring[i][step - 1, at, :].astype(jnp.float32)
            if step < chips - 1:
                mine[i][step, at, :] = total.astype(jnp.bfloat16)
            else:
                last[i][at, :] = total

        if step < chips - 1:
            copy = remote(
                mine[i].at[step], ring[i].at[step], send_sem.at[i, step], recv_sem.at[i, step], target
            )
            begin(copy, copy.wait_send)
        else:
            unit = rows // 2
            place = outs[i].at[:, span(core * cols, cols)]
            copy = remote(
                last[i].at[span((1 - core) * unit, unit), :],
                place,
                last_send.at[i, 0],
                last_recv.at[i],
                partner,
            )
            begin(copy, copy.wait)
            copy = pltpu.make_async_copy(
                last[i].at[span(core * unit, unit), :], place, last_send.at[i, 1]
            )
            begin(copy, copy.wait)

    for step in range(chips):
        for i in range(gathers):
            if step > 0:
                gather_step(i, step)
        for i in range(scatters):
            scatter_step(i, step)
    for end in ends:
        end()


def ring_call(call_id, shards=(), sends=(), parts=(), groups=()):
    size = lax.axis_size("dp")
    chips = size // 2
    gathers, swaps, scatters = len(shards), len(sends), len(parts)
    outs = [jax.ShapeDtypeStruct((s.shape[0] * size, s.shape[1]), s.dtype) for s in shards]
    outs += [jax.ShapeDtypeStruct(s.shape, s.dtype) for s in sends]
    first = 0
    for group in groups:
        shape = (parts[first].shape[0] // size, parts[first].shape[1])
        outs.append(jax.ShapeDtypeStruct(shape if group == 1 else (group,) + shape, jnp.float32))
        first += group
    blocks = [(p.shape[0] // chips, p.shape[1] // 2) for p in parts]
    scratch = [pltpu.VMEM((chips,) + b, jnp.bfloat16) for b in blocks] * 2
    scratch += [pltpu.VMEM((chips - 1,) + b, jnp.bfloat16) for b in blocks]
    scratch += [pltpu.VMEM(b, jnp.float32) for b in blocks]
    if gathers:
        scratch += [pltpu.SemaphoreType.DMA((gathers,))]
        scratch += [pltpu.SemaphoreType.DMA((gathers, chips))] * 4
    if swaps:
        scratch += [pltpu.SemaphoreType.DMA((swaps,))] * 2
    if scatters:
        scratch += [pltpu.SemaphoreType.DMA((scatters, chips))] * 5
        scratch += [pltpu.SemaphoreType.DMA((scatters, 2)), pltpu.SemaphoreType.DMA((scatters,))]
    moved = sum(s.size * 2 * size for s in shards) + sum(p.size * 2 for p in parts)
    return list(
        pl.pallas_call(
            functools.partial(ring_kernel, chips, gathers, swaps, tuple(groups)),
            out_shape=outs,
            in_specs=[pl.BlockSpec(memory_space=pltpu.VMEM)] * gathers
            + [pl.BlockSpec(memory_space=pl.ANY)] * (swaps + scatters),
            out_specs=[pl.BlockSpec(memory_space=pl.ANY)] * len(outs),
            scratch_shapes=scratch,
            compiler_params=pltpu.CompilerParams(
                collective_id=call_id, has_side_effects=True, vmem_limit_bytes=VMEM_LIMIT
            ),
            cost_estimate=pl.CostEstimate(flops=0, bytes_accessed=moved, transcendentals=0),
        )(*shards, *sends, *parts)
    )


def feed_kernel(
    chips,
    tile,
    up_shard,
    down_shard,
    normed_ref,
    cot_ref,
    gate_full,
    up_full,
    down_full,
    rows_out,
    gate_out,
    up_out,
    hidden_out,
    term_out,
    rows,
    weights,
    gates,
    ups,
    hiddens,
    terms,
    keep_sem,
    give_sem,
    got_sem,
    lend_sem,
    lent_sem,
    swap_sem,
    load_sem,
    gate_sem,
    up_sem,
    hidden_sem,
    term_sem,
):
    device = lax.axis_index("dp")
    chip, core = device // 2, device % 2
    row, side = chip // 2, chip % 2
    spot, way = row + side * (chips - 1 - 2 * row), 1 - 2 * core
    partner = device + way
    after = chip_at((spot + 1) % chips, chips)
    before = chip_at((spot + chips - 1) % chips, chips)
    source = chip_at((spot + chips - way) % chips, chips)
    target = chip_at((spot + chips + way) % chips, chips) * 2 + core
    other = 1 - lax.axis_index("mp")
    barrier = pltpu.get_barrier_semaphore()
    for who in (source * 2, source * 2 + 1, partner):
        pl.semaphore_signal(barrier, inc=1, device_id={"dp": who}, device_id_type=MESH)
    pl.semaphore_signal(barrier, inc=1, device_id={"mp": other}, device_id_type=MESH)
    pl.semaphore_wait(barrier, 4)

    unit, wide = up_shard.shape
    tiles = wide // tile
    first = (wide // 256 + 1) // 2 * 256
    columns = (pl.ds(0, first), pl.ds(first, wide - first))
    shards = [ref.at[:, at] for ref in (up_shard, down_shard) for at in columns]
    fulls = [ref.at[:, at] for ref in (up_full, down_full) for at in columns]
    halves = [first // 2, (wide - first) // 2] * 2
    half_rows = normed_ref.shape[0]

    def own(i, half):
        at = slice(None) if half is None else pl.ds(half * halves[i], halves[i])
        return shards[i].at[:, at], fulls[i].at[span(device * unit, unit), at]

    def sent(i):
        copies = []
        for half, who in ((0, after * 2), (1, before * 2 + 1)):
            src, dst = own(i, half)
            copies.append(remote(src, dst, give_sem.at[i, half], got_sem.at[i, 1], who))
        return copies

    def shared(i):
        src, dst = own(i, None)
        return [
            remote(src, dst, lend_sem.at[i, 0], lent_sem.at[i, 0], partner),
            pltpu.make_async_copy(src, dst, keep_sem.at[i]),
        ]

    def block(i, step):
        held = chip_at((spot + 2 * chips - way * step) % chips, chips)
        return fulls[i].at[span(held * 2 * unit, 2 * unit), span(core * halves[i], halves[i])]

    def passed(i, step):
        at = block(i, step)
        return remote(at, at, give_sem.at[i, step + 1], got_sem.at[i, step + 1], target)

    def lent(i, step):
        at = block(i, step)
        return remote(at, at, lend_sem.at[i, step], lent_sem.at[i, step], partner)

    def relay(i, step):
        at = block(i, step)
        remote(at, at, give_sem.at[i, 0], got_sem.at[i, step], target).wait_recv()

        @pl.when(step < chips - 1)
        def _():
            passed(i, step).start()

        lent(i, step).start()

    def settle(i):
        for copy in shared(i):
            copy.wait()
        for copy in sent(i):
            copy.wait_send()

        @pl.loop(1, chips)
        def _(step):
            lent(i, step).wait()

            @pl.when(step < chips - 1)
            def _():
                passed(i, step).wait_send()

    exchange = pltpu.make_async_remote_copy(
        src_ref=normed_ref,
        dst_ref=rows.at[pl.ds(half_rows, half_rows), :],
        send_sem=swap_sem.at[0],
        recv_sem=swap_sem.at[1],
        device_id={"mp": other},
        device_id_type=MESH,
    )
    place = pltpu.make_async_copy(normed_ref, rows.at[pl.ds(0, half_rows), :], swap_sem.at[2])
    record = pltpu.make_async_copy(rows, rows_out, swap_sem.at[3])

    def load(ref, t):
        return pltpu.make_async_copy(
            ref.at[:, span(t * tile, tile)], weights.at[t % 2], load_sem.at[t % 2]
        )

    def store(buffer, out, sem, t):
        at = span(t * tile, tile)
        return pltpu.make_async_copy(buffer.at[:, at], out.at[:, at], sem.at[t])

    def store_term(t):
        return pltpu.make_async_copy(
            terms.at[t % 2], term_out.at[:, span(t * tile, tile)], term_sem.at[t % 2]
        )

    def weight_of(ref, t):
        load(ref, t).wait()

        @pl.when(t + 1 < tiles)
        def _():
            load(ref, t + 1).start()

        return weights[t % 2]

    def gate_tile(t):
        gates[:, span(t * tile, tile)] = jnp.dot(
            rows[...], weight_of(gate_full, t), preferred_element_type=jnp.float32
        )
        store(gates, gate_out, gate_sem, t).start()

    def up_tile(t):
        at = span(t * tile, tile)
        upward = jnp.dot(rows[...], weight_of(up_full, t), preferred_element_type=jnp.float32)
        ups[:, at] = upward
        store(ups, up_out, up_sem, t).start()
        gate = gates[:, at]
        hidden = (gate * jax.nn.sigmoid(gate) * upward).astype(jnp.bfloat16)
        hiddens[:, at] = hidden
        store(hiddens, hidden_out, hidden_sem, t).start()

        @pl.when(t > 1)
        def _():
            store_term(t - 2).wait()

        terms[t % 2] = jnp.dot(
            cot_ref[...], hidden, preferred_element_type=jnp.float32
        ).astype(jnp.bfloat16)
        store_term(t).start()

    def some(number, start, work):
        @pl.loop(0, number)
        def _(k):
            @pl.when(start + k < tiles)
            def _():
                work(start + k)

    for i in (0, 1):
        for copy in sent(i) + shared(i):
            copy.start()
    exchange.start()
    place.start()
    load(gate_full, 0).start()
    late = chips // 2
    each = -(-tiles // (chips - late))

    @pl.loop(1, chips)
    def _(step):
        relay(0, step)
        relay(1, step)

        @pl.when(step == chips - 2)
        def _():
            for i in (2, 3):
                for copy in sent(i) + shared(i):
                    copy.start()

        @pl.when(step == late)
        def _():
            place.wait()
            exchange.wait()
            record.start()

        @pl.when(step >= late)
        def _():
            some(each, (step - late) * each, gate_tile)

    settle(0)
    settle(1)
    load(up_full, 0).start()
    each = -(-tiles // (chips - 1))
    early = -(-each // 2)

    @pl.loop(1, chips)
    def _(step):
        relay(2, step)
        some(early, (step - 1) * each, up_tile)
        relay(3, step)
        if each > early:
            some(each - early, (step - 1) * each + early, up_tile)

    settle(2)
    settle(3)
    record.wait()

    @pl.loop(0, tiles)
    def _(t):
        store(gates, gate_out, gate_sem, t).wait()
        store(ups, up_out, up_sem, t).wait()
        store(hiddens, hidden_out, hidden_sem, t).wait()

    for t in range(max(tiles - 2, 0), tiles):
        store_term(t).wait()


def feed_call(call_id, up_shard, down_shard, normed_here, cot_turned, gate_full):
    size = lax.axis_size("dp")
    chips = size // 2
    unit, wide = up_shard.shape
    depth, tokens = cot_turned.shape
    tile = 256
    tiles = wide // tile
    low, high = jnp.bfloat16, jnp.float32
    kept = pl.BlockSpec(memory_space=pltpu.VMEM)
    far = pl.BlockSpec(memory_space=pl.ANY)
    dma = pltpu.SemaphoreType.DMA
    return pl.pallas_call(
        functools.partial(feed_kernel, chips, tile),
        out_shape=[
            jax.ShapeDtypeStruct((depth, wide), low),
            jax.ShapeDtypeStruct((depth, wide), low),
            jax.ShapeDtypeStruct((tokens, depth), low),
            jax.ShapeDtypeStruct((tokens, wide), high),
            jax.ShapeDtypeStruct((tokens, wide), high),
            jax.ShapeDtypeStruct((tokens, wide), low),
            jax.ShapeDtypeStruct((depth, wide), low),
        ],
        in_specs=[kept, kept, kept, kept, far],
        out_specs=[far] * 7,
        scratch_shapes=[
            pltpu.VMEM((tokens, depth), low),
            pltpu.VMEM((2, depth, tile), low),
            pltpu.VMEM((tokens, wide), high),
            pltpu.VMEM((tokens, wide), high),
            pltpu.VMEM((tokens, wide), low),
            pltpu.VMEM((2, depth, tile), low),
            dma((4,)),
        ]
        + [dma((4, chips + 1))] * 4
        + [dma((4,)), dma((2,)), dma((tiles,)), dma((tiles,)), dma((tiles,)), dma((2,))],
        compiler_params=pltpu.CompilerParams(
            collective_id=call_id, has_side_effects=True, vmem_limit_bytes=VMEM_LIMIT
        ),
        cost_estimate=pl.CostEstimate(
            flops=6 * tokens * depth * wide,
            bytes_accessed=12 * depth * wide + 12 * tokens * wide,
            transcendentals=tokens * wide,
        ),
    )(up_shard, down_shard, normed_here, cot_turned, gate_full)


def layer_norm(values, norm_gain, norm_shift):
    center = values - jnp.mean(values, axis=-1, keepdims=True)
    inverse = lax.rsqrt(jnp.mean(center * center, axis=-1, keepdims=True) + EPS)
    scaled = center * inverse
    return (scaled * norm_gain + norm_shift, scaled, inverse)


def norm_back(grads, scaled, inverse, norm_gain):
    weighted = grads * norm_gain
    return inverse * (
        weighted
        - jnp.mean(weighted, axis=-1, keepdims=True)
        - scaled * jnp.mean(weighted * scaled, axis=-1, keepdims=True)
    )


def rotary_tables(segments, places, rotary_dims):
    earlier = (segments[None, :] < segments[:, None]).astype(jnp.int32)
    position = (places - jnp.sum(earlier, axis=1)).astype(jnp.float32)
    half_dims = rotary_dims // 2
    frequency = BASE ** (-2.0 * jnp.arange(half_dims, dtype=jnp.float32) / rotary_dims)
    angles = position[:, None] * frequency[None, :]
    return (jnp.cos(angles), jnp.sin(angles))


def rotate(values, cosine, sine_table, rotary_dims, turn_sign):
    half_dims = rotary_dims // 2
    leading = values[..., :half_dims]
    trailing = values[..., half_dims:rotary_dims]
    cos_rows = cosine[:, None, :]
    sin_rows = turn_sign * sine_table[:, None, :]
    return jnp.concatenate(
        [
            leading * cos_rows - trailing * sin_rows,
            trailing * cos_rows + leading * sin_rows,
            values[..., rotary_dims:],
        ],
        axis=-1,
    )


def masked_scores(query, key_rot, allowed, score_scale):
    scores = (
        jnp.einsum("qhd,khd->hqk", query, key_rot, preferred_element_type=jnp.float32) * score_scale
    )
    return jnp.where(allowed[None], scores, NEG)


def swap(values):
    return lax.ppermute(values, "mp", [(0, 1), (1, 0)])


def half_sum(part):
    half = part.shape[0] // 2
    other = swap(part[half:].astype(jnp.bfloat16))
    return part[:half] + other.astype(jnp.float32)


def grow(rows):
    return jnp.concatenate([rows, swap(rows)], axis=0)


def scatter(term, axis):
    return lax.psum_scatter(term, "dp", scatter_dimension=axis, tiled=True).astype(jnp.float32)


def body(
    inputs,
    segment_ids,
    norm1_gain,
    norm1_shift,
    qkv_weight,
    qkv_bias,
    out_weight,
    norm2_gain,
    norm2_shift,
    gate_weight,
    up_weight,
    down_weight,
    cotangent,
):
    score_scale = HEAD_DIM ** (-0.5)
    rows_here = inputs.shape[0]
    width = inputs.shape[1]
    *qkv_full, out_turned, far_inputs, far_cot = ring_call(
        0,
        shards=[qkv_weight[0], qkv_weight[1], qkv_weight[2], out_weight.T],
        sends=[inputs, cotangent],
    )
    input_rows = jnp.concatenate([inputs, far_inputs], axis=0)
    cot_rows = jnp.concatenate([cotangent, far_cot], axis=0)
    gate_weight, out_turned = lax.optimization_barrier((gate_weight, out_turned))
    gate_full = lax.all_gather(gate_weight, "dp", axis=0, tiled=True)
    stream_rows = input_rows.astype(jnp.float32)
    stream = stream_rows[:rows_here]
    normed_wide, scaled_rows, inverse_rows = layer_norm(stream_rows, norm1_gain, norm1_shift)
    normed_one = normed_wide.astype(jnp.bfloat16)
    scaled_one = scaled_rows[:rows_here]
    inverse_one = inverse_rows[:rows_here]
    seq_len = normed_one.shape[0]
    local_width = qkv_full[0].shape[1]
    head_count = local_width // HEAD_DIM
    turn = lax.axis_index("mp") * rows_here
    segments = jnp.roll(segment_ids[0], -turn)
    places = jnp.roll(jnp.arange(seq_len, dtype=jnp.int32), -turn)
    allowed = (places[None, :] <= places[:, None]) & (segments[:, None] == segments[None, :])
    cosine, sine_table = rotary_tables(segments, places, ROT)
    shaped = [
        (jnp.dot(normed_one, full, preferred_element_type=jnp.float32) + bias).reshape(
            seq_len, head_count, HEAD_DIM
        )
        for full, bias in zip(qkv_full, qkv_bias)
    ]
    query = rotate(shaped[0], cosine, sine_table, ROT, 1.0).astype(jnp.bfloat16)
    key_rot = rotate(shaped[1], cosine, sine_table, ROT, 1.0).astype(jnp.bfloat16)
    value = shaped[2].astype(jnp.bfloat16)
    scores = masked_scores(query, key_rot, allowed, score_scale)
    row_max = jnp.max(scores, axis=-1, keepdims=True)
    exponent = jnp.exp(scores - row_max)
    row_total = jnp.sum(exponent, axis=-1, keepdims=True)
    log_total = row_max + jnp.log(row_total)
    probs_low = (exponent / row_total).astype(jnp.bfloat16)
    mixed_heads = jnp.einsum(
        "hqk,khd->qhd", probs_low, value, preferred_element_type=jnp.float32
    ).astype(jnp.bfloat16)
    mixed = mixed_heads.reshape(seq_len, local_width)
    branch = jnp.dot(mixed, out_turned.T, preferred_element_type=jnp.float32)
    middle = stream + half_sum(branch)
    normed_wide2, scaled_two, inverse_two = layer_norm(middle, norm2_gain, norm2_shift)
    normed_here = normed_wide2.astype(jnp.bfloat16)
    up_full, down_turned, normed_two, gate, upward, hidden, down_term = feed_call(
        1, up_weight, down_weight.T, normed_here, cot_rows.T, gate_full
    )
    sigma = jax.nn.sigmoid(gate)
    down_weight_grad = scatter(down_term, 0).T
    hidden_grad = jnp.dot(cot_rows, down_turned, preferred_element_type=jnp.float32)
    gate_act = (hidden_grad * upward * sigma * (1.0 + gate * (1.0 - sigma))).astype(jnp.bfloat16)
    up_act = (hidden_grad * gate * sigma).astype(jnp.bfloat16)
    normed_part = jnp.dot(gate_act, gate_full.T, preferred_element_type=jnp.float32) + jnp.dot(
        up_act, up_full.T, preferred_element_type=jnp.float32
    )
    part_low, gate_act, up_act = lax.optimization_barrier(
        (normed_part[rows_here:].astype(jnp.bfloat16), gate_act, up_act)
    )
    normed_two_grad = normed_part[:rows_here] + swap(part_low).astype(jnp.float32)
    gate_term = jnp.dot(normed_two.T, gate_act, preferred_element_type=jnp.float32)
    up_term = jnp.dot(normed_two.T, up_act, preferred_element_type=jnp.float32)
    gate_weight_grad = scatter(gate_term.astype(jnp.bfloat16), 0)
    gain_two = jnp.sum(normed_two_grad * scaled_two, axis=0)
    shift_two = jnp.sum(normed_two_grad, axis=0)
    middle_grad = cotangent.astype(jnp.float32) + norm_back(
        normed_two_grad, scaled_two, inverse_two, norm2_gain
    )
    middle_low, hidden = lax.optimization_barrier((middle_grad.astype(jnp.bfloat16), hidden))
    middle_rows = grow(middle_low)
    feed_part = jnp.dot(hidden, down_turned.T, preferred_element_type=jnp.float32)
    out_term = jnp.dot(middle_rows.T, mixed, preferred_element_type=jnp.float32)
    mixed_grad = (
        jnp.dot(middle_rows, out_turned, preferred_element_type=jnp.float32)
        .astype(jnp.bfloat16)
        .reshape(seq_len, head_count, HEAD_DIM)
    )
    probs_wide = jnp.exp(scores - log_total)
    value_grad = jnp.einsum(
        "hqk,qhd->khd",
        probs_wide.astype(jnp.bfloat16),
        mixed_grad,
        preferred_element_type=jnp.float32,
    )
    prob_grad = jnp.einsum("qhd,khd->hqk", mixed_grad, value, preferred_element_type=jnp.float32)
    row_delta = jnp.transpose(
        jnp.sum(mixed_grad.astype(jnp.float32) * mixed_heads.astype(jnp.float32), axis=-1)
    )
    score_grad = (probs_wide * (prob_grad - row_delta[:, :, None]) * score_scale).astype(
        jnp.bfloat16
    )
    query_grad = jnp.einsum("hqk,khd->qhd", score_grad, key_rot, preferred_element_type=jnp.float32)
    key_grad = jnp.einsum("hqk,qhd->khd", score_grad, query, preferred_element_type=jnp.float32)
    query_back = rotate(query_grad, cosine, sine_table, ROT, -1.0)
    key_back = rotate(key_grad, cosine, sine_table, ROT, -1.0)
    proj_grad = [
        part.reshape(seq_len, local_width) for part in (query_back, key_back, value_grad)
    ]
    rotated_cols = jnp.arange(local_width, dtype=jnp.int32) % HEAD_DIM < ROT
    bias_sums = [jnp.sum(part, axis=0) for part in proj_grad]
    bias_term = [bias_sums[0], jnp.where(rotated_cols, bias_sums[1], 0.0), bias_sums[2]]
    proj_low = [part.astype(jnp.bfloat16) for part in proj_grad]
    normed_one_part = jnp.zeros((), jnp.float32)
    for part, full in zip(proj_low, qkv_full):
        normed_one_part = normed_one_part + jnp.dot(
            part, full.T, preferred_element_type=jnp.float32
        )
    gain_one = jnp.sum(normed_one_part * scaled_rows, axis=0)
    shift_one = jnp.sum(normed_one_part, axis=0)
    norm_sums = jnp.concatenate([gain_one, shift_one, gain_two, shift_two])
    norm_sums = norm_sums + swap(norm_sums)
    sums = jnp.concatenate([norm_sums] + bias_term)
    spare = -sums.size % (8 * 256)
    qkv_term = [
        jnp.dot(normed_one.T, part, preferred_element_type=jnp.float32) for part in proj_low
    ]
    all_sums, far_part, far_feed, up_weight_grad, out_grad_turned, qkv_weight_grad = ring_call(
        2,
        shards=[jnp.pad(sums, (0, spare)).reshape(8, -1)],
        sends=[part[rows_here:].astype(jnp.bfloat16) for part in (normed_one_part, feed_part)],
        parts=[term.astype(jnp.bfloat16) for term in [up_term, out_term] + qkv_term],
        groups=[1, 1, 3],
    )
    out_weight_grad = out_grad_turned.T
    normed_one_grad = normed_one_part[:rows_here] + far_part.astype(jnp.float32)
    feed = feed_part[:rows_here] + far_feed.astype(jnp.float32)
    output = (middle + feed).astype(jnp.bfloat16)
    all_sums = jnp.sum(all_sums.reshape(-1, 8, all_sums.shape[1]), axis=0).reshape(-1)
    gain_one, shift_one, gain_two, shift_two = all_sums[: 4 * width].reshape(4, width)
    qkv_bias_grad = all_sums[4 * width : sums.size].reshape(3, local_width)
    input_grad = middle_grad + norm_back(normed_one_grad, scaled_one, inverse_one, norm1_gain)
    return (
        output,
        input_grad,
        gain_one,
        shift_one,
        qkv_weight_grad,
        qkv_bias_grad,
        out_weight_grad,
        gain_two,
        shift_two,
        gate_weight_grad,
        up_weight_grad,
        down_weight_grad,
    )


def solution(mesh):
    in_specs = (
        P(("dp", "mp"), None),
        P("dp", None),
        P(),
        P(),
        P(None, "dp", "mp"),
        P(None, "mp"),
        P("mp", "dp"),
        P(),
        P(),
        P("dp", "mp"),
        P("dp", "mp"),
        P("mp", "dp"),
        P(("dp", "mp"), None),
    )
    out_specs = (
        P(("dp", "mp"), None),
        P(("dp", "mp"), None),
        P(),
        P(),
        P(None, "dp", "mp"),
        P(None, "mp"),
        P("mp", "dp"),
        P(),
        P(),
        P("dp", "mp"),
        P("dp", "mp"),
        P("mp", "dp"),
    )
    return jax.shard_map(body, mesh=mesh, in_specs=in_specs, out_specs=out_specs, check_vma=False)
```

```python
import functools

import jax
import jax.numpy as jnp
from jax import lax
from jax.experimental import pallas as pl
from jax.experimental.pallas import tpu as pltpu
from jax.sharding import PartitionSpec as P

HEAD_DIM = 64
ROT = 16


NEG = -1e30
EPS = 1e-05
BASE = 10000.0

MESH = pl.DeviceIdType.MESH
VMEM_LIMIT = 60 * 1024 * 1024


def chip_at(spot, chips):
    side = spot // (chips // 2)
    return (spot + side * (chips - 1 - 2 * spot)) * 2 + side


def span(start, size):
    return pl.ds(pl.multiple_of(start, size), size)


def remote(src, dst, send, recv, who):
    return pltpu.make_async_remote_copy(
        src_ref=src,
        dst_ref=dst,
        send_sem=send,
        recv_sem=recv,
        device_id={"dp": who},
        device_id_type=MESH,
    )


def ring_kernel(chips, gathers, swaps, groups, *refs):
    refs = list(refs)
    scatters = sum(groups)

    def take(number):
        taken = refs[:number]
        del refs[:number]
        return taken

    shards, sends, parts = take(gathers), take(swaps), take(scatters)
    fulls, gets, grouped = take(gathers), take(swaps), take(len(groups))
    outs = []
    for group, out in zip(groups, grouped):
        outs += [out] if group == 1 else [out.at[j] for j in range(group)]
    mine, pair, ring, last = take(scatters), take(scatters), take(scatters), take(scatters)
    if gathers:
        keep_sem, give_sem, got_sem, lend_sem, lent_sem = take(5)
    if swaps:
        swap_send, swap_recv = take(2)
    if scatters:
        load_sem, pair_send, pair_recv, send_sem, recv_sem, last_send, last_recv = take(7)
    device = lax.axis_index("dp")
    chip, core = device // 2, device % 2
    row, side = chip // 2, chip % 2
    spot, way = row + side * (chips - 1 - 2 * row), 1 - 2 * core
    partner = device + way
    after = chip_at((spot + 1) % chips, chips)
    before = chip_at((spot + chips - 1) % chips, chips)
    source = chip_at((spot + chips - way) % chips, chips)
    target = chip_at((spot + chips + way) % chips, chips) * 2 + core
    barrier = pltpu.get_barrier_semaphore()
    for who in (source * 2, source * 2 + 1, partner):
        pl.semaphore_signal(barrier, inc=1, device_id={"dp": who}, device_id_type=MESH)
    if swaps:
        other = 1 - lax.axis_index("mp")
        pl.semaphore_signal(barrier, inc=1, device_id={"mp": other}, device_id_type=MESH)
    pl.semaphore_wait(barrier, 4 if swaps else 3)
    ends = []

    def begin(copy, end):
        copy.start()
        ends.append(end)
        return copy

    for i in range(swaps):
        copy = pltpu.make_async_remote_copy(
            src_ref=sends[i],
            dst_ref=gets[i],
            send_sem=swap_send.at[i],
            recv_sem=swap_recv.at[i],
            device_id={"mp": other},
            device_id_type=MESH,
        )
        begin(copy, copy.wait)
    for i in range(gathers):
        unit, cols = shards[i].shape[0], shards[i].shape[1] // 2
        own = fulls[i].at[span(device * unit, unit), :]
        for half, who in ((0, after * 2), (1, before * 2 + 1)):
            copy = remote(
                shards[i].at[:, pl.ds(half * cols, cols)],
                fulls[i].at[span(device * unit, unit), pl.ds(half * cols, cols)],
                give_sem.at[i, half],
                got_sem.at[i, core],
                who,
            )
            begin(copy, copy.wait_send)
        copy = remote(shards[i], own, lend_sem.at[i, 0], lent_sem.at[i, 0], partner)
        begin(copy, copy.wait)
        copy = pltpu.make_async_copy(shards[i], own, keep_sem.at[i])
        begin(copy, copy.wait)

    loads, pairs = {}, {}
    for step in range(chips):
        away = chip_at((spot + 2 * chips + way * (step + 1)) % chips, chips)
        here = chip_at((spot + 2 * chips - way * (step + 1)) % chips, chips)
        for i in range(scatters):
            rows, cols = mine[i].shape[1:]
            copy = remote(
                parts[i].at[span(away * rows, rows), span((1 - core) * cols, cols)],
                pair[i].at[step],
                pair_send.at[i, step],
                pair_recv.at[i, step],
                partner,
            )
            pairs[step, i] = begin(copy, copy.wait_send)
            loads[step, i] = pltpu.make_async_copy(
                parts[i].at[span(here * rows, rows), span(core * cols, cols)],
                mine[i].at[step],
                load_sem.at[i, step],
            )
            loads[step, i].start()

    def gather_step(i, step):
        held = chip_at((spot + 2 * chips - way * step) % chips, chips)
        unit, cols = shards[i].shape[0], shards[i].shape[1] // 2
        block = fulls[i].at[span(held * 2 * unit, 2 * unit), span(core * cols, cols)]
        if step == 1:
            for sender in range(2):
                piece = fulls[i].at[span((held * 2 + sender) * unit, unit), span(core * cols, cols)]
                remote(piece, piece, give_sem.at[i, 0], got_sem.at[i, sender], target).wait_recv()
        else:
            remote(block, block, give_sem.at[i, 0], got_sem.at[i, step], target).wait_recv()
        if step < chips - 1:
            copy = remote(block, block, give_sem.at[i, step + 1], got_sem.at[i, step + 1], target)
            begin(copy, copy.wait_send)
        copy = remote(block, block, lend_sem.at[i, step], lent_sem.at[i, step], partner)
        begin(copy, copy.wait)

    def scatter_step(i, step):
        rows, cols = mine[i].shape[1:]
        lines = min(rows, 32)
        loads[step, i].wait()
        pairs[step, i].wait_recv()
        if step > 0:
            came = ring[i].at[step - 1]
            remote(came, came, send_sem.at[i, 0], recv_sem.at[i, step - 1], target).wait_recv()

        @pl.loop(0, rows // lines)
        def _(k):
            at = span(k * lines, lines)
            total = mine[i][step, at, :].astype(jnp.float32)
            total = total + pair[i][step, at, :].astype(jnp.float32)
            if step > 0:
                total = total + ring[i][step - 1, at, :].astype(jnp.float32)
            if step < chips - 1:
                mine[i][step, at, :] = total.astype(jnp.bfloat16)
            else:
                last[i][at, :] = total

        if step < chips - 1:
            copy = remote(
                mine[i].at[step], ring[i].at[step], send_sem.at[i, step], recv_sem.at[i, step], target
            )
            begin(copy, copy.wait_send)
        else:
            unit = rows // 2
            place = outs[i].at[:, span(core * cols, cols)]
            copy = remote(
                last[i].at[span((1 - core) * unit, unit), :],
                place,
                last_send.at[i, 0],
                last_recv.at[i],
                partner,
            )
            begin(copy, copy.wait)
            copy = pltpu.make_async_copy(
                last[i].at[span(core * unit, unit), :], place, last_send.at[i, 1]
            )
            begin(copy, copy.wait)

    for step in range(chips):
        for i in range(gathers):
            if step > 0:
                gather_step(i, step)
        for i in range(scatters):
            scatter_step(i, step)
    for end in ends:
        end()


def ring_call(call_id, shards=(), sends=(), parts=(), groups=()):
    size = lax.axis_size("dp")
    chips = size // 2
    gathers, swaps, scatters = len(shards), len(sends), len(parts)
    outs = [jax.ShapeDtypeStruct((s.shape[0] * size, s.shape[1]), s.dtype) for s in shards]
    outs += [jax.ShapeDtypeStruct(s.shape, s.dtype) for s in sends]
    first = 0
    for group in groups:
        shape = (parts[first].shape[0] // size, parts[first].shape[1])
        outs.append(jax.ShapeDtypeStruct(shape if group == 1 else (group,) + shape, jnp.float32))
        first += group
    blocks = [(p.shape[0] // chips, p.shape[1] // 2) for p in parts]
    scratch = [pltpu.VMEM((chips,) + b, jnp.bfloat16) for b in blocks] * 2
    scratch += [pltpu.VMEM((chips - 1,) + b, jnp.bfloat16) for b in blocks]
    scratch += [pltpu.VMEM(b, jnp.float32) for b in blocks]
    if gathers:
        scratch += [pltpu.SemaphoreType.DMA((gathers,))]
        scratch += [pltpu.SemaphoreType.DMA((gathers, chips))] * 4
    if swaps:
        scratch += [pltpu.SemaphoreType.DMA((swaps,))] * 2
    if scatters:
        scratch += [pltpu.SemaphoreType.DMA((scatters, chips))] * 5
        scratch += [pltpu.SemaphoreType.DMA((scatters, 2)), pltpu.SemaphoreType.DMA((scatters,))]
    moved = sum(s.size * 2 * size for s in shards) + sum(p.size * 2 for p in parts)
    return list(
        pl.pallas_call(
            functools.partial(ring_kernel, chips, gathers, swaps, tuple(groups)),
            out_shape=outs,
            in_specs=[pl.BlockSpec(memory_space=pltpu.VMEM)] * gathers
            + [pl.BlockSpec(memory_space=pl.ANY)] * (swaps + scatters),
            out_specs=[pl.BlockSpec(memory_space=pl.ANY)] * len(outs),
            scratch_shapes=scratch,
            compiler_params=pltpu.CompilerParams(
                collective_id=call_id, has_side_effects=True, vmem_limit_bytes=VMEM_LIMIT
            ),
            cost_estimate=pl.CostEstimate(flops=0, bytes_accessed=moved, transcendentals=0),
        )(*shards, *sends, *parts)
    )


def feed_kernel(
    chips,
    tile,
    up_shard,
    down_shard,
    normed_ref,
    cot_ref,
    gate_full,
    up_full,
    down_full,
    rows_out,
    gate_out,
    up_out,
    hidden_out,
    term_out,
    rows,
    weights,
    gates,
    ups,
    hiddens,
    terms,
    keep_sem,
    give_sem,
    got_sem,
    lend_sem,
    lent_sem,
    swap_sem,
    load_sem,
    gate_sem,
    up_sem,
    hidden_sem,
    term_sem,
):
    device = lax.axis_index("dp")
    chip, core = device // 2, device % 2
    row, side = chip // 2, chip % 2
    spot, way = row + side * (chips - 1 - 2 * row), 1 - 2 * core
    partner = device + way
    after = chip_at((spot + 1) % chips, chips)
    before = chip_at((spot + chips - 1) % chips, chips)
    source = chip_at((spot + chips - way) % chips, chips)
    target = chip_at((spot + chips + way) % chips, chips) * 2 + core
    other = 1 - lax.axis_index("mp")
    barrier = pltpu.get_barrier_semaphore()
    for who in (source * 2, source * 2 + 1, partner):
        pl.semaphore_signal(barrier, inc=1, device_id={"dp": who}, device_id_type=MESH)
    pl.semaphore_signal(barrier, inc=1, device_id={"mp": other}, device_id_type=MESH)
    pl.semaphore_wait(barrier, 4)

    unit, wide = up_shard.shape
    tiles = wide // tile
    first = (wide // 256 + 1) // 2 * 256
    columns = (pl.ds(0, first), pl.ds(first, wide - first))
    shards = [ref.at[:, at] for ref in (up_shard, down_shard) for at in columns]
    fulls = [ref.at[:, at] for ref in (up_full, down_full) for at in columns]
    halves = [first // 2, (wide - first) // 2] * 2
    half_rows = normed_ref.shape[0]

    def own(i, half):
        at = slice(None) if half is None else pl.ds(half * halves[i], halves[i])
        return shards[i].at[:, at], fulls[i].at[span(device * unit, unit), at]

    def sent(i):
        copies = []
        for half, who in ((0, after * 2), (1, before * 2 + 1)):
            src, dst = own(i, half)
            copies.append(remote(src, dst, give_sem.at[i, half], got_sem.at[i, 1], who))
        return copies

    def shared(i):
        src, dst = own(i, None)
        return [
            remote(src, dst, lend_sem.at[i, 0], lent_sem.at[i, 0], partner),
            pltpu.make_async_copy(src, dst, keep_sem.at[i]),
        ]

    def block(i, step):
        held = chip_at((spot + 2 * chips - way * step) % chips, chips)
        return fulls[i].at[span(held * 2 * unit, 2 * unit), span(core * halves[i], halves[i])]

    def passed(i, step):
        at = block(i, step)
        return remote(at, at, give_sem.at[i, step + 1], got_sem.at[i, step + 1], target)

    def lent(i, step):
        at = block(i, step)
        return remote(at, at, lend_sem.at[i, step], lent_sem.at[i, step], partner)

    def relay(i, step):
        at = block(i, step)
        remote(at, at, give_sem.at[i, 0], got_sem.at[i, step], target).wait_recv()

        @pl.when(step < chips - 1)
        def _():
            passed(i, step).start()

        lent(i, step).start()

    def settle(i):
        for copy in shared(i):
            copy.wait()
        for copy in sent(i):
            copy.wait_send()

        @pl.loop(1, chips)
        def _(step):
            lent(i, step).wait()

            @pl.when(step < chips - 1)
            def _():
                passed(i, step).wait_send()

    exchange = pltpu.make_async_remote_copy(
        src_ref=normed_ref,
        dst_ref=rows.at[pl.ds(half_rows, half_rows), :],
        send_sem=swap_sem.at[0],
        recv_sem=swap_sem.at[1],
        device_id={"mp": other},
        device_id_type=MESH,
    )
    place = pltpu.make_async_copy(normed_ref, rows.at[pl.ds(0, half_rows), :], swap_sem.at[2])
    record = pltpu.make_async_copy(rows, rows_out, swap_sem.at[3])

    def load(ref, t):
        return pltpu.make_async_copy(
            ref.at[:, span(t * tile, tile)], weights.at[t % 2], load_sem.at[t % 2]
        )

    def store(buffer, out, sem, t):
        at = span(t * tile, tile)
        return pltpu.make_async_copy(buffer.at[:, at], out.at[:, at], sem.at[t])

    def store_term(t):
        return pltpu.make_async_copy(
            terms.at[t % 2], term_out.at[:, span(t * tile, tile)], term_sem.at[t % 2]
        )

    def weight_of(ref, t):
        load(ref, t).wait()

        @pl.when(t + 1 < tiles)
        def _():
            load(ref, t + 1).start()

        return weights[t % 2]

    def gate_tile(t):
        gates[:, span(t * tile, tile)] = jnp.dot(
            rows[...], weight_of(gate_full, t), preferred_element_type=jnp.float32
        )
        store(gates, gate_out, gate_sem, t).start()

    def up_tile(t):
        at = span(t * tile, tile)
        upward = jnp.dot(rows[...], weight_of(up_full, t), preferred_element_type=jnp.float32)
        ups[:, at] = upward
        store(ups, up_out, up_sem, t).start()
        gate = gates[:, at]
        hidden = (gate * jax.nn.sigmoid(gate) * upward).astype(jnp.bfloat16)
        hiddens[:, at] = hidden
        store(hiddens, hidden_out, hidden_sem, t).start()

        @pl.when(t > 1)
        def _():
            store_term(t - 2).wait()

        terms[t % 2] = jnp.dot(
            cot_ref[...], hidden, preferred_element_type=jnp.float32
        ).astype(jnp.bfloat16)
        store_term(t).start()

    def some(number, start, work):
        @pl.loop(0, number)
        def _(k):
            @pl.when(start + k < tiles)
            def _():
                work(start + k)

    for i in (0, 1):
        for copy in sent(i) + shared(i):
            copy.start()
    exchange.start()
    place.start()
    load(gate_full, 0).start()
    late = chips // 2
    each = -(-tiles // (chips - late))

    @pl.loop(1, chips)
    def _(step):
        relay(0, step)
        relay(1, step)

        @pl.when(step == chips - 2)
        def _():
            for i in (2, 3):
                for copy in sent(i) + shared(i):
                    copy.start()

        @pl.when(step == late)
        def _():
            place.wait()
            exchange.wait()
            record.start()

        @pl.when(step >= late)
        def _():
            some(each, (step - late) * each, gate_tile)

    settle(0)
    settle(1)
    load(up_full, 0).start()
    each = -(-tiles // (chips - 1))
    early = -(-each // 2)

    @pl.loop(1, chips)
    def _(step):
        relay(2, step)
        some(early, (step - 1) * each, up_tile)
        relay(3, step)
        if each > early:
            some(each - early, (step - 1) * each + early, up_tile)

    settle(2)
    settle(3)
    record.wait()

    @pl.loop(0, tiles)
    def _(t):
        store(gates, gate_out, gate_sem, t).wait()
        store(ups, up_out, up_sem, t).wait()
        store(hiddens, hidden_out, hidden_sem, t).wait()

    for t in range(max(tiles - 2, 0), tiles):
        store_term(t).wait()


def feed_call(call_id, up_shard, down_shard, normed_here, cot_turned, gate_full):
    size = lax.axis_size("dp")
    chips = size // 2
    unit, wide = up_shard.shape
    depth, tokens = cot_turned.shape
    tile = 256
    tiles = wide // tile
    low, high = jnp.bfloat16, jnp.float32
    kept = pl.BlockSpec(memory_space=pltpu.VMEM)
    far = pl.BlockSpec(memory_space=pl.ANY)
    dma = pltpu.SemaphoreType.DMA
    return pl.pallas_call(
        functools.partial(feed_kernel, chips, tile),
        out_shape=[
            jax.ShapeDtypeStruct((depth, wide), low),
            jax.ShapeDtypeStruct((depth, wide), low),
            jax.ShapeDtypeStruct((tokens, depth), low),
            jax.ShapeDtypeStruct((tokens, wide), high),
            jax.ShapeDtypeStruct((tokens, wide), high),
            jax.ShapeDtypeStruct((tokens, wide), low),
            jax.ShapeDtypeStruct((depth, wide), low),
        ],
        in_specs=[kept, kept, kept, kept, far],
        out_specs=[far] * 7,
        scratch_shapes=[
            pltpu.VMEM((tokens, depth), low),
            pltpu.VMEM((2, depth, tile), low),
            pltpu.VMEM((tokens, wide), high),
            pltpu.VMEM((tokens, wide), high),
            pltpu.VMEM((tokens, wide), low),
            pltpu.VMEM((2, depth, tile), low),
            dma((4,)),
        ]
        + [dma((4, chips + 1))] * 4
        + [dma((4,)), dma((2,)), dma((tiles,)), dma((tiles,)), dma((tiles,)), dma((2,))],
        compiler_params=pltpu.CompilerParams(
            collective_id=call_id, has_side_effects=True, vmem_limit_bytes=VMEM_LIMIT
        ),
        cost_estimate=pl.CostEstimate(
            flops=6 * tokens * depth * wide,
            bytes_accessed=12 * depth * wide + 12 * tokens * wide,
            transcendentals=tokens * wide,
        ),
    )(up_shard, down_shard, normed_here, cot_turned, gate_full)


def back_kernel(
    chips,
    tile,
    cot_ref,
    gate_ref,
    up_ref,
    gate_full,
    up_full,
    down_full,
    term_ref,
    gate_out,
    up_out,
    part_out,
    far_out,
    grad_out,
    mine_a,
    mine_b,
    pair_a,
    pair_b,
    ring_a,
    ring_b,
    last_a,
    last_b,
    weights,
    states,
    acts,
    total,
    low,
    load_sem,
    state_sem,
    act_sem,
    keep_sem,
    swap_sem,
    own_sem,
    pair_send,
    pair_recv,
    send_sem,
    recv_sem,
    last_send,
    last_recv,
):
    device = lax.axis_index("dp")
    chip, core = device // 2, device % 2
    row, side = chip // 2, chip % 2
    spot, way = row + side * (chips - 1 - 2 * row), 1 - 2 * core
    partner = device + way
    source = chip_at((spot + chips - way) % chips, chips)
    target = chip_at((spot + chips + way) % chips, chips) * 2 + core
    other = 1 - lax.axis_index("mp")
    barrier = pltpu.get_barrier_semaphore()
    for who in (source * 2, source * 2 + 1, partner):
        pl.semaphore_signal(barrier, inc=1, device_id={"dp": who}, device_id_type=MESH)
    pl.semaphore_signal(barrier, inc=1, device_id={"mp": other}, device_id_type=MESH)
    pl.semaphore_wait(barrier, 4)

    mine, pair, ring, last = (mine_a, mine_b), (pair_a, pair_b), (ring_a, ring_b), (last_a, last_b)
    wide = gate_ref.shape[1]
    half_rows = part_out.shape[0]
    tiles = wide // tile
    first = (wide // 256 + 1) // 2 * 256
    columns = (pl.ds(0, first), pl.ds(first, wide - first))
    parts = [term_ref.at[:, at] for at in columns]
    outs = [grad_out.at[:, at] for at in columns]

    def own(i, step):
        rows, cols = mine[i].shape[1:]
        here = chip_at((spot + 2 * chips - way * (step + 1)) % chips, chips)
        return pltpu.make_async_copy(
            parts[i].at[span(here * rows, rows), span(core * cols, cols)],
            mine[i].at[step],
            own_sem.at[i, step],
        )

    def trade(i, step):
        rows, cols = mine[i].shape[1:]
        away = chip_at((spot + 2 * chips + way * (step + 1)) % chips, chips)
        return remote(
            parts[i].at[span(away * rows, rows), span((1 - core) * cols, cols)],
            pair[i].at[step],
            pair_send.at[i, step],
            pair_recv.at[i, step],
            partner,
        )

    def onward(i, step):
        return remote(
            mine[i].at[step], ring[i].at[step], send_sem.at[i, step], recv_sem.at[i, step], target
        )

    def ending(i):
        rows, cols = mine[i].shape[1:]
        unit = rows // 2
        place = outs[i].at[:, span(core * cols, cols)]
        return (
            remote(
                last[i].at[span((1 - core) * unit, unit), :],
                place,
                last_send.at[i, 0],
                last_recv.at[i],
                partner,
            ),
            pltpu.make_async_copy(
                last[i].at[span(core * unit, unit), :], place, last_send.at[i, 1]
            ),
        )

    def sum_step(i, step):
        rows = mine[i].shape[1]
        lines = min(rows, 32)
        own(i, step).wait()
        trade(i, step).wait_recv()

        def added(at):
            value = mine[i][step, at, :].astype(jnp.float32)
            return value + pair[i][step, at, :].astype(jnp.float32)

        @pl.when(step == 0)
        def _():
            @pl.loop(0, rows // lines)
            def _(k):
                at = span(k * lines, lines)
                mine[i][step, at, :] = added(at).astype(jnp.bfloat16)

        @pl.when(step > 0)
        def _():
            came = ring[i].at[step - 1]
            remote(came, came, send_sem.at[i, 0], recv_sem.at[i, step - 1], target).wait_recv()

            @pl.when(step < chips - 1)
            def _():
                @pl.loop(0, rows // lines)
                def _(k):
                    at = span(k * lines, lines)
                    value = added(at) + ring[i][step - 1, at, :].astype(jnp.float32)
                    mine[i][step, at, :] = value.astype(jnp.bfloat16)

            @pl.when(step == chips - 1)
            def _():
                @pl.loop(0, rows // lines)
                def _(k):
                    at = span(k * lines, lines)
                    last[i][at, :] = added(at) + ring[i][step - 1, at, :].astype(jnp.float32)

        @pl.when(step < chips - 1)
        def _():
            onward(i, step).start()

        @pl.when(step == chips - 1)
        def _():
            for copy in ending(i):
                copy.start()

    def loads(t):
        at, slot = span(t * tile, tile), t % 2
        copies = [
            pltpu.make_async_copy(ref.at[:, at], weights.at[k, slot], load_sem.at[k, slot])
            for k, ref in enumerate((down_full, gate_full, up_full))
        ]
        return copies + [
            pltpu.make_async_copy(ref.at[:, at], states.at[k, slot], state_sem.at[k, slot])
            for k, ref in enumerate((gate_ref, up_ref))
        ]

    def stores(t):
        at, slot = span(t * tile, tile), t % 2
        return [
            pltpu.make_async_copy(acts.at[k, slot], ref.at[:, at], act_sem.at[k, slot])
            for k, ref in enumerate((gate_out, up_out))
        ]

    def work(t):
        slot = t % 2
        for copy in loads(t):
            copy.wait()

        @pl.when(t + 1 < tiles)
        def _():
            for copy in loads(t + 1):
                copy.start()

        @pl.when(t > 1)
        def _():
            for copy in stores(t - 2):
                copy.wait()

        hidden_grad = jnp.dot(
            cot_ref[...], weights[0, slot], preferred_element_type=jnp.float32
        )
        gate, upward = states[0, slot], states[1, slot]
        sigma = jax.nn.sigmoid(gate)
        gate_act = hidden_grad * upward * sigma * (1.0 + gate * (1.0 - sigma))
        acts[0, slot] = gate_act.astype(jnp.bfloat16)
        acts[1, slot] = (hidden_grad * gate * sigma).astype(jnp.bfloat16)
        for copy in stores(t):
            copy.start()
        depth = total.shape[1]
        band = depth // 4

        @pl.loop(0, 4)
        def _(k):
            at = span(k * band, band)
            value = total[:, at]
            for which in range(2):
                value = value + lax.dot_general(
                    acts[which, slot],
                    weights[which + 1, slot, at, :],
                    (((1,), (1,)), ((), ())),
                    preferred_element_type=jnp.float32,
                )
            total[:, at] = value

    def some(number, start):
        @pl.loop(0, number)
        def _(k):
            @pl.when(start + k < tiles)
            def _():
                work(start + k)

    keep = pltpu.make_async_copy(total.at[pl.ds(0, half_rows), :], part_out, keep_sem.at[0])
    exchange = pltpu.make_async_remote_copy(
        src_ref=low,
        dst_ref=far_out,
        send_sem=swap_sem.at[0],
        recv_sem=swap_sem.at[1],
        device_id={"mp": other},
        device_id_type=MESH,
    )

    @pl.loop(0, chips)
    def _(step):
        for i in range(2):
            trade(i, step).start()
            own(i, step).start()

    for copy in loads(0):
        copy.start()
    total[...] = jnp.zeros_like(total)
    each = -(-tiles // (chips - 1))
    early = -(-each // 2)

    @pl.loop(0, chips)
    def _(step):
        sum_step(0, step)
        some(early, step * each)
        sum_step(1, step)
        if each > early:
            some(each - early, step * each + early)

        @pl.when(step == -(-tiles // each) - 1)
        def _():
            low[...] = total[pl.ds(half_rows, half_rows), :].astype(jnp.bfloat16)
            exchange.start()
            keep.start()

    keep.wait()
    exchange.wait()
    for t in range(max(tiles - 2, 0), tiles):
        for copy in stores(t):
            copy.wait()
    for i in range(2):
        for copy in ending(i):
            copy.wait()

    @pl.loop(0, chips)
    def _(step):
        for i in range(2):
            trade(i, step).wait_send()

            @pl.when(step < chips - 1)
            def _():
                onward(i, step).wait_send()


def back_call(call_id, cot_rows, gate, upward, gate_full, up_full, down_full, down_term):
    size = lax.axis_size("dp")
    chips = size // 2
    tokens, depth = cot_rows.shape
    wide = gate.shape[1]
    tile = 256
    first = (wide // 256 + 1) // 2 * 256
    blocks = [(depth // chips, first // 2), (depth // chips, (wide - first) // 2)]
    low, high = jnp.bfloat16, jnp.float32
    far = pl.BlockSpec(memory_space=pl.ANY)
    dma = pltpu.SemaphoreType.DMA
    return pl.pallas_call(
        functools.partial(back_kernel, chips, tile),
        out_shape=[
            jax.ShapeDtypeStruct((tokens, wide), low),
            jax.ShapeDtypeStruct((tokens, wide), low),
            jax.ShapeDtypeStruct((tokens // 2, depth), high),
            jax.ShapeDtypeStruct((tokens // 2, depth), low),
            jax.ShapeDtypeStruct((depth // size, wide), high),
        ],
        in_specs=[pl.BlockSpec(memory_space=pltpu.VMEM)] + [far] * 6,
        out_specs=[far] * 5,
        scratch_shapes=[pltpu.VMEM((chips,) + b, low) for b in blocks] * 2
        + [pltpu.VMEM((chips - 1,) + b, low) for b in blocks]
        + [pltpu.VMEM(b, high) for b in blocks]
        + [
            pltpu.VMEM((3, 2, depth, tile), low),
            pltpu.VMEM((2, 2, tokens, tile), high),
            pltpu.VMEM((2, 2, tokens, tile), low),
            pltpu.VMEM((tokens, depth), high),
            pltpu.VMEM((tokens // 2, depth), low),
            dma((3, 2)),
            dma((2, 2)),
            dma((2, 2)),
            dma((1,)),
            dma((2,)),
        ]
        + [dma((2, chips))] * 5
        + [dma((2, 2)), dma((2,))],
        compiler_params=pltpu.CompilerParams(
            collective_id=call_id, has_side_effects=True, vmem_limit_bytes=VMEM_LIMIT
        ),
        cost_estimate=pl.CostEstimate(
            flops=6 * tokens * depth * wide,
            bytes_accessed=8 * depth * wide + 12 * tokens * wide,
            transcendentals=tokens * wide,
        ),
    )(cot_rows, gate, upward, gate_full, up_full, down_full, down_term)


def layer_norm(values, norm_gain, norm_shift):
    center = values - jnp.mean(values, axis=-1, keepdims=True)
    inverse = lax.rsqrt(jnp.mean(center * center, axis=-1, keepdims=True) + EPS)
    scaled = center * inverse
    return (scaled * norm_gain + norm_shift, scaled, inverse)


def norm_back(grads, scaled, inverse, norm_gain):
    weighted = grads * norm_gain
    return inverse * (
        weighted
        - jnp.mean(weighted, axis=-1, keepdims=True)
        - scaled * jnp.mean(weighted * scaled, axis=-1, keepdims=True)
    )


def rotary_tables(segments, places, rotary_dims):
    earlier = (segments[None, :] < segments[:, None]).astype(jnp.int32)
    position = (places - jnp.sum(earlier, axis=1)).astype(jnp.float32)
    half_dims = rotary_dims // 2
    frequency = BASE ** (-2.0 * jnp.arange(half_dims, dtype=jnp.float32) / rotary_dims)
    angles = position[:, None] * frequency[None, :]
    return (jnp.cos(angles), jnp.sin(angles))


def rotate(values, cosine, sine_table, rotary_dims, turn_sign):
    half_dims = rotary_dims // 2
    leading = values[..., :half_dims]
    trailing = values[..., half_dims:rotary_dims]
    cos_rows = cosine[:, None, :]
    sin_rows = turn_sign * sine_table[:, None, :]
    return jnp.concatenate(
        [
            leading * cos_rows - trailing * sin_rows,
            trailing * cos_rows + leading * sin_rows,
            values[..., rotary_dims:],
        ],
        axis=-1,
    )


def masked_scores(query, key_rot, allowed, score_scale):
    scores = (
        jnp.einsum("qhd,khd->hqk", query, key_rot, preferred_element_type=jnp.float32) * score_scale
    )
    return jnp.where(allowed[None], scores, NEG)


def swap(values):
    return lax.ppermute(values, "mp", [(0, 1), (1, 0)])


def half_sum(part):
    half = part.shape[0] // 2
    other = swap(part[half:].astype(jnp.bfloat16))
    return part[:half] + other.astype(jnp.float32)


def grow(rows):
    return jnp.concatenate([rows, swap(rows)], axis=0)


def scatter(term, axis):
    return lax.psum_scatter(term, "dp", scatter_dimension=axis, tiled=True).astype(jnp.float32)


def body(
    inputs,
    segment_ids,
    norm1_gain,
    norm1_shift,
    qkv_weight,
    qkv_bias,
    out_weight,
    norm2_gain,
    norm2_shift,
    gate_weight,
    up_weight,
    down_weight,
    cotangent,
):
    score_scale = HEAD_DIM ** (-0.5)
    rows_here = inputs.shape[0]
    width = inputs.shape[1]
    *qkv_full, out_turned, far_inputs, far_cot = ring_call(
        0,
        shards=[qkv_weight[0], qkv_weight[1], qkv_weight[2], out_weight.T],
        sends=[inputs, cotangent],
    )
    input_rows = jnp.concatenate([inputs, far_inputs], axis=0)
    cot_rows = jnp.concatenate([cotangent, far_cot], axis=0)
    gate_weight, out_turned = lax.optimization_barrier((gate_weight, out_turned))
    gate_full = lax.all_gather(gate_weight, "dp", axis=0, tiled=True)
    stream_rows = input_rows.astype(jnp.float32)
    stream = stream_rows[:rows_here]
    normed_wide, scaled_rows, inverse_rows = layer_norm(stream_rows, norm1_gain, norm1_shift)
    normed_one = normed_wide.astype(jnp.bfloat16)
    scaled_one = scaled_rows[:rows_here]
    inverse_one = inverse_rows[:rows_here]
    seq_len = normed_one.shape[0]
    local_width = qkv_full[0].shape[1]
    head_count = local_width // HEAD_DIM
    turn = lax.axis_index("mp") * rows_here
    segments = jnp.roll(segment_ids[0], -turn)
    places = jnp.roll(jnp.arange(seq_len, dtype=jnp.int32), -turn)
    allowed = (places[None, :] <= places[:, None]) & (segments[:, None] == segments[None, :])
    cosine, sine_table = rotary_tables(segments, places, ROT)
    shaped = [
        (jnp.dot(normed_one, full, preferred_element_type=jnp.float32) + bias).reshape(
            seq_len, head_count, HEAD_DIM
        )
        for full, bias in zip(qkv_full, qkv_bias)
    ]
    query = rotate(shaped[0], cosine, sine_table, ROT, 1.0).astype(jnp.bfloat16)
    key_rot = rotate(shaped[1], cosine, sine_table, ROT, 1.0).astype(jnp.bfloat16)
    value = shaped[2].astype(jnp.bfloat16)
    scores = masked_scores(query, key_rot, allowed, score_scale)
    row_max = jnp.max(scores, axis=-1, keepdims=True)
    exponent = jnp.exp(scores - row_max)
    row_total = jnp.sum(exponent, axis=-1, keepdims=True)
    log_total = row_max + jnp.log(row_total)
    probs_low = (exponent / row_total).astype(jnp.bfloat16)
    mixed_heads = jnp.einsum(
        "hqk,khd->qhd", probs_low, value, preferred_element_type=jnp.float32
    ).astype(jnp.bfloat16)
    mixed = mixed_heads.reshape(seq_len, local_width)
    branch = jnp.dot(mixed, out_turned.T, preferred_element_type=jnp.float32)
    middle = stream + half_sum(branch)
    normed_wide2, scaled_two, inverse_two = layer_norm(middle, norm2_gain, norm2_shift)
    normed_here = normed_wide2.astype(jnp.bfloat16)
    up_full, down_turned, normed_two, gate, upward, hidden, down_term = feed_call(
        1, up_weight, down_weight.T, normed_here, cot_rows.T, gate_full
    )
    gate_act, up_act, part_here, part_far, down_grad_turned = back_call(
        3, cot_rows, gate, upward, gate_full, up_full, down_turned, down_term
    )
    down_weight_grad = down_grad_turned.T
    normed_two_grad = part_here + part_far.astype(jnp.float32)
    gate_term = jnp.dot(normed_two.T, gate_act, preferred_element_type=jnp.float32)
    gate_weight_grad = scatter(gate_term.astype(jnp.bfloat16), 0)
    gain_two = jnp.sum(normed_two_grad * scaled_two, axis=0)
    shift_two = jnp.sum(normed_two_grad, axis=0)
    middle_grad = cotangent.astype(jnp.float32) + norm_back(
        normed_two_grad, scaled_two, inverse_two, norm2_gain
    )
    middle_low, hidden, up_act = lax.optimization_barrier(
        (middle_grad.astype(jnp.bfloat16), hidden, up_act)
    )
    middle_rows = grow(middle_low)
    up_term = jnp.dot(normed_two.T, up_act, preferred_element_type=jnp.float32)
    feed_part = jnp.dot(hidden, down_turned.T, preferred_element_type=jnp.float32)
    out_term = jnp.dot(middle_rows.T, mixed, preferred_element_type=jnp.float32)
    mixed_grad = (
        jnp.dot(middle_rows, out_turned, preferred_element_type=jnp.float32)
        .astype(jnp.bfloat16)
        .reshape(seq_len, head_count, HEAD_DIM)
    )
    probs_wide = jnp.exp(scores - log_total)
    value_grad = jnp.einsum(
        "hqk,qhd->khd",
        probs_wide.astype(jnp.bfloat16),
        mixed_grad,
        preferred_element_type=jnp.float32,
    )
    prob_grad = jnp.einsum("qhd,khd->hqk", mixed_grad, value, preferred_element_type=jnp.float32)
    row_delta = jnp.transpose(
        jnp.sum(mixed_grad.astype(jnp.float32) * mixed_heads.astype(jnp.float32), axis=-1)
    )
    score_grad = (probs_wide * (prob_grad - row_delta[:, :, None]) * score_scale).astype(
        jnp.bfloat16
    )
    query_grad = jnp.einsum("hqk,khd->qhd", score_grad, key_rot, preferred_element_type=jnp.float32)
    key_grad = jnp.einsum("hqk,qhd->khd", score_grad, query, preferred_element_type=jnp.float32)
    query_back = rotate(query_grad, cosine, sine_table, ROT, -1.0)
    key_back = rotate(key_grad, cosine, sine_table, ROT, -1.0)
    proj_grad = [
        part.reshape(seq_len, local_width) for part in (query_back, key_back, value_grad)
    ]
    rotated_cols = jnp.arange(local_width, dtype=jnp.int32) % HEAD_DIM < ROT
    bias_sums = [jnp.sum(part, axis=0) for part in proj_grad]
    bias_term = [bias_sums[0], jnp.where(rotated_cols, bias_sums[1], 0.0), bias_sums[2]]
    proj_low = [part.astype(jnp.bfloat16) for part in proj_grad]
    normed_one_part = jnp.zeros((), jnp.float32)
    for part, full in zip(proj_low, qkv_full):
        normed_one_part = normed_one_part + jnp.dot(
            part, full.T, preferred_element_type=jnp.float32
        )
    gain_one = jnp.sum(normed_one_part * scaled_rows, axis=0)
    shift_one = jnp.sum(normed_one_part, axis=0)
    norm_sums = jnp.concatenate([gain_one, shift_one, gain_two, shift_two])
    norm_sums = norm_sums + swap(norm_sums)
    sums = jnp.concatenate([norm_sums] + bias_term)
    spare = -sums.size % (8 * 256)
    qkv_term = [
        jnp.dot(normed_one.T, part, preferred_element_type=jnp.float32) for part in proj_low
    ]
    all_sums, far_part, far_feed, up_weight_grad, out_grad_turned, qkv_weight_grad = ring_call(
        2,
        shards=[jnp.pad(sums, (0, spare)).reshape(8, -1)],
        sends=[part[rows_here:].astype(jnp.bfloat16) for part in (normed_one_part, feed_part)],
        parts=[term.astype(jnp.bfloat16) for term in [up_term, out_term] + qkv_term],
        groups=[1, 1, 3],
    )
    out_weight_grad = out_grad_turned.T
    normed_one_grad = normed_one_part[:rows_here] + far_part.astype(jnp.float32)
    feed = feed_part[:rows_here] + far_feed.astype(jnp.float32)
    output = (middle + feed).astype(jnp.bfloat16)
    all_sums = jnp.sum(all_sums.reshape(-1, 8, all_sums.shape[1]), axis=0).reshape(-1)
    gain_one, shift_one, gain_two, shift_two = all_sums[: 4 * width].reshape(4, width)
    qkv_bias_grad = all_sums[4 * width : sums.size].reshape(3, local_width)
    input_grad = middle_grad + norm_back(normed_one_grad, scaled_one, inverse_one, norm1_gain)
    return (
        output,
        input_grad,
        gain_one,
        shift_one,
        qkv_weight_grad,
        qkv_bias_grad,
        out_weight_grad,
        gain_two,
        shift_two,
        gate_weight_grad,
        up_weight_grad,
        down_weight_grad,
    )


def solution(mesh):
    in_specs = (
        P(("dp", "mp"), None),
        P("dp", None),
        P(),
        P(),
        P(None, "dp", "mp"),
        P(None, "mp"),
        P("mp", "dp"),
        P(),
        P(),
        P("dp", "mp"),
        P("dp", "mp"),
        P("mp", "dp"),
        P(("dp", "mp"), None),
    )
    out_specs = (
        P(("dp", "mp"), None),
        P(("dp", "mp"), None),
        P(),
        P(),
        P(None, "dp", "mp"),
        P(None, "mp"),
        P("mp", "dp"),
        P(),
        P(),
        P("dp", "mp"),
        P("dp", "mp"),
        P("mp", "dp"),
    )
    return jax.shard_map(body, mesh=mesh, in_specs=in_specs, out_specs=out_specs, check_vma=False)
```

```python
import functools

import jax
import jax.numpy as jnp
from jax import lax
from jax.experimental import pallas as pl
from jax.experimental.pallas import tpu as pltpu
from jax.sharding import PartitionSpec as P


HEAD_DIM = 64
ROT = 16


NEG = -1e30
EPS = 1e-05
BASE = 10000.0

MESH = pl.DeviceIdType.MESH
VMEM_LIMIT = 60 * 1024 * 1024


def chip_at(spot, chips):
    side = spot // (chips // 2)
    return (spot + side * (chips - 1 - 2 * spot)) * 2 + side


def span(start, size):
    return pl.ds(pl.multiple_of(start, size), size)


def remote(src, dst, send, recv, who):
    return pltpu.make_async_remote_copy(
        src_ref=src,
        dst_ref=dst,
        send_sem=send,
        recv_sem=recv,
        device_id={"dp": who},
        device_id_type=MESH,
    )


def ring_kernel(chips, gathers, swaps, groups, *refs):
    refs = list(refs)
    scatters = sum(groups)

    def take(number):
        taken = refs[:number]
        del refs[:number]
        return taken

    shards, sends, parts = take(gathers), take(swaps), take(scatters)
    fulls, gets, grouped = take(gathers), take(swaps), take(len(groups))
    outs = []
    for group, out in zip(groups, grouped):
        outs += [out] if group == 1 else [out.at[j] for j in range(group)]
    mine, pair, ring, last = take(scatters), take(scatters), take(scatters), take(scatters)
    if gathers:
        keep_sem, give_sem, got_sem, lend_sem, lent_sem = take(5)
    if swaps:
        swap_send, swap_recv = take(2)
    if scatters:
        load_sem, pair_send, pair_recv, send_sem, recv_sem, last_send, last_recv = take(7)
    device = lax.axis_index("dp")
    chip, core = device // 2, device % 2
    row, side = chip // 2, chip % 2
    spot, way = row + side * (chips - 1 - 2 * row), 1 - 2 * core
    partner = device + way
    after = chip_at((spot + 1) % chips, chips)
    before = chip_at((spot + chips - 1) % chips, chips)
    source = chip_at((spot + chips - way) % chips, chips)
    target = chip_at((spot + chips + way) % chips, chips) * 2 + core
    barrier = pltpu.get_barrier_semaphore()
    for who in (source * 2, source * 2 + 1, partner):
        pl.semaphore_signal(barrier, inc=1, device_id={"dp": who}, device_id_type=MESH)
    if swaps:
        other = 1 - lax.axis_index("mp")
        pl.semaphore_signal(barrier, inc=1, device_id={"mp": other}, device_id_type=MESH)
    pl.semaphore_wait(barrier, 4 if swaps else 3)
    ends = []

    def begin(copy, end):
        copy.start()
        ends.append(end)
        return copy

    for i in range(swaps):
        copy = pltpu.make_async_remote_copy(
            src_ref=sends[i],
            dst_ref=gets[i],
            send_sem=swap_send.at[i],
            recv_sem=swap_recv.at[i],
            device_id={"mp": other},
            device_id_type=MESH,
        )
        begin(copy, copy.wait)
    for i in range(gathers):
        unit, cols = shards[i].shape[0], shards[i].shape[1] // 2
        own = fulls[i].at[span(device * unit, unit), :]
        for half, who in ((0, after * 2), (1, before * 2 + 1)):
            copy = remote(
                shards[i].at[:, pl.ds(half * cols, cols)],
                fulls[i].at[span(device * unit, unit), pl.ds(half * cols, cols)],
                give_sem.at[i, half],
                got_sem.at[i, core],
                who,
            )
            begin(copy, copy.wait_send)
        copy = remote(shards[i], own, lend_sem.at[i, 0], lent_sem.at[i, 0], partner)
        begin(copy, copy.wait)
        copy = pltpu.make_async_copy(shards[i], own, keep_sem.at[i])
        begin(copy, copy.wait)

    loads, pairs = {}, {}
    for step in range(chips):
        away = chip_at((spot + 2 * chips + way * (step + 1)) % chips, chips)
        here = chip_at((spot + 2 * chips - way * (step + 1)) % chips, chips)
        for i in range(scatters):
            rows, cols = mine[i].shape[1:]
            copy = remote(
                parts[i].at[span(away * rows, rows), span((1 - core) * cols, cols)],
                pair[i].at[step],
                pair_send.at[i, step],
                pair_recv.at[i, step],
                partner,
            )
            pairs[step, i] = begin(copy, copy.wait_send)
            loads[step, i] = pltpu.make_async_copy(
                parts[i].at[span(here * rows, rows), span(core * cols, cols)],
                mine[i].at[step],
                load_sem.at[i, step],
            )
            loads[step, i].start()

    def gather_step(i, step):
        held = chip_at((spot + 2 * chips - way * step) % chips, chips)
        unit, cols = shards[i].shape[0], shards[i].shape[1] // 2
        block = fulls[i].at[span(held * 2 * unit, 2 * unit), span(core * cols, cols)]
        if step == 1:
            for sender in range(2):
                piece = fulls[i].at[span((held * 2 + sender) * unit, unit), span(core * cols, cols)]
                remote(piece, piece, give_sem.at[i, 0], got_sem.at[i, sender], target).wait_recv()
        else:
            remote(block, block, give_sem.at[i, 0], got_sem.at[i, step], target).wait_recv()
        if step < chips - 1:
            copy = remote(block, block, give_sem.at[i, step + 1], got_sem.at[i, step + 1], target)
            begin(copy, copy.wait_send)
        copy = remote(block, block, lend_sem.at[i, step], lent_sem.at[i, step], partner)
        begin(copy, copy.wait)

    def scatter_step(i, step):
        rows, cols = mine[i].shape[1:]
        lines = min(rows, 32)
        loads[step, i].wait()
        pairs[step, i].wait_recv()
        if step > 0:
            came = ring[i].at[step - 1]
            remote(came, came, send_sem.at[i, 0], recv_sem.at[i, step - 1], target).wait_recv()

        @pl.loop(0, rows // lines)
        def _(k):
            at = span(k * lines, lines)
            total = mine[i][step, at, :].astype(jnp.float32)
            total = total + pair[i][step, at, :].astype(jnp.float32)
            if step > 0:
                total = total + ring[i][step - 1, at, :].astype(jnp.float32)
            if step < chips - 1:
                mine[i][step, at, :] = total.astype(jnp.bfloat16)
            else:
                last[i][at, :] = total

        if step < chips - 1:
            copy = remote(
                mine[i].at[step], ring[i].at[step], send_sem.at[i, step], recv_sem.at[i, step], target
            )
            begin(copy, copy.wait_send)
        else:
            unit = rows // 2
            place = outs[i].at[:, span(core * cols, cols)]
            copy = remote(
                last[i].at[span((1 - core) * unit, unit), :],
                place,
                last_send.at[i, 0],
                last_recv.at[i],
                partner,
            )
            begin(copy, copy.wait)
            copy = pltpu.make_async_copy(
                last[i].at[span(core * unit, unit), :], place, last_send.at[i, 1]
            )
            begin(copy, copy.wait)

    for step in range(chips):
        for i in range(gathers):
            if step > 0:
                gather_step(i, step)
        for i in range(scatters):
            scatter_step(i, step)
    for end in ends:
        end()


def ring_call(call_id, shards=(), sends=(), parts=(), groups=()):
    size = lax.axis_size("dp")
    chips = size // 2
    gathers, swaps, scatters = len(shards), len(sends), len(parts)
    outs = [jax.ShapeDtypeStruct((s.shape[0] * size, s.shape[1]), s.dtype) for s in shards]
    outs += [jax.ShapeDtypeStruct(s.shape, s.dtype) for s in sends]
    first = 0
    for group in groups:
        shape = (parts[first].shape[0] // size, parts[first].shape[1])
        outs.append(jax.ShapeDtypeStruct(shape if group == 1 else (group,) + shape, jnp.float32))
        first += group
    blocks = [(p.shape[0] // chips, p.shape[1] // 2) for p in parts]
    scratch = [pltpu.VMEM((chips,) + b, jnp.bfloat16) for b in blocks] * 2
    scratch += [pltpu.VMEM((chips - 1,) + b, jnp.bfloat16) for b in blocks]
    scratch += [pltpu.VMEM(b, jnp.float32) for b in blocks]
    if gathers:
        scratch += [pltpu.SemaphoreType.DMA((gathers,))]
        scratch += [pltpu.SemaphoreType.DMA((gathers, chips))] * 4
    if swaps:
        scratch += [pltpu.SemaphoreType.DMA((swaps,))] * 2
    if scatters:
        scratch += [pltpu.SemaphoreType.DMA((scatters, chips))] * 5
        scratch += [pltpu.SemaphoreType.DMA((scatters, 2)), pltpu.SemaphoreType.DMA((scatters,))]
    moved = sum(s.size * 2 * size for s in shards) + sum(p.size * 2 for p in parts)
    return list(
        pl.pallas_call(
            functools.partial(ring_kernel, chips, gathers, swaps, tuple(groups)),
            out_shape=outs,
            in_specs=[pl.BlockSpec(memory_space=pltpu.VMEM)] * gathers
            + [pl.BlockSpec(memory_space=pl.ANY)] * (swaps + scatters),
            out_specs=[pl.BlockSpec(memory_space=pl.ANY)] * len(outs),
            scratch_shapes=scratch,
            compiler_params=pltpu.CompilerParams(
                collective_id=call_id, has_side_effects=True, vmem_limit_bytes=VMEM_LIMIT
            ),
            cost_estimate=pl.CostEstimate(flops=0, bytes_accessed=moved, transcendentals=0),
        )(*shards, *sends, *parts)
    )


def feed_kernel(
    chips,
    tile,
    up_shard,
    down_shard,
    normed_ref,
    cot_ref,
    gate_full,
    up_full,
    down_full,
    rows_out,
    gate_out,
    up_out,
    hidden_out,
    term_out,
    rows,
    weights,
    gates,
    ups,
    hiddens,
    terms,
    keep_sem,
    give_sem,
    got_sem,
    lend_sem,
    lent_sem,
    swap_sem,
    load_sem,
    gate_sem,
    up_sem,
    hidden_sem,
    term_sem,
):
    device = lax.axis_index("dp")
    chip, core = device // 2, device % 2
    row, side = chip // 2, chip % 2
    spot, way = row + side * (chips - 1 - 2 * row), 1 - 2 * core
    partner = device + way
    after = chip_at((spot + 1) % chips, chips)
    before = chip_at((spot + chips - 1) % chips, chips)
    source = chip_at((spot + chips - way) % chips, chips)
    target = chip_at((spot + chips + way) % chips, chips) * 2 + core
    other = 1 - lax.axis_index("mp")
    barrier = pltpu.get_barrier_semaphore()
    for who in (source * 2, source * 2 + 1, partner):
        pl.semaphore_signal(barrier, inc=1, device_id={"dp": who}, device_id_type=MESH)
    pl.semaphore_signal(barrier, inc=1, device_id={"mp": other}, device_id_type=MESH)
    pl.semaphore_wait(barrier, 4)

    unit, wide = up_shard.shape
    tiles = wide // tile
    first = (wide // 256 + 1) // 2 * 256
    columns = (pl.ds(0, first), pl.ds(first, wide - first))
    shards = [ref.at[:, at] for ref in (up_shard, down_shard) for at in columns]
    fulls = [ref.at[:, at] for ref in (up_full, down_full) for at in columns]
    halves = [first // 2, (wide - first) // 2] * 2
    half_rows = normed_ref.shape[0]

    def own(i, half):
        at = slice(None) if half is None else pl.ds(half * halves[i], halves[i])
        return shards[i].at[:, at], fulls[i].at[span(device * unit, unit), at]

    def sent(i):
        copies = []
        for half, who in ((0, after * 2), (1, before * 2 + 1)):
            src, dst = own(i, half)
            copies.append(remote(src, dst, give_sem.at[i, half], got_sem.at[i, 1], who))
        return copies

    def shared(i):
        src, dst = own(i, None)
        return [
            remote(src, dst, lend_sem.at[i, 0], lent_sem.at[i, 0], partner),
            pltpu.make_async_copy(src, dst, keep_sem.at[i]),
        ]

    def block(i, step):
        held = chip_at((spot + 2 * chips - way * step) % chips, chips)
        return fulls[i].at[span(held * 2 * unit, 2 * unit), span(core * halves[i], halves[i])]

    def passed(i, step):
        at = block(i, step)
        return remote(at, at, give_sem.at[i, step + 1], got_sem.at[i, step + 1], target)

    def lent(i, step):
        at = block(i, step)
        return remote(at, at, lend_sem.at[i, step], lent_sem.at[i, step], partner)

    def relay(i, step):
        at = block(i, step)
        remote(at, at, give_sem.at[i, 0], got_sem.at[i, step], target).wait_recv()

        @pl.when(step < chips - 1)
        def _():
            passed(i, step).start()

        lent(i, step).start()

    def settle(i):
        for copy in shared(i):
            copy.wait()
        for copy in sent(i):
            copy.wait_send()

        @pl.loop(1, chips)
        def _(step):
            lent(i, step).wait()

            @pl.when(step < chips - 1)
            def _():
                passed(i, step).wait_send()

    exchange = pltpu.make_async_remote_copy(
        src_ref=normed_ref,
        dst_ref=rows.at[pl.ds(half_rows, half_rows), :],
        send_sem=swap_sem.at[0],
        recv_sem=swap_sem.at[1],
        device_id={"mp": other},
        device_id_type=MESH,
    )
    place = pltpu.make_async_copy(normed_ref, rows.at[pl.ds(0, half_rows), :], swap_sem.at[2])
    record = pltpu.make_async_copy(rows, rows_out, swap_sem.at[3])

    def load(ref, t):
        return pltpu.make_async_copy(
            ref.at[:, span(t * tile, tile)], weights.at[t % 2], load_sem.at[t % 2]
        )

    def store(buffer, out, sem, t):
        at = span(t * tile, tile)
        return pltpu.make_async_copy(buffer.at[:, at], out.at[:, at], sem.at[t])

    def store_term(t):
        return pltpu.make_async_copy(
            terms.at[t % 2], term_out.at[:, span(t * tile, tile)], term_sem.at[t % 2]
        )

    def weight_of(ref, t):
        load(ref, t).wait()

        @pl.when(t + 1 < tiles)
        def _():
            load(ref, t + 1).start()

        return weights[t % 2]

    def gate_tile(t):
        gates[:, span(t * tile, tile)] = jnp.dot(
            rows[...], weight_of(gate_full, t), preferred_element_type=jnp.float32
        )
        store(gates, gate_out, gate_sem, t).start()

    def up_tile(t):
        at = span(t * tile, tile)
        upward = jnp.dot(rows[...], weight_of(up_full, t), preferred_element_type=jnp.float32)
        ups[:, at] = upward
        store(ups, up_out, up_sem, t).start()
        gate = gates[:, at]
        hidden = (gate * jax.nn.sigmoid(gate) * upward).astype(jnp.bfloat16)
        hiddens[:, at] = hidden
        store(hiddens, hidden_out, hidden_sem, t).start()

        @pl.when(t > 1)
        def _():
            store_term(t - 2).wait()

        terms[t % 2] = jnp.dot(
            cot_ref[...], hidden, preferred_element_type=jnp.float32
        ).astype(jnp.bfloat16)
        store_term(t).start()

    def some(number, start, work):
        @pl.loop(0, number)
        def _(k):
            @pl.when(start + k < tiles)
            def _():
                work(start + k)

    for i in (0, 1):
        for copy in sent(i) + shared(i):
            copy.start()
    exchange.start()
    place.start()
    load(gate_full, 0).start()
    late = chips // 2
    each = -(-tiles // (chips - late))

    @pl.loop(1, chips)
    def _(step):
        relay(0, step)
        relay(1, step)

        @pl.when(step == chips - 2)
        def _():
            for i in (2, 3):
                for copy in sent(i) + shared(i):
                    copy.start()

        @pl.when(step == late)
        def _():
            place.wait()
            exchange.wait()
            record.start()

        @pl.when(step >= late)
        def _():
            some(each, (step - late) * each, gate_tile)

    settle(0)
    settle(1)
    load(up_full, 0).start()
    each = -(-tiles // (chips - 1))
    early = -(-each // 2)

    @pl.loop(1, chips)
    def _(step):
        relay(2, step)
        some(early, (step - 1) * each, up_tile)
        relay(3, step)
        if each > early:
            some(each - early, (step - 1) * each + early, up_tile)

    settle(2)
    settle(3)
    record.wait()

    @pl.loop(0, tiles)
    def _(t):
        store(gates, gate_out, gate_sem, t).wait()
        store(ups, up_out, up_sem, t).wait()
        store(hiddens, hidden_out, hidden_sem, t).wait()

    for t in range(max(tiles - 2, 0), tiles):
        store_term(t).wait()


def feed_call(call_id, up_shard, down_shard, normed_here, cot_turned, gate_full):
    size = lax.axis_size("dp")
    chips = size // 2
    _, wide = up_shard.shape
    depth, tokens = cot_turned.shape
    tile = 256
    tiles = wide // tile
    low, high = jnp.bfloat16, jnp.float32
    kept = pl.BlockSpec(memory_space=pltpu.VMEM)
    far = pl.BlockSpec(memory_space=pl.ANY)
    dma = pltpu.SemaphoreType.DMA
    return pl.pallas_call(
        functools.partial(feed_kernel, chips, tile),
        out_shape=[
            jax.ShapeDtypeStruct((depth, wide), low),
            jax.ShapeDtypeStruct((depth, wide), low),
            jax.ShapeDtypeStruct((tokens, depth), low),
            jax.ShapeDtypeStruct((tokens, wide), high),
            jax.ShapeDtypeStruct((tokens, wide), high),
            jax.ShapeDtypeStruct((tokens, wide), low),
            jax.ShapeDtypeStruct((depth, wide), low),
        ],
        in_specs=[kept, kept, kept, kept, far],
        out_specs=[far] * 7,
        scratch_shapes=[
            pltpu.VMEM((tokens, depth), low),
            pltpu.VMEM((2, depth, tile), low),
            pltpu.VMEM((tokens, wide), high),
            pltpu.VMEM((tokens, wide), high),
            pltpu.VMEM((tokens, wide), low),
            pltpu.VMEM((2, depth, tile), low),
            dma((4,)),
        ]
        + [dma((4, chips + 1))] * 4
        + [dma((4,)), dma((2,)), dma((tiles,)), dma((tiles,)), dma((tiles,)), dma((2,))],
        compiler_params=pltpu.CompilerParams(
            collective_id=call_id, has_side_effects=True, vmem_limit_bytes=VMEM_LIMIT
        ),
        cost_estimate=pl.CostEstimate(
            flops=6 * tokens * depth * wide,
            bytes_accessed=12 * depth * wide + 12 * tokens * wide,
            transcendentals=tokens * wide,
        ),
    )(up_shard, down_shard, normed_here, cot_turned, gate_full)


def back_kernel(
    chips,
    tile,
    cot_ref,
    normed_ref,
    gate_ref,
    up_ref,
    gate_full,
    up_full,
    down_full,
    term_ref,
    gate_out,
    up_out,
    part_out,
    far_out,
    grad_out,
    gate_term_out,
    mine_a,
    mine_b,
    pair_a,
    pair_b,
    ring_a,
    ring_b,
    last_a,
    last_b,
    weights,
    states,
    acts,
    total,
    low,
    turned,
    kept,
    terms,
    load_sem,
    state_sem,
    act_sem,
    term_sem,
    keep_sem,
    swap_sem,
    own_sem,
    pair_send,
    pair_recv,
    send_sem,
    recv_sem,
    last_send,
    last_recv,
):
    device = lax.axis_index("dp")
    chip, core = device // 2, device % 2
    row, side = chip // 2, chip % 2
    spot, way = row + side * (chips - 1 - 2 * row), 1 - 2 * core
    partner = device + way
    source = chip_at((spot + chips - way) % chips, chips)
    target = chip_at((spot + chips + way) % chips, chips) * 2 + core
    other = 1 - lax.axis_index("mp")
    barrier = pltpu.get_barrier_semaphore()
    for who in (source * 2, source * 2 + 1, partner):
        pl.semaphore_signal(barrier, inc=1, device_id={"dp": who}, device_id_type=MESH)
    pl.semaphore_signal(barrier, inc=1, device_id={"mp": other}, device_id_type=MESH)
    pl.semaphore_wait(barrier, 4)

    mine, pair, ring, last = (mine_a, mine_b), (pair_a, pair_b), (ring_a, ring_b), (last_a, last_b)
    wide = gate_ref.shape[1]
    half_rows = part_out.shape[0]
    tiles = wide // tile
    first = (wide // 256 + 1) // 2 * 256
    columns = (pl.ds(0, first), pl.ds(first, wide - first))
    parts = [term_ref.at[:, at] for at in columns]
    outs = [grad_out.at[:, at] for at in columns]

    def own(i, step):
        rows, cols = mine[i].shape[1:]
        here = chip_at((spot + 2 * chips - way * (step + 1)) % chips, chips)
        return pltpu.make_async_copy(
            parts[i].at[span(here * rows, rows), span(core * cols, cols)],
            mine[i].at[step],
            own_sem.at[i, step],
        )

    def trade(i, step):
        rows, cols = mine[i].shape[1:]
        away = chip_at((spot + 2 * chips + way * (step + 1)) % chips, chips)
        return remote(
            parts[i].at[span(away * rows, rows), span((1 - core) * cols, cols)],
            pair[i].at[step],
            pair_send.at[i, step],
            pair_recv.at[i, step],
            partner,
        )

    def onward(i, step):
        return remote(
            mine[i].at[step], ring[i].at[step], send_sem.at[i, step], recv_sem.at[i, step], target
        )

    def ending(i):
        rows, cols = mine[i].shape[1:]
        unit = rows // 2
        place = outs[i].at[:, span(core * cols, cols)]
        return (
            remote(
                last[i].at[span((1 - core) * unit, unit), :],
                place,
                last_send.at[i, 0],
                last_recv.at[i],
                partner,
            ),
            pltpu.make_async_copy(
                last[i].at[span(core * unit, unit), :], place, last_send.at[i, 1]
            ),
        )

    def sum_step(i, step):
        rows = mine[i].shape[1]
        lines = min(rows, 32)
        own(i, step).wait()
        trade(i, step).wait_recv()

        def added(at):
            value = mine[i][step, at, :].astype(jnp.float32)
            return value + pair[i][step, at, :].astype(jnp.float32)

        @pl.when(step == 0)
        def _():
            @pl.loop(0, rows // lines)
            def _(k):
                at = span(k * lines, lines)
                mine[i][step, at, :] = added(at).astype(jnp.bfloat16)

        @pl.when(step > 0)
        def _():
            came = ring[i].at[step - 1]
            remote(came, came, send_sem.at[i, 0], recv_sem.at[i, step - 1], target).wait_recv()

            @pl.when(step < chips - 1)
            def _():
                @pl.loop(0, rows // lines)
                def _(k):
                    at = span(k * lines, lines)
                    value = added(at) + ring[i][step - 1, at, :].astype(jnp.float32)
                    mine[i][step, at, :] = value.astype(jnp.bfloat16)

            @pl.when(step == chips - 1)
            def _():
                @pl.loop(0, rows // lines)
                def _(k):
                    at = span(k * lines, lines)
                    last[i][at, :] = added(at) + ring[i][step - 1, at, :].astype(jnp.float32)

        @pl.when(step < chips - 1)
        def _():
            onward(i, step).start()

        @pl.when(step == chips - 1)
        def _():
            for copy in ending(i):
                copy.start()

    def loads(t):
        at, slot = span(t * tile, tile), t % 2
        copies = [
            pltpu.make_async_copy(ref.at[:, at], weights.at[k, slot], load_sem.at[k, slot])
            for k, ref in enumerate((down_full, gate_full, up_full))
        ]
        return copies + [
            pltpu.make_async_copy(ref.at[:, at], states.at[k, slot], state_sem.at[k, slot])
            for k, ref in enumerate((gate_ref, up_ref))
        ]

    def stores(t):
        at, slot = span(t * tile, tile), t % 2
        return [
            pltpu.make_async_copy(acts.at[k, slot], ref.at[:, at], act_sem.at[k, slot])
            for k, ref in enumerate((gate_out, up_out))
        ]

    def work(t):
        slot = t % 2
        for copy in loads(t):
            copy.wait()

        @pl.when(t + 1 < tiles)
        def _():
            for copy in loads(t + 1):
                copy.start()

        @pl.when(t > 1)
        def _():
            for copy in stores(t - 2):
                copy.wait()

        hidden_grad = jnp.dot(
            cot_ref[...], weights[0, slot], preferred_element_type=jnp.float32
        )
        gate, upward = states[0, slot], states[1, slot]
        sigma = jax.nn.sigmoid(gate)
        gate_act = hidden_grad * upward * sigma * (1.0 + gate * (1.0 - sigma))
        gate_low = gate_act.astype(jnp.bfloat16)
        acts[0, slot] = gate_low
        kept[:, span(t * tile, tile)] = gate_low
        acts[1, slot] = (hidden_grad * gate * sigma).astype(jnp.bfloat16)
        for copy in stores(t):
            copy.start()
        depth = total.shape[1]
        band = depth // 4

        @pl.loop(0, 4)
        def _(k):
            at = span(k * band, band)
            value = total[:, at]
            for which in range(2):
                value = value + lax.dot_general(
                    acts[which, slot],
                    weights[which + 1, slot, at, :],
                    (((1,), (1,)), ((), ())),
                    preferred_element_type=jnp.float32,
                )
            total[:, at] = value

    def store_term(t):
        return pltpu.make_async_copy(
            terms.at[t % 2], gate_term_out.at[:, span(t * tile, tile)], term_sem.at[t % 2]
        )

    def term_work(t):
        @pl.when(t > 1)
        def _():
            store_term(t - 2).wait()

        terms[t % 2] = jnp.dot(
            turned[...], kept[:, span(t * tile, tile)], preferred_element_type=jnp.float32
        ).astype(jnp.bfloat16)
        store_term(t).start()

    def some(number, start, task):
        @pl.loop(0, number)
        def _(k):
            @pl.when((start + k >= 0) & (start + k < tiles))
            def _():
                task(start + k)

    keep = pltpu.make_async_copy(total.at[pl.ds(0, half_rows), :], part_out, keep_sem.at[0])
    exchange = pltpu.make_async_remote_copy(
        src_ref=low,
        dst_ref=far_out,
        send_sem=swap_sem.at[0],
        recv_sem=swap_sem.at[1],
        device_id={"mp": other},
        device_id_type=MESH,
    )

    @pl.loop(0, chips)
    def _(step):
        for i in range(2):
            trade(i, step).start()
            own(i, step).start()

    for copy in loads(0):
        copy.start()
    total[...] = jnp.zeros_like(total)

    @pl.loop(0, normed_ref.shape[1] // 256)
    def _(k):
        turned[span(k * 256, 256), :] = normed_ref[:, span(k * 256, 256)].T

    each = -(-tiles // (chips - 1))
    early = -(-each // 2)
    done = -(-tiles // each)
    rest = -(-tiles // (chips - done))
    half_rest = -(-rest // 2)

    @pl.loop(0, chips)
    def _(step):
        sum_step(0, step)
        some(early, step * each, work)

        @pl.when(step >= done)
        def _():
            some(half_rest, (step - done) * rest, term_work)

        sum_step(1, step)
        if each > early:
            some(each - early, step * each + early, work)
        if rest > half_rest:

            @pl.when(step >= done)
            def _():
                some(rest - half_rest, (step - done) * rest + half_rest, term_work)

        @pl.when(step == done - 1)
        def _():
            low[...] = total[pl.ds(half_rows, half_rows), :].astype(jnp.bfloat16)
            exchange.start()
            keep.start()

    keep.wait()
    exchange.wait()
    for t in range(max(tiles - 2, 0), tiles):
        for copy in stores(t):
            copy.wait()
        store_term(t).wait()
    for i in range(2):
        for copy in ending(i):
            copy.wait()

    @pl.loop(0, chips)
    def _(step):
        for i in range(2):
            trade(i, step).wait_send()

            @pl.when(step < chips - 1)
            def _():
                onward(i, step).wait_send()


def back_call(call_id, cot_rows, normed_two, gate, upward, gate_full, up_full, down_full, down_term):
    size = lax.axis_size("dp")
    chips = size // 2
    tokens, depth = cot_rows.shape
    wide = gate.shape[1]
    tile = 256
    first = (wide // 256 + 1) // 2 * 256
    blocks = [(depth // chips, first // 2), (depth // chips, (wide - first) // 2)]
    low, high = jnp.bfloat16, jnp.float32
    far = pl.BlockSpec(memory_space=pl.ANY)
    dma = pltpu.SemaphoreType.DMA
    return pl.pallas_call(
        functools.partial(back_kernel, chips, tile),
        out_shape=[
            jax.ShapeDtypeStruct((tokens, wide), low),
            jax.ShapeDtypeStruct((tokens, wide), low),
            jax.ShapeDtypeStruct((tokens // 2, depth), high),
            jax.ShapeDtypeStruct((tokens // 2, depth), low),
            jax.ShapeDtypeStruct((depth // size, wide), high),
            jax.ShapeDtypeStruct((depth, wide), low),
        ],
        in_specs=[pl.BlockSpec(memory_space=pltpu.VMEM)] * 2 + [far] * 6,
        out_specs=[far] * 6,
        scratch_shapes=[pltpu.VMEM((chips,) + b, low) for b in blocks] * 2
        + [pltpu.VMEM((chips - 1,) + b, low) for b in blocks]
        + [pltpu.VMEM(b, high) for b in blocks]
        + [
            pltpu.VMEM((3, 2, depth, tile), low),
            pltpu.VMEM((2, 2, tokens, tile), high),
            pltpu.VMEM((2, 2, tokens, tile), low),
            pltpu.VMEM((tokens, depth), high),
            pltpu.VMEM((tokens // 2, depth), low),
            pltpu.VMEM((depth, tokens), low),
            pltpu.VMEM((tokens, wide), low),
            pltpu.VMEM((2, depth, tile), low),
            dma((3, 2)),
            dma((2, 2)),
            dma((2, 2)),
            dma((2,)),
            dma((1,)),
            dma((2,)),
        ]
        + [dma((2, chips))] * 5
        + [dma((2, 2)), dma((2,))],
        compiler_params=pltpu.CompilerParams(
            collective_id=call_id, has_side_effects=True, vmem_limit_bytes=VMEM_LIMIT
        ),
        cost_estimate=pl.CostEstimate(
            flops=8 * tokens * depth * wide,
            bytes_accessed=8 * depth * wide + 12 * tokens * wide,
            transcendentals=tokens * wide,
        ),
    )(cot_rows, normed_two, gate, upward, gate_full, up_full, down_full, down_term)


def layer_norm(values, norm_gain, norm_shift):
    center = values - jnp.mean(values, axis=-1, keepdims=True)
    inverse = lax.rsqrt(jnp.mean(center * center, axis=-1, keepdims=True) + EPS)
    scaled = center * inverse
    return (scaled * norm_gain + norm_shift, scaled, inverse)


def norm_back(grads, scaled, inverse, norm_gain):
    weighted = grads * norm_gain
    return inverse * (
        weighted
        - jnp.mean(weighted, axis=-1, keepdims=True)
        - scaled * jnp.mean(weighted * scaled, axis=-1, keepdims=True)
    )


def rotary_tables(segments, places, rotary_dims):
    earlier = (segments[None, :] < segments[:, None]).astype(jnp.int32)
    position = (places - jnp.sum(earlier, axis=1)).astype(jnp.float32)
    half_dims = rotary_dims // 2
    frequency = BASE ** (-2.0 * jnp.arange(half_dims, dtype=jnp.float32) / rotary_dims)
    angles = position[:, None] * frequency[None, :]
    return (jnp.cos(angles), jnp.sin(angles))


def rotate(values, cosine, sine_table, rotary_dims, turn_sign):
    half_dims = rotary_dims // 2
    leading = values[..., :half_dims]
    trailing = values[..., half_dims:rotary_dims]
    cos_rows = cosine[:, None, :]
    sin_rows = turn_sign * sine_table[:, None, :]
    return jnp.concatenate(
        [
            leading * cos_rows - trailing * sin_rows,
            trailing * cos_rows + leading * sin_rows,
            values[..., rotary_dims:],
        ],
        axis=-1,
    )


def masked_scores(query, key_rot, allowed, score_scale):
    scores = (
        jnp.einsum("qhd,khd->hqk", query, key_rot, preferred_element_type=jnp.float32) * score_scale
    )
    return jnp.where(allowed[None], scores, NEG)


def swap(values):
    return lax.ppermute(values, "mp", [(0, 1), (1, 0)])


def half_sum(part):
    half = part.shape[0] // 2
    other = swap(part[half:].astype(jnp.bfloat16))
    return part[:half] + other.astype(jnp.float32)


def grow(rows):
    return jnp.concatenate([rows, swap(rows)], axis=0)


def scatter(term, axis):
    return lax.psum_scatter(term, "dp", scatter_dimension=axis, tiled=True).astype(jnp.float32)


def body(
    inputs,
    segment_ids,
    norm1_gain,
    norm1_shift,
    qkv_weight,
    qkv_bias,
    out_weight,
    norm2_gain,
    norm2_shift,
    gate_weight,
    up_weight,
    down_weight,
    cotangent,
):
    score_scale = HEAD_DIM ** (-0.5)
    rows_here = inputs.shape[0]
    width = inputs.shape[1]
    *qkv_full, out_turned, far_inputs, far_cot = ring_call(
        0,
        shards=[qkv_weight[0], qkv_weight[1], qkv_weight[2], out_weight.T],
        sends=[inputs, cotangent],
    )
    input_rows = jnp.concatenate([inputs, far_inputs], axis=0)
    cot_rows = jnp.concatenate([cotangent, far_cot], axis=0)
    gate_weight, out_turned = lax.optimization_barrier((gate_weight, out_turned))
    gate_full = lax.all_gather(gate_weight, "dp", axis=0, tiled=True)
    stream_rows = input_rows.astype(jnp.float32)
    stream = stream_rows[:rows_here]
    normed_wide, scaled_rows, inverse_rows = layer_norm(stream_rows, norm1_gain, norm1_shift)
    normed_one = normed_wide.astype(jnp.bfloat16)
    scaled_one = scaled_rows[:rows_here]
    inverse_one = inverse_rows[:rows_here]
    seq_len = normed_one.shape[0]
    local_width = qkv_full[0].shape[1]
    head_count = local_width // HEAD_DIM
    turn = lax.axis_index("mp") * rows_here
    segments = jnp.roll(segment_ids[0], -turn)
    places = jnp.roll(jnp.arange(seq_len, dtype=jnp.int32), -turn)
    allowed = (places[None, :] <= places[:, None]) & (segments[:, None] == segments[None, :])
    cosine, sine_table = rotary_tables(segments, places, ROT)
    shaped = [
        (jnp.dot(normed_one, full, preferred_element_type=jnp.float32) + bias).reshape(
            seq_len, head_count, HEAD_DIM
        )
        for full, bias in zip(qkv_full, qkv_bias)
    ]
    query = rotate(shaped[0], cosine, sine_table, ROT, 1.0).astype(jnp.bfloat16)
    key_rot = rotate(shaped[1], cosine, sine_table, ROT, 1.0).astype(jnp.bfloat16)
    value = shaped[2].astype(jnp.bfloat16)
    scores = masked_scores(query, key_rot, allowed, score_scale)
    row_max = jnp.max(scores, axis=-1, keepdims=True)
    exponent = jnp.exp(scores - row_max)
    row_total = jnp.sum(exponent, axis=-1, keepdims=True)
    log_total = row_max + jnp.log(row_total)
    probs_low = (exponent / row_total).astype(jnp.bfloat16)
    mixed_heads = jnp.einsum(
        "hqk,khd->qhd", probs_low, value, preferred_element_type=jnp.float32
    ).astype(jnp.bfloat16)
    mixed = mixed_heads.reshape(seq_len, local_width)
    branch = jnp.dot(mixed, out_turned.T, preferred_element_type=jnp.float32)
    middle = stream + half_sum(branch)
    normed_wide2, scaled_two, inverse_two = layer_norm(middle, norm2_gain, norm2_shift)
    normed_here = normed_wide2.astype(jnp.bfloat16)
    up_full, down_turned, normed_two, gate, upward, hidden, down_term = feed_call(
        1, up_weight, down_weight.T, normed_here, cot_rows.T, gate_full
    )
    _, up_act, part_here, part_far, down_grad_turned, gate_term = back_call(
        3, cot_rows, normed_two, gate, upward, gate_full, up_full, down_turned, down_term
    )
    down_weight_grad = down_grad_turned.T
    normed_two_grad = part_here + part_far.astype(jnp.float32)
    gate_weight_grad = scatter(gate_term, 0)
    gain_two = jnp.sum(normed_two_grad * scaled_two, axis=0)
    shift_two = jnp.sum(normed_two_grad, axis=0)
    middle_grad = cotangent.astype(jnp.float32) + norm_back(
        normed_two_grad, scaled_two, inverse_two, norm2_gain
    )
    middle_low, hidden, up_act = lax.optimization_barrier(
        (middle_grad.astype(jnp.bfloat16), hidden, up_act)
    )
    middle_rows = grow(middle_low)
    up_term = jnp.dot(normed_two.T, up_act, preferred_element_type=jnp.float32)
    feed_part = jnp.dot(hidden, down_turned.T, preferred_element_type=jnp.float32)
    out_term = jnp.dot(middle_rows.T, mixed, preferred_element_type=jnp.float32)
    mixed_grad = (
        jnp.dot(middle_rows, out_turned, preferred_element_type=jnp.float32)
        .astype(jnp.bfloat16)
        .reshape(seq_len, head_count, HEAD_DIM)
    )
    probs_wide = jnp.exp(scores - log_total)
    value_grad = jnp.einsum(
        "hqk,qhd->khd",
        probs_wide.astype(jnp.bfloat16),
        mixed_grad,
        preferred_element_type=jnp.float32,
    )
    prob_grad = jnp.einsum("qhd,khd->hqk", mixed_grad, value, preferred_element_type=jnp.float32)
    row_delta = jnp.transpose(
        jnp.sum(mixed_grad.astype(jnp.float32) * mixed_heads.astype(jnp.float32), axis=-1)
    )
    score_grad = (probs_wide * (prob_grad - row_delta[:, :, None]) * score_scale).astype(
        jnp.bfloat16
    )
    query_grad = jnp.einsum("hqk,khd->qhd", score_grad, key_rot, preferred_element_type=jnp.float32)
    key_grad = jnp.einsum("hqk,qhd->khd", score_grad, query, preferred_element_type=jnp.float32)
    query_back = rotate(query_grad, cosine, sine_table, ROT, -1.0)
    key_back = rotate(key_grad, cosine, sine_table, ROT, -1.0)
    proj_grad = [
        part.reshape(seq_len, local_width) for part in (query_back, key_back, value_grad)
    ]
    rotated_cols = jnp.arange(local_width, dtype=jnp.int32) % HEAD_DIM < ROT
    bias_sums = [jnp.sum(part, axis=0) for part in proj_grad]
    bias_term = [bias_sums[0], jnp.where(rotated_cols, bias_sums[1], 0.0), bias_sums[2]]
    proj_low = [part.astype(jnp.bfloat16) for part in proj_grad]
    normed_one_part = jnp.zeros((), jnp.float32)
    for part, full in zip(proj_low, qkv_full):
        normed_one_part = normed_one_part + jnp.dot(
            part, full.T, preferred_element_type=jnp.float32
        )
    gain_one = jnp.sum(normed_one_part * scaled_rows, axis=0)
    shift_one = jnp.sum(normed_one_part, axis=0)
    norm_sums = jnp.concatenate([gain_one, shift_one, gain_two, shift_two])
    norm_sums = norm_sums + swap(norm_sums)
    sums = jnp.concatenate([norm_sums] + bias_term)
    spare = -sums.size % (8 * 256)
    qkv_term = [
        jnp.dot(normed_one.T, part, preferred_element_type=jnp.float32) for part in proj_low
    ]
    all_sums, far_part, far_feed, up_weight_grad, out_grad_turned, qkv_weight_grad = ring_call(
        2,
        shards=[jnp.pad(sums, (0, spare)).reshape(8, -1)],
        sends=[part[rows_here:].astype(jnp.bfloat16) for part in (normed_one_part, feed_part)],
        parts=[term.astype(jnp.bfloat16) for term in [up_term, out_term] + qkv_term],
        groups=[1, 1, 3],
    )
    out_weight_grad = out_grad_turned.T
    normed_one_grad = normed_one_part[:rows_here] + far_part.astype(jnp.float32)
    feed = feed_part[:rows_here] + far_feed.astype(jnp.float32)
    output = (middle + feed).astype(jnp.bfloat16)
    all_sums = jnp.sum(all_sums.reshape(-1, 8, all_sums.shape[1]), axis=0).reshape(-1)
    gain_one, shift_one, gain_two, shift_two = all_sums[: 4 * width].reshape(4, width)
    qkv_bias_grad = all_sums[4 * width : sums.size].reshape(3, local_width)
    input_grad = middle_grad + norm_back(normed_one_grad, scaled_one, inverse_one, norm1_gain)
    return (
        output,
        input_grad,
        gain_one,
        shift_one,
        qkv_weight_grad,
        qkv_bias_grad,
        out_weight_grad,
        gain_two,
        shift_two,
        gate_weight_grad,
        up_weight_grad,
        down_weight_grad,
    )


def solution(mesh):
    in_specs = (
        P(("dp", "mp"), None),
        P("dp", None),
        P(),
        P(),
        P(None, "dp", "mp"),
        P(None, "mp"),
        P("mp", "dp"),
        P(),
        P(),
        P("dp", "mp"),
        P("dp", "mp"),
        P("mp", "dp"),
        P(("dp", "mp"), None),
    )
    out_specs = (
        P(("dp", "mp"), None),
        P(("dp", "mp"), None),
        P(),
        P(),
        P(None, "dp", "mp"),
        P(None, "mp"),
        P("mp", "dp"),
        P(),
        P(),
        P("dp", "mp"),
        P("dp", "mp"),
        P("mp", "dp"),
    )
    return jax.shard_map(body, mesh=mesh, in_specs=in_specs, out_specs=out_specs, check_vma=False)
```

```python
import functools

import jax
import jax.numpy as jnp
from jax import lax
from jax.experimental import pallas as pl
from jax.experimental.pallas import tpu as pltpu
from jax.sharding import PartitionSpec as P


HEAD_DIM = 64
ROT = 16


NEG = -1e30
EPS = 1e-05
BASE = 10000.0

MESH = pl.DeviceIdType.MESH
VMEM_LIMIT = 60 * 1024 * 1024


def chip_at(spot, chips):
    side = spot // (chips // 2)
    return (spot + side * (chips - 1 - 2 * spot)) * 2 + side


def span(start, size):
    return pl.ds(pl.multiple_of(start, size), size)


def remote(src, dst, send, recv, who):
    return pltpu.make_async_remote_copy(
        src_ref=src,
        dst_ref=dst,
        send_sem=send,
        recv_sem=recv,
        device_id={"dp": who},
        device_id_type=MESH,
    )


def ring_kernel(chips, bundles, swaps, groups, *refs):
    refs = list(refs)
    scatters, gathers = sum(groups), sum(bundles)

    def take(number):
        taken = refs[:number]
        del refs[:number]
        return taken

    bundled, sends, parts = take(len(bundles)), take(swaps), take(scatters)
    shards = []
    for bundle, ref in zip(bundles, bundled):
        shards += [ref] if bundle == 1 else [ref.at[j] for j in range(bundle)]
    fulls, gets, grouped = take(gathers), take(swaps), take(len(groups))
    outs = []
    for group, out in zip(groups, grouped):
        outs += [out] if group == 1 else [out.at[j] for j in range(group)]
    mine, pair, ring, last = take(scatters), take(scatters), take(scatters), take(scatters)
    if gathers:
        keep_sem, give_sem, got_sem, lend_sem, lent_sem = take(5)
    if swaps:
        swap_send, swap_recv = take(2)
    if scatters:
        load_sem, pair_send, pair_recv, send_sem, recv_sem, last_send, last_recv = take(7)
    device = lax.axis_index("dp")
    chip, core = device // 2, device % 2
    row, side = chip // 2, chip % 2
    spot, way = row + side * (chips - 1 - 2 * row), 1 - 2 * core
    partner = device + way
    after = chip_at((spot + 1) % chips, chips)
    before = chip_at((spot + chips - 1) % chips, chips)
    source = chip_at((spot + chips - way) % chips, chips)
    target = chip_at((spot + chips + way) % chips, chips) * 2 + core
    barrier = pltpu.get_barrier_semaphore()
    for who in (source * 2, source * 2 + 1, partner):
        pl.semaphore_signal(barrier, inc=1, device_id={"dp": who}, device_id_type=MESH)
    if swaps:
        other = 1 - lax.axis_index("mp")
        pl.semaphore_signal(barrier, inc=1, device_id={"mp": other}, device_id_type=MESH)
    pl.semaphore_wait(barrier, 4 if swaps else 3)
    ends = []

    def begin(copy, end):
        copy.start()
        ends.append(end)
        return copy

    for i in range(swaps):
        copy = pltpu.make_async_remote_copy(
            src_ref=sends[i],
            dst_ref=gets[i],
            send_sem=swap_send.at[i],
            recv_sem=swap_recv.at[i],
            device_id={"mp": other},
            device_id_type=MESH,
        )
        begin(copy, copy.wait)
    for i in range(gathers):
        unit, cols = shards[i].shape[0], shards[i].shape[1] // 2
        own = fulls[i].at[span(device * unit, unit), :]
        for half, who in ((0, after * 2), (1, before * 2 + 1)):
            copy = remote(
                shards[i].at[:, pl.ds(half * cols, cols)],
                fulls[i].at[span(device * unit, unit), pl.ds(half * cols, cols)],
                give_sem.at[i, half],
                got_sem.at[i, core],
                who,
            )
            begin(copy, copy.wait_send)
        copy = remote(shards[i], own, lend_sem.at[i, 0], lent_sem.at[i, 0], partner)
        begin(copy, copy.wait)
        copy = pltpu.make_async_copy(shards[i], own, keep_sem.at[i])
        begin(copy, copy.wait)

    loads, pairs = {}, {}
    for step in range(chips):
        away = chip_at((spot + 2 * chips + way * (step + 1)) % chips, chips)
        here = chip_at((spot + 2 * chips - way * (step + 1)) % chips, chips)
        for i in range(scatters):
            rows, cols = mine[i].shape[1:]
            copy = remote(
                parts[i].at[span(away * rows, rows), span((1 - core) * cols, cols)],
                pair[i].at[step],
                pair_send.at[i, step],
                pair_recv.at[i, step],
                partner,
            )
            pairs[step, i] = begin(copy, copy.wait_send)
            loads[step, i] = pltpu.make_async_copy(
                parts[i].at[span(here * rows, rows), span(core * cols, cols)],
                mine[i].at[step],
                load_sem.at[i, step],
            )
            loads[step, i].start()

    def gather_step(i, step):
        held = chip_at((spot + 2 * chips - way * step) % chips, chips)
        unit, cols = shards[i].shape[0], shards[i].shape[1] // 2
        block = fulls[i].at[span(held * 2 * unit, 2 * unit), span(core * cols, cols)]
        if step == 1:
            for sender in range(2):
                piece = fulls[i].at[span((held * 2 + sender) * unit, unit), span(core * cols, cols)]
                remote(piece, piece, give_sem.at[i, 0], got_sem.at[i, sender], target).wait_recv()
        else:
            remote(block, block, give_sem.at[i, 0], got_sem.at[i, step], target).wait_recv()
        if step < chips - 1:
            copy = remote(block, block, give_sem.at[i, step + 1], got_sem.at[i, step + 1], target)
            begin(copy, copy.wait_send)
        copy = remote(block, block, lend_sem.at[i, step], lent_sem.at[i, step], partner)
        begin(copy, copy.wait)

    def scatter_step(i, step):
        rows, cols = mine[i].shape[1:]
        lines = min(rows, 32)
        loads[step, i].wait()
        pairs[step, i].wait_recv()
        if step > 0:
            came = ring[i].at[step - 1]
            remote(came, came, send_sem.at[i, 0], recv_sem.at[i, step - 1], target).wait_recv()

        @pl.loop(0, rows // lines)
        def _(k):
            at = span(k * lines, lines)
            total = mine[i][step, at, :].astype(jnp.float32)
            total = total + pair[i][step, at, :].astype(jnp.float32)
            if step > 0:
                total = total + ring[i][step - 1, at, :].astype(jnp.float32)
            if step < chips - 1:
                mine[i][step, at, :] = total.astype(jnp.bfloat16)
            else:
                last[i][at, :] = total

        if step < chips - 1:
            copy = remote(
                mine[i].at[step], ring[i].at[step], send_sem.at[i, step], recv_sem.at[i, step], target
            )
            begin(copy, copy.wait_send)
        else:
            unit = rows // 2
            place = outs[i].at[:, span(core * cols, cols)]
            copy = remote(
                last[i].at[span((1 - core) * unit, unit), :],
                place,
                last_send.at[i, 0],
                last_recv.at[i],
                partner,
            )
            begin(copy, copy.wait)
            copy = pltpu.make_async_copy(
                last[i].at[span(core * unit, unit), :], place, last_send.at[i, 1]
            )
            begin(copy, copy.wait)

    for step in range(chips):
        for i in range(gathers):
            if step > 0:
                gather_step(i, step)
        for i in range(scatters):
            scatter_step(i, step)
    for end in ends:
        end()


def ring_call(call_id, shards=(), sends=(), parts=(), groups=()):
    size = lax.axis_size("dp")
    chips = size // 2
    bundles = [1 if s.ndim == 2 else s.shape[0] for s in shards]
    gathers, swaps, scatters = sum(bundles), len(sends), len(parts)
    outs = []
    for bundle, s in zip(bundles, shards):
        rows, cols = s.shape[-2:]
        outs += [jax.ShapeDtypeStruct((rows * size, cols), s.dtype)] * bundle
    outs += [jax.ShapeDtypeStruct(s.shape, s.dtype) for s in sends]
    first = 0
    for group in groups:
        shape = (parts[first].shape[0] // size, parts[first].shape[1])
        outs.append(jax.ShapeDtypeStruct(shape if group == 1 else (group,) + shape, jnp.float32))
        first += group
    blocks = [(p.shape[0] // chips, p.shape[1] // 2) for p in parts]
    scratch = [pltpu.VMEM((chips,) + b, jnp.bfloat16) for b in blocks] * 2
    scratch += [pltpu.VMEM((chips - 1,) + b, jnp.bfloat16) for b in blocks]
    scratch += [pltpu.VMEM(b, jnp.float32) for b in blocks]
    if gathers:
        scratch += [pltpu.SemaphoreType.DMA((gathers,))]
        scratch += [pltpu.SemaphoreType.DMA((gathers, chips))] * 4
    if swaps:
        scratch += [pltpu.SemaphoreType.DMA((swaps,))] * 2
    if scatters:
        scratch += [pltpu.SemaphoreType.DMA((scatters, chips))] * 5
        scratch += [pltpu.SemaphoreType.DMA((scatters, 2)), pltpu.SemaphoreType.DMA((scatters,))]
    moved = sum(s.size * 2 * size for s in shards) + sum(p.size * 2 for p in parts)
    return list(
        pl.pallas_call(
            functools.partial(ring_kernel, chips, tuple(bundles), swaps, tuple(groups)),
            out_shape=outs,
            in_specs=[pl.BlockSpec(memory_space=pltpu.VMEM)] * len(shards)
            + [pl.BlockSpec(memory_space=pl.ANY)] * (swaps + scatters),
            out_specs=[pl.BlockSpec(memory_space=pl.ANY)] * len(outs),
            scratch_shapes=scratch,
            compiler_params=pltpu.CompilerParams(
                collective_id=call_id, has_side_effects=True, vmem_limit_bytes=VMEM_LIMIT
            ),
            cost_estimate=pl.CostEstimate(flops=0, bytes_accessed=moved, transcendentals=0),
        )(*shards, *sends, *parts)
    )


def feed_kernel(
    chips,
    tile,
    up_shard,
    down_shard,
    normed_ref,
    cot_ref,
    gate_full,
    up_full,
    down_full,
    rows_out,
    gate_out,
    up_out,
    hidden_out,
    term_out,
    rows,
    weights,
    gates,
    ups,
    hiddens,
    terms,
    keep_sem,
    give_sem,
    got_sem,
    lend_sem,
    lent_sem,
    swap_sem,
    load_sem,
    gate_sem,
    up_sem,
    hidden_sem,
    term_sem,
):
    device = lax.axis_index("dp")
    chip, core = device // 2, device % 2
    row, side = chip // 2, chip % 2
    spot, way = row + side * (chips - 1 - 2 * row), 1 - 2 * core
    partner = device + way
    after = chip_at((spot + 1) % chips, chips)
    before = chip_at((spot + chips - 1) % chips, chips)
    source = chip_at((spot + chips - way) % chips, chips)
    target = chip_at((spot + chips + way) % chips, chips) * 2 + core
    other = 1 - lax.axis_index("mp")
    barrier = pltpu.get_barrier_semaphore()
    for who in (source * 2, source * 2 + 1, partner):
        pl.semaphore_signal(barrier, inc=1, device_id={"dp": who}, device_id_type=MESH)
    pl.semaphore_signal(barrier, inc=1, device_id={"mp": other}, device_id_type=MESH)
    pl.semaphore_wait(barrier, 4)

    unit, wide = up_shard.shape
    tiles = wide // tile
    first = (wide // 256 + 1) // 2 * 256
    columns = (pl.ds(0, first), pl.ds(first, wide - first))
    shards = [ref.at[:, at] for ref in (up_shard, down_shard) for at in columns]
    fulls = [ref.at[:, at] for ref in (up_full, down_full) for at in columns]
    halves = [first // 2, (wide - first) // 2] * 2
    half_rows = normed_ref.shape[0]

    def own(i, half):
        at = slice(None) if half is None else pl.ds(half * halves[i], halves[i])
        return shards[i].at[:, at], fulls[i].at[span(device * unit, unit), at]

    def sent(i):
        copies = []
        for half, who in ((0, after * 2), (1, before * 2 + 1)):
            src, dst = own(i, half)
            copies.append(remote(src, dst, give_sem.at[i, half], got_sem.at[i, 1], who))
        return copies

    def shared(i):
        src, dst = own(i, None)
        return [
            remote(src, dst, lend_sem.at[i, 0], lent_sem.at[i, 0], partner),
            pltpu.make_async_copy(src, dst, keep_sem.at[i]),
        ]

    def block(i, step):
        held = chip_at((spot + 2 * chips - way * step) % chips, chips)
        return fulls[i].at[span(held * 2 * unit, 2 * unit), span(core * halves[i], halves[i])]

    def passed(i, step):
        at = block(i, step)
        return remote(at, at, give_sem.at[i, step + 1], got_sem.at[i, step + 1], target)

    def lent(i, step):
        at = block(i, step)
        return remote(at, at, lend_sem.at[i, step], lent_sem.at[i, step], partner)

    def relay(i, step):
        at = block(i, step)
        remote(at, at, give_sem.at[i, 0], got_sem.at[i, step], target).wait_recv()

        @pl.when(step < chips - 1)
        def _():
            passed(i, step).start()

        lent(i, step).start()

    def settle(i):
        for copy in shared(i):
            copy.wait()
        for copy in sent(i):
            copy.wait_send()

        @pl.loop(1, chips)
        def _(step):
            lent(i, step).wait()

            @pl.when(step < chips - 1)
            def _():
                passed(i, step).wait_send()

    exchange = pltpu.make_async_remote_copy(
        src_ref=normed_ref,
        dst_ref=rows.at[pl.ds(half_rows, half_rows), :],
        send_sem=swap_sem.at[0],
        recv_sem=swap_sem.at[1],
        device_id={"mp": other},
        device_id_type=MESH,
    )
    place = pltpu.make_async_copy(normed_ref, rows.at[pl.ds(0, half_rows), :], swap_sem.at[2])
    record = pltpu.make_async_copy(rows, rows_out, swap_sem.at[3])

    def load(ref, t):
        return pltpu.make_async_copy(
            ref.at[:, span(t * tile, tile)], weights.at[t % 2], load_sem.at[t % 2]
        )

    def store(buffer, out, sem, t):
        at = span(t * tile, tile)
        return pltpu.make_async_copy(buffer.at[:, at], out.at[:, at], sem.at[t])

    def store_term(t):
        return pltpu.make_async_copy(
            terms.at[t % 2], term_out.at[:, span(t * tile, tile)], term_sem.at[t % 2]
        )

    def weight_of(ref, t):
        load(ref, t).wait()

        @pl.when(t + 1 < tiles)
        def _():
            load(ref, t + 1).start()

        return weights[t % 2]

    def gate_tile(t):
        gates[:, span(t * tile, tile)] = jnp.dot(
            rows[...], weight_of(gate_full, t), preferred_element_type=jnp.float32
        )
        store(gates, gate_out, gate_sem, t).start()

    def up_tile(t):
        at = span(t * tile, tile)
        upward = jnp.dot(rows[...], weight_of(up_full, t), preferred_element_type=jnp.float32)
        ups[:, at] = upward
        store(ups, up_out, up_sem, t).start()
        gate = gates[:, at]
        hidden = (gate * jax.nn.sigmoid(gate) * upward).astype(jnp.bfloat16)
        hiddens[:, at] = hidden
        store(hiddens, hidden_out, hidden_sem, t).start()

        @pl.when(t > 1)
        def _():
            store_term(t - 2).wait()

        terms[t % 2] = jnp.dot(
            cot_ref[...], hidden, preferred_element_type=jnp.float32
        ).astype(jnp.bfloat16)
        store_term(t).start()

    def some(number, start, work):
        @pl.loop(0, number)
        def _(k):
            @pl.when(start + k < tiles)
            def _():
                work(start + k)

    for i in (0, 1):
        for copy in sent(i) + shared(i):
            copy.start()
    exchange.start()
    place.start()
    load(gate_full, 0).start()
    late = chips // 2
    each = -(-tiles // (chips - late))

    @pl.loop(1, chips)
    def _(step):
        relay(0, step)
        relay(1, step)

        @pl.when(step == chips - 2)
        def _():
            for i in (2, 3):
                for copy in sent(i) + shared(i):
                    copy.start()

        @pl.when(step == late)
        def _():
            place.wait()
            exchange.wait()
            record.start()

        @pl.when(step >= late)
        def _():
            some(each, (step - late) * each, gate_tile)

    settle(0)
    settle(1)
    load(up_full, 0).start()
    each = -(-tiles // (chips - 1))
    early = -(-each // 2)

    @pl.loop(1, chips)
    def _(step):
        relay(2, step)
        some(early, (step - 1) * each, up_tile)
        relay(3, step)
        if each > early:
            some(each - early, (step - 1) * each + early, up_tile)

    settle(2)
    settle(3)
    record.wait()

    @pl.loop(0, tiles)
    def _(t):
        store(gates, gate_out, gate_sem, t).wait()
        store(ups, up_out, up_sem, t).wait()
        store(hiddens, hidden_out, hidden_sem, t).wait()

    for t in range(max(tiles - 2, 0), tiles):
        store_term(t).wait()


def feed_call(call_id, up_shard, down_shard, normed_here, cot_turned, gate_full):
    size = lax.axis_size("dp")
    chips = size // 2
    _, wide = up_shard.shape
    depth, tokens = cot_turned.shape
    tile = 256
    tiles = wide // tile
    low, high = jnp.bfloat16, jnp.float32
    kept = pl.BlockSpec(memory_space=pltpu.VMEM)
    far = pl.BlockSpec(memory_space=pl.ANY)
    dma = pltpu.SemaphoreType.DMA
    return pl.pallas_call(
        functools.partial(feed_kernel, chips, tile),
        out_shape=[
            jax.ShapeDtypeStruct((depth, wide), low),
            jax.ShapeDtypeStruct((depth, wide), low),
            jax.ShapeDtypeStruct((tokens, depth), low),
            jax.ShapeDtypeStruct((tokens, wide), high),
            jax.ShapeDtypeStruct((tokens, wide), high),
            jax.ShapeDtypeStruct((tokens, wide), low),
            jax.ShapeDtypeStruct((depth, wide), low),
        ],
        in_specs=[kept, kept, kept, kept, far],
        out_specs=[far] * 7,
        scratch_shapes=[
            pltpu.VMEM((tokens, depth), low),
            pltpu.VMEM((2, depth, tile), low),
            pltpu.VMEM((tokens, wide), high),
            pltpu.VMEM((tokens, wide), high),
            pltpu.VMEM((tokens, wide), low),
            pltpu.VMEM((2, depth, tile), low),
            dma((4,)),
        ]
        + [dma((4, chips + 1))] * 4
        + [dma((4,)), dma((2,)), dma((tiles,)), dma((tiles,)), dma((tiles,)), dma((2,))],
        compiler_params=pltpu.CompilerParams(
            collective_id=call_id, has_side_effects=True, vmem_limit_bytes=VMEM_LIMIT
        ),
        cost_estimate=pl.CostEstimate(
            flops=6 * tokens * depth * wide,
            bytes_accessed=12 * depth * wide + 12 * tokens * wide,
            transcendentals=tokens * wide,
        ),
    )(up_shard, down_shard, normed_here, cot_turned, gate_full)


def back_kernel(
    chips,
    tile,
    cot_ref,
    normed_ref,
    gate_ref,
    up_ref,
    gate_full,
    up_full,
    down_full,
    term_ref,
    gate_out,
    up_out,
    part_out,
    far_out,
    grad_out,
    gate_term_out,
    mine_a,
    mine_b,
    pair_a,
    pair_b,
    ring_a,
    ring_b,
    last_a,
    last_b,
    weights,
    states,
    acts,
    total,
    low,
    turned,
    kept,
    terms,
    load_sem,
    state_sem,
    act_sem,
    term_sem,
    keep_sem,
    swap_sem,
    own_sem,
    pair_send,
    pair_recv,
    send_sem,
    recv_sem,
    last_send,
    last_recv,
):
    device = lax.axis_index("dp")
    chip, core = device // 2, device % 2
    row, side = chip // 2, chip % 2
    spot, way = row + side * (chips - 1 - 2 * row), 1 - 2 * core
    partner = device + way
    source = chip_at((spot + chips - way) % chips, chips)
    target = chip_at((spot + chips + way) % chips, chips) * 2 + core
    other = 1 - lax.axis_index("mp")
    barrier = pltpu.get_barrier_semaphore()
    for who in (source * 2, source * 2 + 1, partner):
        pl.semaphore_signal(barrier, inc=1, device_id={"dp": who}, device_id_type=MESH)
    pl.semaphore_signal(barrier, inc=1, device_id={"mp": other}, device_id_type=MESH)
    pl.semaphore_wait(barrier, 4)

    mine, pair, ring, last = (mine_a, mine_b), (pair_a, pair_b), (ring_a, ring_b), (last_a, last_b)
    wide = gate_ref.shape[1]
    half_rows = part_out.shape[0]
    tiles = wide // tile
    first = (wide // 256 + 1) // 2 * 256
    columns = (pl.ds(0, first), pl.ds(first, wide - first))
    parts = [term_ref.at[:, at] for at in columns]
    outs = [grad_out.at[:, at] for at in columns]

    def own(i, step):
        rows, cols = mine[i].shape[1:]
        here = chip_at((spot + 2 * chips - way * (step + 1)) % chips, chips)
        return pltpu.make_async_copy(
            parts[i].at[span(here * rows, rows), span(core * cols, cols)],
            mine[i].at[step],
            own_sem.at[i, step],
        )

    def trade(i, step):
        rows, cols = mine[i].shape[1:]
        away = chip_at((spot + 2 * chips + way * (step + 1)) % chips, chips)
        return remote(
            parts[i].at[span(away * rows, rows), span((1 - core) * cols, cols)],
            pair[i].at[step],
            pair_send.at[i, step],
            pair_recv.at[i, step],
            partner,
        )

    def onward(i, step):
        return remote(
            mine[i].at[step], ring[i].at[step], send_sem.at[i, step], recv_sem.at[i, step], target
        )

    def ending(i):
        rows, cols = mine[i].shape[1:]
        unit = rows // 2
        place = outs[i].at[:, span(core * cols, cols)]
        return (
            remote(
                last[i].at[span((1 - core) * unit, unit), :],
                place,
                last_send.at[i, 0],
                last_recv.at[i],
                partner,
            ),
            pltpu.make_async_copy(
                last[i].at[span(core * unit, unit), :], place, last_send.at[i, 1]
            ),
        )

    def sum_step(i, step):
        rows = mine[i].shape[1]
        lines = min(rows, 32)
        own(i, step).wait()
        trade(i, step).wait_recv()

        def added(at):
            value = mine[i][step, at, :].astype(jnp.float32)
            return value + pair[i][step, at, :].astype(jnp.float32)

        @pl.when(step == 0)
        def _():
            @pl.loop(0, rows // lines)
            def _(k):
                at = span(k * lines, lines)
                mine[i][step, at, :] = added(at).astype(jnp.bfloat16)

        @pl.when(step > 0)
        def _():
            came = ring[i].at[step - 1]
            remote(came, came, send_sem.at[i, 0], recv_sem.at[i, step - 1], target).wait_recv()

            @pl.when(step < chips - 1)
            def _():
                @pl.loop(0, rows // lines)
                def _(k):
                    at = span(k * lines, lines)
                    value = added(at) + ring[i][step - 1, at, :].astype(jnp.float32)
                    mine[i][step, at, :] = value.astype(jnp.bfloat16)

            @pl.when(step == chips - 1)
            def _():
                @pl.loop(0, rows // lines)
                def _(k):
                    at = span(k * lines, lines)
                    last[i][at, :] = added(at) + ring[i][step - 1, at, :].astype(jnp.float32)

        @pl.when(step < chips - 1)
        def _():
            onward(i, step).start()

        @pl.when(step == chips - 1)
        def _():
            for copy in ending(i):
                copy.start()

    def loads(t):
        at, slot = span(t * tile, tile), t % 2
        copies = [
            pltpu.make_async_copy(ref.at[:, at], weights.at[k, slot], load_sem.at[k, slot])
            for k, ref in enumerate((down_full, gate_full, up_full))
        ]
        return copies + [
            pltpu.make_async_copy(ref.at[:, at], states.at[k, slot], state_sem.at[k, slot])
            for k, ref in enumerate((gate_ref, up_ref))
        ]

    def stores(t):
        at, slot = span(t * tile, tile), t % 2
        return [
            pltpu.make_async_copy(acts.at[k, slot], ref.at[:, at], act_sem.at[k, slot])
            for k, ref in enumerate((gate_out, up_out))
        ]

    def work(t):
        slot = t % 2
        for copy in loads(t):
            copy.wait()

        @pl.when(t + 1 < tiles)
        def _():
            for copy in loads(t + 1):
                copy.start()

        @pl.when(t > 1)
        def _():
            for copy in stores(t - 2):
                copy.wait()

        hidden_grad = jnp.dot(
            cot_ref[...], weights[0, slot], preferred_element_type=jnp.float32
        )
        gate, upward = states[0, slot], states[1, slot]
        sigma = jax.nn.sigmoid(gate)
        gate_act = hidden_grad * upward * sigma * (1.0 + gate * (1.0 - sigma))
        gate_low = gate_act.astype(jnp.bfloat16)
        acts[0, slot] = gate_low
        kept[:, span(t * tile, tile)] = gate_low
        acts[1, slot] = (hidden_grad * gate * sigma).astype(jnp.bfloat16)
        for copy in stores(t):
            copy.start()
        depth = total.shape[1]
        band = depth // 4

        @pl.loop(0, 4)
        def _(k):
            at = span(k * band, band)
            value = total[:, at]
            for which in range(2):
                value = value + lax.dot_general(
                    acts[which, slot],
                    weights[which + 1, slot, at, :],
                    (((1,), (1,)), ((), ())),
                    preferred_element_type=jnp.float32,
                )
            total[:, at] = value

    def store_term(t):
        return pltpu.make_async_copy(
            terms.at[t % 2], gate_term_out.at[:, span(t * tile, tile)], term_sem.at[t % 2]
        )

    def term_work(t):
        @pl.when(t > 1)
        def _():
            store_term(t - 2).wait()

        terms[t % 2] = jnp.dot(
            turned[...], kept[:, span(t * tile, tile)], preferred_element_type=jnp.float32
        ).astype(jnp.bfloat16)
        store_term(t).start()

    def some(number, start, task):
        @pl.loop(0, number)
        def _(k):
            @pl.when((start + k >= 0) & (start + k < tiles))
            def _():
                task(start + k)

    keep = pltpu.make_async_copy(total.at[pl.ds(0, half_rows), :], part_out, keep_sem.at[0])
    exchange = pltpu.make_async_remote_copy(
        src_ref=low,
        dst_ref=far_out,
        send_sem=swap_sem.at[0],
        recv_sem=swap_sem.at[1],
        device_id={"mp": other},
        device_id_type=MESH,
    )

    @pl.loop(0, chips)
    def _(step):
        for i in range(2):
            trade(i, step).start()
            own(i, step).start()

    for copy in loads(0):
        copy.start()
    total[...] = jnp.zeros_like(total)

    @pl.loop(0, normed_ref.shape[1] // 256)
    def _(k):
        turned[span(k * 256, 256), :] = normed_ref[:, span(k * 256, 256)].T

    each = -(-tiles // (chips - 1))
    early = -(-each // 2)
    done = -(-tiles // each)
    rest = -(-tiles // (chips - done))
    half_rest = -(-rest // 2)

    @pl.loop(0, chips)
    def _(step):
        sum_step(0, step)
        some(early, step * each, work)

        @pl.when(step >= done)
        def _():
            some(half_rest, (step - done) * rest, term_work)

        sum_step(1, step)
        if each > early:
            some(each - early, step * each + early, work)
        if rest > half_rest:

            @pl.when(step >= done)
            def _():
                some(rest - half_rest, (step - done) * rest + half_rest, term_work)

        @pl.when(step == done - 1)
        def _():
            low[...] = total[pl.ds(half_rows, half_rows), :].astype(jnp.bfloat16)
            exchange.start()
            keep.start()

    keep.wait()
    exchange.wait()
    for t in range(max(tiles - 2, 0), tiles):
        for copy in stores(t):
            copy.wait()
        store_term(t).wait()
    for i in range(2):
        for copy in ending(i):
            copy.wait()

    @pl.loop(0, chips)
    def _(step):
        for i in range(2):
            trade(i, step).wait_send()

            @pl.when(step < chips - 1)
            def _():
                onward(i, step).wait_send()


def back_call(call_id, cot_rows, normed_two, gate, upward, gate_full, up_full, down_full, down_term):
    size = lax.axis_size("dp")
    chips = size // 2
    tokens, depth = cot_rows.shape
    wide = gate.shape[1]
    tile = 256
    first = (wide // 256 + 1) // 2 * 256
    blocks = [(depth // chips, first // 2), (depth // chips, (wide - first) // 2)]
    low, high = jnp.bfloat16, jnp.float32
    far = pl.BlockSpec(memory_space=pl.ANY)
    dma = pltpu.SemaphoreType.DMA
    return pl.pallas_call(
        functools.partial(back_kernel, chips, tile),
        out_shape=[
            jax.ShapeDtypeStruct((tokens, wide), low),
            jax.ShapeDtypeStruct((tokens, wide), low),
            jax.ShapeDtypeStruct((tokens // 2, depth), high),
            jax.ShapeDtypeStruct((tokens // 2, depth), low),
            jax.ShapeDtypeStruct((depth // size, wide), high),
            jax.ShapeDtypeStruct((depth, wide), low),
        ],
        in_specs=[pl.BlockSpec(memory_space=pltpu.VMEM)] * 2 + [far] * 6,
        out_specs=[far] * 6,
        scratch_shapes=[pltpu.VMEM((chips,) + b, low) for b in blocks] * 2
        + [pltpu.VMEM((chips - 1,) + b, low) for b in blocks]
        + [pltpu.VMEM(b, high) for b in blocks]
        + [
            pltpu.VMEM((3, 2, depth, tile), low),
            pltpu.VMEM((2, 2, tokens, tile), high),
            pltpu.VMEM((2, 2, tokens, tile), low),
            pltpu.VMEM((tokens, depth), high),
            pltpu.VMEM((tokens // 2, depth), low),
            pltpu.VMEM((depth, tokens), low),
            pltpu.VMEM((tokens, wide), low),
            pltpu.VMEM((2, depth, tile), low),
            dma((3, 2)),
            dma((2, 2)),
            dma((2, 2)),
            dma((2,)),
            dma((1,)),
            dma((2,)),
        ]
        + [dma((2, chips))] * 5
        + [dma((2, 2)), dma((2,))],
        compiler_params=pltpu.CompilerParams(
            collective_id=call_id, has_side_effects=True, vmem_limit_bytes=VMEM_LIMIT
        ),
        cost_estimate=pl.CostEstimate(
            flops=8 * tokens * depth * wide,
            bytes_accessed=8 * depth * wide + 12 * tokens * wide,
            transcendentals=tokens * wide,
        ),
    )(cot_rows, normed_two, gate, upward, gate_full, up_full, down_full, down_term)


def layer_norm(values, norm_gain, norm_shift):
    center = values - jnp.mean(values, axis=-1, keepdims=True)
    inverse = lax.rsqrt(jnp.mean(center * center, axis=-1, keepdims=True) + EPS)
    scaled = center * inverse
    return (scaled * norm_gain + norm_shift, scaled, inverse)


def norm_back(grads, scaled, inverse, norm_gain):
    weighted = grads * norm_gain
    return inverse * (
        weighted
        - jnp.mean(weighted, axis=-1, keepdims=True)
        - scaled * jnp.mean(weighted * scaled, axis=-1, keepdims=True)
    )


def rotary_tables(segments, places, rotary_dims):
    earlier = (segments[None, :] < segments[:, None]).astype(jnp.int32)
    position = (places - jnp.sum(earlier, axis=1)).astype(jnp.float32)
    half_dims = rotary_dims // 2
    frequency = BASE ** (-2.0 * jnp.arange(half_dims, dtype=jnp.float32) / rotary_dims)
    angles = position[:, None] * frequency[None, :]
    return (jnp.cos(angles), jnp.sin(angles))


def rotate(values, cosine, sine_table, rotary_dims, turn_sign):
    half_dims = rotary_dims // 2
    leading = values[..., :half_dims]
    trailing = values[..., half_dims:rotary_dims]
    cos_rows = cosine[:, None, :]
    sin_rows = turn_sign * sine_table[:, None, :]
    return jnp.concatenate(
        [
            leading * cos_rows - trailing * sin_rows,
            trailing * cos_rows + leading * sin_rows,
            values[..., rotary_dims:],
        ],
        axis=-1,
    )


def masked_scores(query, key_rot, allowed, score_scale):
    scores = (
        jnp.einsum("qhd,khd->hqk", query, key_rot, preferred_element_type=jnp.float32) * score_scale
    )
    return jnp.where(allowed[None], scores, NEG)


def swap(values):
    return lax.ppermute(values, "mp", [(0, 1), (1, 0)])


def half_sum(part):
    half = part.shape[0] // 2
    other = swap(part[half:].astype(jnp.bfloat16))
    return part[:half] + other.astype(jnp.float32)


def grow(rows):
    return jnp.concatenate([rows, swap(rows)], axis=0)


def scatter(term, axis):
    return lax.psum_scatter(term, "dp", scatter_dimension=axis, tiled=True).astype(jnp.float32)


def body(
    inputs,
    segment_ids,
    norm1_gain,
    norm1_shift,
    qkv_weight,
    qkv_bias,
    out_weight,
    norm2_gain,
    norm2_shift,
    gate_weight,
    up_weight,
    down_weight,
    cotangent,
):
    score_scale = HEAD_DIM ** (-0.5)
    rows_here = inputs.shape[0]
    width = inputs.shape[1]
    *qkv_full, out_turned, far_inputs, far_cot = ring_call(
        0,
        shards=[qkv_weight, out_weight.T],
        sends=[inputs, cotangent],
    )
    input_rows = jnp.concatenate([inputs, far_inputs], axis=0)
    cot_rows = jnp.concatenate([cotangent, far_cot], axis=0)
    gate_weight, out_turned = lax.optimization_barrier((gate_weight, out_turned))
    gate_full = lax.all_gather(gate_weight, "dp", axis=0, tiled=True)
    stream_rows = input_rows.astype(jnp.float32)
    stream = stream_rows[:rows_here]
    normed_wide, scaled_rows, inverse_rows = layer_norm(stream_rows, norm1_gain, norm1_shift)
    normed_one = normed_wide.astype(jnp.bfloat16)
    scaled_one = scaled_rows[:rows_here]
    inverse_one = inverse_rows[:rows_here]
    seq_len = normed_one.shape[0]
    local_width = qkv_full[0].shape[1]
    head_count = local_width // HEAD_DIM
    turn = lax.axis_index("mp") * rows_here
    segments = jnp.roll(segment_ids[0], -turn)
    places = jnp.roll(jnp.arange(seq_len, dtype=jnp.int32), -turn)
    allowed = (places[None, :] <= places[:, None]) & (segments[:, None] == segments[None, :])
    cosine, sine_table = rotary_tables(segments, places, ROT)
    shaped = [
        (jnp.dot(normed_one, full, preferred_element_type=jnp.float32) + bias).reshape(
            seq_len, head_count, HEAD_DIM
        )
        for full, bias in zip(qkv_full, qkv_bias)
    ]
    query = rotate(shaped[0], cosine, sine_table, ROT, 1.0).astype(jnp.bfloat16)
    key_rot = rotate(shaped[1], cosine, sine_table, ROT, 1.0).astype(jnp.bfloat16)
    value = shaped[2].astype(jnp.bfloat16)
    scores = masked_scores(query, key_rot, allowed, score_scale)
    row_max = jnp.max(scores, axis=-1, keepdims=True)
    exponent = jnp.exp(scores - row_max)
    row_total = jnp.sum(exponent, axis=-1, keepdims=True)
    log_total = row_max + jnp.log(row_total)
    probs_low = (exponent / row_total).astype(jnp.bfloat16)
    mixed_heads = jnp.einsum(
        "hqk,khd->qhd", probs_low, value, preferred_element_type=jnp.float32
    ).astype(jnp.bfloat16)
    mixed = mixed_heads.reshape(seq_len, local_width)
    branch = jnp.dot(mixed, out_turned.T, preferred_element_type=jnp.float32)
    middle = stream + half_sum(branch)
    normed_wide2, scaled_two, inverse_two = layer_norm(middle, norm2_gain, norm2_shift)
    normed_here = normed_wide2.astype(jnp.bfloat16)
    up_full, down_turned, normed_two, gate, upward, hidden, down_term = feed_call(
        1, up_weight, down_weight.T, normed_here, cot_rows.T, gate_full
    )
    _, up_act, part_here, part_far, down_grad_turned, gate_term = back_call(
        3, cot_rows, normed_two, gate, upward, gate_full, up_full, down_turned, down_term
    )
    down_weight_grad = down_grad_turned.T
    normed_two_grad = part_here + part_far.astype(jnp.float32)
    gate_weight_grad = scatter(gate_term, 0)
    gain_two = jnp.sum(normed_two_grad * scaled_two, axis=0)
    shift_two = jnp.sum(normed_two_grad, axis=0)
    middle_grad = cotangent.astype(jnp.float32) + norm_back(
        normed_two_grad, scaled_two, inverse_two, norm2_gain
    )
    middle_low, hidden, up_act = lax.optimization_barrier(
        (middle_grad.astype(jnp.bfloat16), hidden, up_act)
    )
    middle_rows = grow(middle_low)
    up_term = jnp.dot(normed_two.T, up_act, preferred_element_type=jnp.float32)
    feed_part = jnp.dot(hidden, down_turned.T, preferred_element_type=jnp.float32)
    feed_low, middle_rows = lax.optimization_barrier(
        (feed_part[rows_here:].astype(jnp.bfloat16), middle_rows)
    )
    feed_far = swap(feed_low)
    feed = feed_part[:rows_here] + feed_far.astype(jnp.float32)
    output = (middle + feed).astype(jnp.bfloat16)
    out_term = jnp.dot(middle_rows.T, mixed, preferred_element_type=jnp.float32)
    mixed_flat = jnp.dot(middle_rows, out_turned, preferred_element_type=jnp.float32)
    mixed_grad = mixed_flat.astype(jnp.bfloat16).reshape(seq_len, head_count, HEAD_DIM)
    probs_wide = jnp.exp(scores - log_total)
    value_grad = jnp.einsum(
        "hqk,qhd->khd",
        probs_wide.astype(jnp.bfloat16),
        mixed_grad,
        preferred_element_type=jnp.float32,
    )
    prob_grad = jnp.einsum("qhd,khd->hqk", mixed_grad, value, preferred_element_type=jnp.float32)
    row_delta = jnp.transpose(
        jnp.sum(mixed_grad.astype(jnp.float32) * mixed_heads.astype(jnp.float32), axis=-1)
    )
    score_grad = (probs_wide * (prob_grad - row_delta[:, :, None]) * score_scale).astype(
        jnp.bfloat16
    )
    query_grad = jnp.einsum("hqk,khd->qhd", score_grad, key_rot, preferred_element_type=jnp.float32)
    key_grad = jnp.einsum("hqk,qhd->khd", score_grad, query, preferred_element_type=jnp.float32)
    query_back = rotate(query_grad, cosine, sine_table, ROT, -1.0)
    key_back = rotate(key_grad, cosine, sine_table, ROT, -1.0)
    proj_grad = [
        part.reshape(seq_len, local_width) for part in (query_back, key_back, value_grad)
    ]
    rotated_cols = jnp.arange(local_width, dtype=jnp.int32) % HEAD_DIM < ROT
    bias_sums = [jnp.sum(part, axis=0) for part in proj_grad]
    bias_term = [bias_sums[0], jnp.where(rotated_cols, bias_sums[1], 0.0), bias_sums[2]]
    proj_low = [part.astype(jnp.bfloat16) for part in proj_grad]
    normed_one_part = jnp.zeros((), jnp.float32)
    for part, full in zip(proj_low, qkv_full):
        product = jnp.dot(part, full.T, preferred_element_type=jnp.float32)
        normed_one_part = normed_one_part + product
    gain_one = jnp.sum(normed_one_part * scaled_rows, axis=0)
    shift_one = jnp.sum(normed_one_part, axis=0)
    norm_sums = jnp.concatenate([gain_one, shift_one, gain_two, shift_two])
    norm_sums = norm_sums + swap(norm_sums)
    sums = jnp.concatenate([norm_sums] + bias_term)
    spare = -sums.size % (8 * 256)
    qkv_term = [
        jnp.dot(normed_one.T, part, preferred_element_type=jnp.float32) for part in proj_low
    ]
    output, sums = lax.optimization_barrier((output, sums))
    all_sums, far_part, up_weight_grad, out_grad_turned, qkv_weight_grad = ring_call(
        2,
        shards=[jnp.pad(sums, (0, spare)).reshape(8, -1)],
        sends=[normed_one_part[rows_here:].astype(jnp.bfloat16)],
        parts=[term.astype(jnp.bfloat16) for term in [up_term, out_term] + qkv_term],
        groups=[1, 1, 3],
    )
    out_weight_grad = out_grad_turned.T
    normed_one_grad = normed_one_part[:rows_here] + far_part.astype(jnp.float32)
    all_sums = jnp.sum(all_sums.reshape(-1, 8, all_sums.shape[1]), axis=0).reshape(-1)
    gain_one, shift_one, gain_two, shift_two = all_sums[: 4 * width].reshape(4, width)
    qkv_bias_grad = all_sums[4 * width : sums.size].reshape(3, local_width)
    input_grad = middle_grad + norm_back(normed_one_grad, scaled_one, inverse_one, norm1_gain)
    return (
        output,
        input_grad,
        gain_one,
        shift_one,
        qkv_weight_grad,
        qkv_bias_grad,
        out_weight_grad,
        gain_two,
        shift_two,
        gate_weight_grad,
        up_weight_grad,
        down_weight_grad,
    )


def solution(mesh):
    in_specs = (
        P(("dp", "mp"), None),
        P("dp", None),
        P(),
        P(),
        P(None, "dp", "mp"),
        P(None, "mp"),
        P("mp", "dp"),
        P(),
        P(),
        P("dp", "mp"),
        P("dp", "mp"),
        P("mp", "dp"),
        P(("dp", "mp"), None),
    )
    out_specs = (
        P(("dp", "mp"), None),
        P(("dp", "mp"), None),
        P(),
        P(),
        P(None, "dp", "mp"),
        P(None, "mp"),
        P("mp", "dp"),
        P(),
        P(),
        P("dp", "mp"),
        P("dp", "mp"),
        P("mp", "dp"),
    )
    return jax.shard_map(body, mesh=mesh, in_specs=in_specs, out_specs=out_specs, check_vma=False)
```
